32 devices in a mesh: slab: 4 (over z), tile: 8 (over y, x, core).
Axes of the slice: x: 2, y: 2, z: 4, core: 2. Of those that a mesh axis runs over, the one named last changes fastest.
Arguments:
- voxel_grid: float32 [4, 64, 64, 256], P(None, 'slab', 'tile'), may hold values from -4 to 4
- first_moment: float32 [4, 64, 64, 256], P(None, 'slab', 'tile'), may hold values from -0.75 to 0.75
- second_moment: float32 [4, 64, 64, 256], P(None, 'slab', 'tile'), may hold values from 0.01 to 0.5
- pixel_index: int32 [32768], P('tile'), may hold values from 0 to 2047
- start_slab: int32 [32768], P('tile'), may hold values from 0 to 1
- ray_count: int32 [32768], P('tile'), may hold values from 16 to 48
- target: float32 [3, 32768], P(None, 'tile'), may hold values from 0 to 1
Outputs:
- new_grid: float32 [4, 64, 64, 256], P(None, 'slab', 'tile')
- new_first: float32 [4, 64, 64, 256], P(None, 'slab', 'tile')
- new_second: float32 [4, 64, 64, 256], P(None, 'slab', 'tile')
The draws below stay inside these ranges and needn't reach their ends.
All inputs are finite; a program needn't handle non-finite values.
Results may differ from the reference program's by a relative error of at most 0.0003.
Values sent between devices are 32-bit elements; how exact they have to be, the bound alone decides.
A program may use at most 128 MiB of HBM per device.

```python
import math
import jax
import jax.numpy as jnp
from jax import lax

CZ = 16
CX = 8
NY = 256
RAYS_DEV = 4096
STEP = 20
NZ = 64
NX = 64
RAYS = 32768
HALF_SLABS = 2
N_TILE = 8


def place_ends(result, rng, least, top_value):
    longest = result.shape.index(max(result.shape))
    spots = []
    for shift in (0, 1):
        where = [jax.random.randint(jax.random.fold_in(rng, axis), (), 0, length) for axis, length in enumerate(result.shape)]
        where[longest] = (where[longest] + shift) % result.shape[longest]
        spots.append(tuple(where))
    return result.at[spots[0]].set(least).at[spots[1]].set(top_value)


def block_levels(key, shape, pieces, least, top_value):
    loudness = 1.0
    for axis_at, blocks in pieces:
        draws = jax.random.uniform(jax.random.fold_in(jax.random.fold_in(key, 6), axis_at), (blocks,), jnp.float32, least / len(pieces), top_value / len(pieces))
        loudness = loudness * jnp.repeat(jnp.exp(draws), shape[axis_at] // blocks).reshape((-1,) + (1,) * (len(shape) - 1 - axis_at))
    return loudness


def bell_draw(key, dims, spread, reach, split=(), kind=jnp.bfloat16):
    array = spread * jax.random.normal(key, dims, jnp.float32)
    if split:
        array = array * block_levels(key, dims, split, -0.22, 0.18)
    return jnp.clip(array, -reach, reach).astype(kind)


def setup_inputs(seed: int = 0) -> dict:
    seeds = jax.random.split(jax.random.key(seed), 8)
    return {
        "voxel_grid": bell_draw(seeds[0], (4, NZ, NX, NY), 1.0, 4.0, ((1, 4), (2, 8)), jnp.float32),
        "first_moment": bell_draw(seeds[1], (4, NZ, NX, NY), 0.05, 0.75, ((1, 4), (2, 8)), jnp.float32),
        "second_moment": jnp.clip(jnp.exp(math.log(0.5) - 3.912023 * jax.random.uniform(seeds[2], (4, NZ, NX, NY), jnp.float32) ** block_levels(seeds[2], (4, NZ, NX, NY), ((1, 4), (2, 8)), -0.2, 0.2)), 0.01, 0.5),
        "pixel_index": place_ends(jax.random.randint(seeds[3], (RAYS,), 0, CX * NY), jax.random.fold_in(seeds[3], 1), 0, (CX * NY) - 1).astype(jnp.int32),
        "start_slab": place_ends(jax.random.randint(seeds[4], (RAYS,), 0, HALF_SLABS), jax.random.fold_in(seeds[4], 1), 0, HALF_SLABS - 1).astype(jnp.int32),
        "ray_count": place_ends(jax.random.randint(seeds[5], (RAYS,), NZ // 4, NZ // 2 + CZ + 1), jax.random.fold_in(seeds[5], 1), NZ // 4, (NZ // 2 + CZ + 1) - 1).astype(jnp.int32),
        "target": jnp.clip(1.0 * jax.random.uniform(seeds[6], (3, RAYS), jnp.float32) ** block_levels(seeds[6], (3, RAYS), ((1, 8),), -0.2, 0.2), 0.0, 1.0),
    }


RENDER_WEIGHT = 1000.0
TV_WEIGHT = 0.05
BACKGROUND = 1.0
STEP_SPAN = 4.0
CLIP_RMS = 0.25
LEARN_RATE = 0.02
BETA_ONE = 0.9
BETA_TWO = 0.99
EPSILON = 1e-08

def tile_loss(tile_grid, pixel_index, start_slab, ray_count, target):
    flat = tile_grid.reshape(4, NZ, CX * NY)
    samples = jnp.take(flat, pixel_index, axis=2)
    depth_pos = jnp.arange(NZ, dtype=jnp.int32)[:, None]
    first_cell = start_slab[None, :] * CZ
    inside = (depth_pos >= first_cell) & (depth_pos < first_cell + ray_count[None, :])
    optical = jnp.where(inside, jax.nn.softplus(samples[0]) * (STEP_SPAN / NZ), 0.0)
    running = jnp.cumsum(optical, axis=0)
    weights = jnp.exp(-(running - optical)) * (1.0 - jnp.exp(-optical))
    colors = jax.nn.sigmoid(samples[1:4])
    rendered = lax.optimization_barrier(jnp.sum(weights[None] * colors, axis=1)) + jnp.exp(-running[-1])[None] * BACKGROUND
    return 0.5 * RENDER_WEIGHT * jnp.sum((rendered - target) ** 2)

def reference(voxel_grid, first_moment, second_moment, pixel_index, start_slab, ray_count, target):
    tiles = voxel_grid.reshape(4, NZ, N_TILE, CX, NY).transpose(2, 0, 1, 3, 4)
    pixels = pixel_index.reshape(N_TILE, RAYS_DEV)
    starts = start_slab.reshape(N_TILE, RAYS_DEV)
    counts = ray_count.reshape(N_TILE, RAYS_DEV)
    targets = target.reshape(3, N_TILE, RAYS_DEV).transpose(1, 0, 2)

    def one_tile(inputs):
        return jax.grad(tile_loss)(*inputs)
    tile_grads = lax.map(one_tile, (tiles, pixels, starts, counts, targets))
    render_grad = tile_grads.transpose(1, 2, 0, 3, 4).reshape(4, NZ, NX, NY)
    smooth = jnp.zeros_like(voxel_grid)
    for axis_num in (1, 2, 3):
        step_diff = jnp.diff(voxel_grid, axis=axis_num)
        low_pad = [(0, 0)] * 4
        high_pad = [(0, 0)] * 4
        low_pad[axis_num] = (0, 1)
        high_pad[axis_num] = (1, 0)
        smooth = smooth + jnp.pad(-step_diff, low_pad) + jnp.pad(step_diff, high_pad)
    gradient = render_grad + 2.0 * TV_WEIGHT * smooth
    norm_value = jnp.sqrt(jnp.sum(gradient * gradient))
    limit = CLIP_RMS * math.sqrt(4.0 * NZ * NX * NY)
    clipped = gradient * (limit / jnp.maximum(norm_value, limit))
    new_first = BETA_ONE * first_moment + (1.0 - BETA_ONE) * clipped
    new_second = BETA_TWO * second_moment + (1.0 - BETA_TWO) * clipped * clipped
    first_hat = new_first / (1.0 - BETA_ONE ** STEP)
    second_hat = new_second / (1.0 - BETA_TWO ** STEP)
    new_grid = voxel_grid - LEARN_RATE * first_hat / (jnp.sqrt(second_hat) + EPSILON)
    return (new_grid, new_first, new_second)
```

```python
import functools
import math

import jax
import jax.numpy as jnp
from jax import lax
from jax.experimental import pallas as pl
from jax.experimental.pallas import tpu as pltpu
from jax.sharding import PartitionSpec as P

STEP = 20
RENDER_WEIGHT = 1000.0
TV_WEIGHT = 0.05
BACKGROUND = 1.0
STEP_SPAN = 4.0
CLIP_RMS = 0.25
LEARN_RATE = 0.02
BETA_ONE = 0.9
BETA_TWO = 0.99
EPSILON = 1e-08
CHUNK = 512
DIRECT_LIMIT = 64
MESH = pl.DeviceIdType.MESH


def kernel(
    ns, nt, chunk,
    grid_hbm, first_hbm, second_hbm, pix_hbm, start_hbm, count_hbm, target_hbm,
    grid_ref, first_ref, second_ref, grad_ref, scale_ref,
    pix_ref, start_ref, count_ref, target_ref,
    pair_ref, trans_ref, weight_ref, sig_ref, onehot_ref, row_ref, parts_ref, table_ref,
    edge_ref, xhalo_ref, zhalo_ref, nsend_ref, nrecv_ref,
    part_send, part_recv, ready_sem, halo_send, halo_recv, norm_send, norm_recv, load_sem,
):
    channels, depth, rx, ry = grid_ref.shape
    rays = pix_ref.shape[1]
    chunks = rays // chunk
    total_depth = depth * ns
    reach = span_reach(ns)
    span = STEP_SPAN / total_depth
    rows = depth * rx
    slab = lax.axis_index("slab")
    tile = lax.axis_index("tile")

    def slab_peer(d):
        return {"slab": lax.rem(slab + d, ns)}

    def tile_peer(d):
        return {"tile": lax.rem(tile + d, nt)}

    if direct(ns, nt):
        pair = {"tile": tile + 1 - 2 * lax.rem(tile, 2)}
        half = nt // 2
        others = [
            {"slab": lax.rem(slab + k // half, ns), "tile": lax.rem(tile + 2 * (k % half), nt)}
            for k in range(1, ns * half)
        ]
        phases = [[pair], others]
        near = reach
    else:
        phases = [[tile_peer(d) for d in range(1, nt)], [slab_peer(d) for d in range(1, ns)]]
        near = ns - 1
    offsets = [k for k in range(-near, near + 1) if k]
    travels = [k for k in range(-reach, reach + 1) if k]

    def inside(s):
        return (s >= 0) & (s < ns)

    loads = [
        pltpu.make_async_copy(grid_hbm.at[c], grid_ref.at[c], load_sem.at[c])
        for c in range(channels)
    ]
    rest = (
        (pix_hbm, pix_ref), (start_hbm, start_ref), (count_hbm, count_ref),
        (target_hbm, target_ref), (first_hbm, first_ref), (second_hbm, second_ref),
    )
    loads += [
        pltpu.make_async_copy(a, b, load_sem.at[channels + i]) for i, (a, b) in enumerate(rest)
    ]
    for copy in loads:
        copy.start()

    barrier = pltpu.get_barrier_semaphore()
    for d in range(1, nt):
        pl.semaphore_signal(barrier, inc=1, device_id=tile_peer(d), device_id_type=MESH)
    greeters = nt - 1
    for k in offsets:
        @pl.when(inside(slab + k))
        def _(k=k):
            pl.semaphore_signal(
                barrier, inc=1, device_id={"slab": slab + k}, device_id_type=MESH)
        greeters = greeters + inside(slab + k).astype(jnp.int32)

    for c in range(channels):
        loads[c].wait()
    edge_ref[0] = grid_ref[:, :, rx - 1, :]
    edge_ref[1] = grid_ref[:, :, 0, :]

    total = jnp.zeros((rx, ry), jnp.float32)
    before = jnp.ones((rx, ry), jnp.float32)
    sums = [jnp.zeros((rx, ry), jnp.float32) for _ in range(3)]
    for z in range(depth):
        s = grid_ref[0, z]
        e = jnp.exp(-jnp.abs(s))
        tau = (jnp.maximum(s, 0.0) + jnp.log1p(e)) * span
        sig_ref[0, z] = jnp.where(s >= 0, 1.0, e) / (1.0 + e)
        total = total + tau
        after = jnp.exp(-total)
        w = before * (1.0 - jnp.exp(-tau))
        before = after
        trans_ref[z] = after
        weight_ref[z] = w
        for c in range(3):
            col = 1.0 / (1.0 + jnp.exp(-grid_ref[c + 1, z]))
            sig_ref[c + 1, z] = col
            sums[c] = sums[c] + w * col
            table_ref[pl.ds(c * rows + z * rx, rx), :] = sums[c]
        table_ref[pl.ds(3 * rows + z * rx, rx), :] = after
    full = table_ref[...]
    high = full.astype(jnp.bfloat16)
    pair_ref[:, :ry] = high
    pair_ref[:, ry:] = (full - high.astype(jnp.float32)).astype(jnp.bfloat16)

    pl.semaphore_wait(barrier, greeters)

    def halo_copy(src, dst, i, peer):
        return pltpu.make_async_remote_copy(
            src_ref=src, dst_ref=dst, send_sem=halo_send.at[i], recv_sem=halo_recv.at[i],
            device_id=peer, device_id_type=MESH)

    halos = [
        (halo_copy(grid_ref.at[:, depth - 1], zhalo_ref.at[0], 0, slab_peer(1)), slab < ns - 1, slab > 0),
        (halo_copy(grid_ref.at[:, 0], zhalo_ref.at[1], 1, slab_peer(ns - 1)), slab > 0, slab < ns - 1),
        (halo_copy(edge_ref.at[0], xhalo_ref.at[0], 2, tile_peer(1)), tile < nt - 1, tile > 0),
        (halo_copy(edge_ref.at[1], xhalo_ref.at[1], 3, tile_peer(nt - 1)), tile > 0, tile < nt - 1),
    ]
    for copy, sends, _ in halos:
        pl.when(sends)(copy.start)

    def part_copy(k, j, source):
        lane = travels.index(k)
        return pltpu.make_async_remote_copy(
            src_ref=parts_ref.at[source, j], dst_ref=parts_ref.at[source, j],
            send_sem=part_send.at[lane, j], recv_sem=part_recv.at[lane, j],
            device_id={"slab": source + k}, device_id_type=MESH)

    def part_start(k, j):
        pl.when(inside(slab + k))(lambda: part_copy(k, j, slab).start())

    def part_sent(k, j):
        pl.when(inside(slab + k))(lambda: part_copy(k, j, slab).wait_send())

    def part_wait(k, j):
        pl.when(inside(slab - k))(lambda: part_copy(k, j, slab - k).wait_recv())

    y_ids = lax.broadcasted_iota(jnp.int32, (ry, chunk), 0).astype(jnp.float32).astype(jnp.bfloat16)
    row_ids = lax.broadcasted_iota(jnp.int32, (rows, chunk), 0)

    for copy in loads[channels:channels + 3]:
        copy.wait()
    for j in range(chunks):
        at = pl.ds(j * chunk, chunk)
        pix = pix_ref[:, at]
        start = start_ref[:, at]
        px = pix // ry
        py = (pix - px * ry).astype(jnp.float32).astype(jnp.bfloat16)
        length = jnp.clip((start - slab) * depth + count_ref[:, at], 0, depth)
        length = jnp.where(slab >= start, length, 0)
        row = jnp.where(length > 0, (length - 1) * rx + px, -1)
        row_ref[:, at] = row
        hot = jnp.where(y_ids == py, jnp.ones((), jnp.bfloat16), jnp.zeros((), jnp.bfloat16))
        onehot_ref[:, at] = hot
        mask = row_ids == row
        u = jnp.dot(pair_ref[:, :ry], hot, preferred_element_type=jnp.float32)
        u = u + jnp.dot(pair_ref[:, ry:], hot, preferred_element_type=jnp.float32)
        for c in range(4):
            picked = jnp.where(mask, u[c * rows:(c + 1) * rows], 0.0)
            part = jnp.sum(picked, axis=0, keepdims=True)
            if c == 3:
                part = jnp.where(row < 0, 1.0, part)
            parts_ref[slab, j, pl.ds(c, 1), :] = part
        for k in travels:
            part_start(k, j)

    for copy, _, receives in halos:
        pl.when(receives)(copy.wait_recv)
    x_ids = lax.broadcasted_iota(jnp.int32, (rx, ry), 0)
    lane_ids = lax.broadcasted_iota(jnp.int32, (rx, ry), 1)
    first_x = tile == 0
    last_x = tile == nt - 1
    for c in range(channels):
        for z in range(depth):
            g = grid_ref[c, z]
            if z > 0:
                below = grid_ref[c, z - 1]
            else:
                below = jnp.where(slab > 0, zhalo_ref[0, c], g)
            if z < depth - 1:
                above = grid_ref[c, z + 1]
            else:
                above = jnp.where(slab < ns - 1, zhalo_ref[1, c], g)
            xl = jnp.broadcast_to(xhalo_ref[0, c, pl.ds(z, 1), :], (rx, ry))
            xh = jnp.broadcast_to(xhalo_ref[1, c, pl.ds(z, 1), :], (rx, ry))
            xl = jnp.where(first_x, g, xl)
            xh = jnp.where(last_x, g, xh)
            left = jnp.where(x_ids == 0, xl, pltpu.roll(g, 1, 0))
            right = jnp.where(x_ids == rx - 1, xh, pltpu.roll(g, rx - 1, 0))
            down = jnp.where(lane_ids == 0, g, pltpu.roll(g, 1, 1))
            up = jnp.where(lane_ids == ry - 1, g, pltpu.roll(g, ry - 1, 1))
            smooth = (g - below) + (g - above) + (g - left) + (g - right) + (g - down) + (g - up)
            grad_ref[c, z] = (2.0 * TV_WEIGHT) * smooth

    loads[channels + 3].wait()
    row_ids16 = row_ids.astype(jnp.float32).astype(jnp.bfloat16)
    for j in range(chunks):
        for k in travels:
            part_wait(k, j)
        if j == 0 and direct(ns, nt):
            for k in (-reach, reach):
                @pl.when(inside(slab + k))
                def _(k=k):
                    pl.semaphore_signal(
                        ready_sem, inc=1, device_id={"slab": slab + k}, device_id_type=MESH)
        at = pl.ds(j * chunk, chunk)
        front_c = jnp.zeros((3, chunk), jnp.float32)
        front_t = jnp.ones((1, chunk), jnp.float32)
        beyond = jnp.full((3, chunk), BACKGROUND, jnp.float32)
        for k in range(reach, 0, -1):
            here = slab >= k
            source = jnp.maximum(slab - k, 0)
            pc = parts_ref[source, j, pl.ds(0, 3), :]
            pt = parts_ref[source, j, pl.ds(3, 1), :]
            front_c = jnp.where(here, front_c + front_t * pc, front_c)
            front_t = jnp.where(here, front_t * pt, front_t)
        for k in range(reach, 0, -1):
            here = slab + k < ns
            source = jnp.minimum(slab + k, ns - 1)
            pc = parts_ref[source, j, pl.ds(0, 3), :]
            pt = parts_ref[source, j, pl.ds(3, 1), :]
            beyond = jnp.where(here, pc + pt * beyond, beyond)
        pc = parts_ref[slab, j, pl.ds(0, 3), :]
        pt = parts_ref[slab, j, pl.ds(3, 1), :]
        rendered = front_c + front_t * (pc + pt * beyond)
        residual = RENDER_WEIGHT * (rendered - target_ref[:, at])
        color_cot = front_t * residual
        trans_cot = front_t * jnp.sum(residual * beyond, axis=0, keepdims=True)
        hot = onehot_ref[:, at]
        mask = row_ids16 == row_ref[:, at].astype(jnp.float32).astype(jnp.bfloat16)
        none = jnp.zeros((), jnp.bfloat16)
        tops = []
        lows = []
        for c in range(4):
            cot = color_cot[c:c + 1] if c < 3 else trans_cot
            top = cot.astype(jnp.bfloat16)
            low = (cot - top.astype(jnp.float32)).astype(jnp.bfloat16)
            tops.append(jnp.where(mask, top, none))
            lows.append(jnp.where(mask, low, none))
        u = sum(
            lax.dot_general(
                jnp.concatenate(spread, axis=0), hot, (((1,), (1,)), ((), ())),
                preferred_element_type=jnp.float32)
            for spread in (tops, lows))
        if j == 0:
            table_ref[...] = u
        else:
            table_ref[...] += u

    zero = jnp.zeros((rx, ry), jnp.float32)
    suffix = [zero, zero, zero]
    later = zero
    squares = zero
    for z in range(depth - 1, -1, -1):
        w = weight_ref[z]
        after = trans_ref[z]
        later = later + after * table_ref[pl.ds(3 * rows + z * rx, rx), :]
        dw = zero
        for c in range(3):
            suffix[c] = suffix[c] + table_ref[pl.ds(c * rows + z * rx, rx), :]
            col = sig_ref[c + 1, z]
            dw = dw + col * suffix[c]
            out = grad_ref[c + 1, z] + w * suffix[c] * (col * (1.0 - col))
            grad_ref[c + 1, z] = out
            squares = squares + out * out
        dtau = after * dw - later
        later = later + w * dw
        out = grad_ref[0, z] + dtau * (sig_ref[0, z] * span)
        grad_ref[0, z] = out
        squares = squares + out * out

    local = jnp.sum(squares)

    def norm_copy(phase, slot, peer):
        return pltpu.make_async_remote_copy(
            src_ref=nsend_ref.at[phase], dst_ref=nrecv_ref.at[slot],
            send_sem=norm_send.at[slot], recv_sem=norm_recv.at[slot],
            device_id=peer, device_id_type=MESH)

    if direct(ns, nt):
        far = inside(slab - reach).astype(jnp.int32) + inside(slab + reach).astype(jnp.int32)
        pl.semaphore_wait(ready_sem, far)
    value = jnp.full((1, 128), local, jnp.float32)
    copies = []
    base = 0
    for phase, peers in enumerate(phases):
        nsend_ref[phase] = value
        group = [norm_copy(phase, base + i, peer) for i, peer in enumerate(peers)]
        for copy in group:
            copy.start()
        for i, copy in enumerate(group):
            copy.wait_recv()
            value = value + nrecv_ref[base + i]
        base += len(group)
        copies += group
    limit = CLIP_RMS * math.sqrt(4.0 * total_depth * (rx * nt) * ry)
    scale_ref[...] = limit / jnp.maximum(jnp.sqrt(value), limit)
    for copy in loads[channels + 4:]:
        copy.wait()
    for copy in copies:
        copy.wait_send()
    for copy, sends, _ in halos:
        pl.when(sends)(copy.wait_send)
    for j in range(chunks):
        for k in travels:
            part_sent(k, j)


def span_reach(ns):
    return max(ns // 2, 1)


def direct(ns, nt):
    return ns * nt <= DIRECT_LIMIT and nt % 2 == 0


def adam_kernel(
    grid_ref, first_ref, second_ref, grad_ref, scale_ref,
    grid_hbm, first_hbm, second_hbm, grid_out, first_out, second_out, sem,
):
    channels, depth, rx, ry = grid_ref.shape
    scale = jnp.broadcast_to(scale_ref[0:1, 0:1], (rx, ry))
    copies = []
    for c in range(channels):
        for z in range(depth):
            clipped = grad_ref[c, z] * scale
            first = BETA_ONE * first_ref[c, z] + (1.0 - BETA_ONE) * clipped
            second = BETA_TWO * second_ref[c, z] + (1.0 - BETA_TWO) * clipped * clipped
            first_out[c, z] = first
            second_out[c, z] = second
            first_hat = first * (1.0 / (1.0 - BETA_ONE**STEP))
            second_hat = second * (1.0 / (1.0 - BETA_TWO**STEP))
            grid_out[c, z] = grid_ref[c, z] - LEARN_RATE * first_hat / (
                jnp.sqrt(second_hat) + EPSILON)
        pairs = ((first_out, first_hbm), (second_out, second_hbm), (grid_out, grid_hbm))
        for i, (a, b) in enumerate(pairs):
            copy = pltpu.make_async_copy(a.at[c], b.at[c], sem.at[i, c])
            copy.start()
            copies.append(copy)
    for copy in copies:
        copy.wait()


def per_device(voxel_grid, first_moment, second_moment, pixel_index, start_slab, ray_count, target):
    ns = lax.axis_size("slab")
    nt = lax.axis_size("tile")
    channels, depth, rx, ry = voxel_grid.shape
    rays = pixel_index.shape[0]
    chunk = math.gcd(rays, CHUNK)
    chunks = rays // chunk
    rows = depth * rx
    messages = ns * nt // 2 if direct(ns, nt) else nt + ns - 2
    f32 = jnp.float32
    vmem = pl.BlockSpec(memory_space=pltpu.VMEM)
    hbm = pl.BlockSpec(memory_space=pltpu.HBM)
    cells = jax.ShapeDtypeStruct(voxel_grid.shape, f32)
    staged = pl.pallas_call(
        functools.partial(kernel, ns, nt, chunk),
        out_shape=(cells, cells, cells, cells, jax.ShapeDtypeStruct((1, 128), f32)),
        in_specs=[hbm] * 7,
        out_specs=(vmem,) * 5,
        scratch_shapes=[
            pltpu.VMEM((1, rays), jnp.int32),
            pltpu.VMEM((1, rays), jnp.int32),
            pltpu.VMEM((1, rays), jnp.int32),
            pltpu.VMEM(target.shape, f32),
            pltpu.VMEM((channels * rows, 2 * ry), jnp.bfloat16),
            pltpu.VMEM((depth, rx, ry), f32),
            pltpu.VMEM((depth, rx, ry), f32),
            pltpu.VMEM((channels, depth, rx, ry), f32),
            pltpu.VMEM((ry, rays), jnp.bfloat16),
            pltpu.VMEM((1, rays), jnp.int32),
            pltpu.VMEM((ns, chunks, 4, chunk), f32),
            pltpu.VMEM((channels * rows, ry), f32),
            pltpu.VMEM((2, channels, depth, ry), f32),
            pltpu.VMEM((2, channels, depth, ry), f32),
            pltpu.VMEM((2, channels, rx, ry), f32),
            pltpu.VMEM((2, 1, 128), f32),
            pltpu.VMEM((messages, 1, 128), f32),
            pltpu.SemaphoreType.DMA((2 * span_reach(ns), chunks)),
            pltpu.SemaphoreType.DMA((2 * span_reach(ns), chunks)),
            pltpu.SemaphoreType.REGULAR,
            pltpu.SemaphoreType.DMA((4,)),
            pltpu.SemaphoreType.DMA((4,)),
            pltpu.SemaphoreType.DMA((messages,)),
            pltpu.SemaphoreType.DMA((messages,)),
            pltpu.SemaphoreType.DMA((channels + 6,)),
        ],
        compiler_params=pltpu.CompilerParams(
            collective_id=0, has_side_effects=True, vmem_limit_bytes=32 * 1024 * 1024
        ),
        name="render_step",
    )(*(pltpu.with_memory_space_constraint(a, pltpu.HBM) for a in (
        voxel_grid,
        first_moment,
        second_moment,
        pixel_index.reshape(1, rays),
        start_slab.reshape(1, rays),
        ray_count.reshape(1, rays),
        target,
    )))
    return pl.pallas_call(
        adam_kernel,
        out_shape=(cells, cells, cells),
        in_specs=[vmem] * 5,
        out_specs=(hbm, hbm, hbm),
        scratch_shapes=[
            pltpu.VMEM(voxel_grid.shape, f32),
            pltpu.VMEM(voxel_grid.shape, f32),
            pltpu.VMEM(voxel_grid.shape, f32),
            pltpu.SemaphoreType.DMA((3, channels)),
        ],
        compiler_params=pltpu.CompilerParams(vmem_limit_bytes=32 * 1024 * 1024),
        name="adam",
    )(*staged)


def solution(mesh):
    cells = P(None, "slab", "tile", None)
    return jax.shard_map(
        per_device,
        mesh=mesh,
        in_specs=(cells, cells, cells, P("tile"), P("tile"), P("tile"), P(None, "tile")),
        out_specs=(cells, cells, cells),
        check_vma=False,
    )
```

```python
import functools
import math

import jax
import jax.numpy as jnp
from jax import lax
from jax.experimental import pallas as pl
from jax.experimental.pallas import tpu as pltpu
from jax.sharding import PartitionSpec as P

STEP = 20
RENDER_WEIGHT = 1000.0
TV_WEIGHT = 0.05
BACKGROUND = 1.0
STEP_SPAN = 4.0
CLIP_RMS = 0.25
LEARN_RATE = 0.02
BETA_ONE = 0.9
BETA_TWO = 0.99
EPSILON = 1e-08
CHUNK = 1024
DIRECT_LIMIT = 64
MESH = pl.DeviceIdType.MESH


def kernel(
    ns, nt, chunk,
    grid_hbm, first_hbm, second_hbm, pix_hbm, start_hbm, count_hbm, target_hbm,
    grid_ref, first_ref, second_ref, grad_ref, scale_ref,
    pix_ref, start_ref, count_ref, target_ref,
    pair_ref, trans_ref, weight_ref, sig_ref, onehot_ref, row_ref, table_ref,
    whole_ref, wholes_ref, front_ref, own_ref, last_ref, near_ref, far_ref,
    edge_ref, xhalo_ref, zhalo_ref, nsend_ref, nrecv_ref,
    whole_send, whole_recv, part_send, part_recv, ready_sem, halo_send, halo_recv, norm_send, norm_recv, load_sem,
):
    channels, depth, rx, ry = grid_ref.shape
    rays = pix_ref.shape[1]
    chunks = rays // chunk
    total_depth = depth * ns
    reach = span_reach(ns)
    span = STEP_SPAN / total_depth
    rows = depth * rx
    slab = lax.axis_index("slab")
    tile = lax.axis_index("tile")

    def slab_peer(d):
        return {"slab": lax.rem(slab + d, ns)}

    def tile_peer(d):
        return {"tile": lax.rem(tile + d, nt)}

    if direct(ns, nt):
        pair = {"tile": tile + 1 - 2 * lax.rem(tile, 2)}
        half = nt // 2
        others = [
            {"slab": lax.rem(slab + k // half, ns), "tile": lax.rem(tile + 2 * (k % half), nt)}
            for k in range(1, ns * half)
        ]
        phases = [[pair], others]
        near = reach
    else:
        phases = [[tile_peer(d) for d in range(1, nt)], [slab_peer(d) for d in range(1, ns)]]
        near = ns - 1
    offsets = [k for k in range(-near, near + 1) if k]

    def inside(s):
        return (s >= 0) & (s < ns)

    loads = [
        pltpu.make_async_copy(grid_hbm.at[c], grid_ref.at[c], load_sem.at[c])
        for c in range(channels)
    ]
    rest = (
        (pix_hbm, pix_ref), (start_hbm, start_ref), (count_hbm, count_ref),
        (target_hbm, target_ref), (first_hbm, first_ref), (second_hbm, second_ref),
    )
    loads += [
        pltpu.make_async_copy(a, b, load_sem.at[channels + i]) for i, (a, b) in enumerate(rest)
    ]
    for copy in loads:
        copy.start()

    barrier = pltpu.get_barrier_semaphore()
    for d in range(1, nt):
        pl.semaphore_signal(barrier, inc=1, device_id=tile_peer(d), device_id_type=MESH)
    greeters = nt - 1
    for k in offsets:
        @pl.when(inside(slab + k))
        def _(k=k):
            pl.semaphore_signal(
                barrier, inc=1, device_id={"slab": slab + k}, device_id_type=MESH)
        greeters = greeters + inside(slab + k).astype(jnp.int32)

    for c in range(channels):
        loads[c].wait()
    edge_ref[0] = grid_ref[:, :, rx - 1, :]
    edge_ref[1] = grid_ref[:, :, 0, :]

    total = jnp.zeros((rx, ry), jnp.float32)
    before = jnp.ones((rx, ry), jnp.float32)
    sums = [jnp.zeros((rx, ry), jnp.float32) for _ in range(3)]
    for z in range(depth):
        s = grid_ref[0, z]
        e = jnp.exp(-jnp.abs(s))
        tau = (jnp.maximum(s, 0.0) + jnp.log1p(e)) * span
        sig_ref[0, z] = jnp.where(s >= 0, 1.0, e) / (1.0 + e)
        total = total + tau
        after = jnp.exp(-total)
        w = before * (1.0 - jnp.exp(-tau))
        before = after
        trans_ref[z] = after
        weight_ref[z] = w
        for c in range(3):
            col = 1.0 / (1.0 + jnp.exp(-grid_ref[c + 1, z]))
            sig_ref[c + 1, z] = col
            sums[c] = sums[c] + w * col
            table_ref[pl.ds(c * rows + z * rx, rx), :] = sums[c]
        table_ref[pl.ds(3 * rows + z * rx, rx), :] = after
    for c in range(3):
        whole_ref[c] = sums[c]
    whole_ref[3] = before
    full = table_ref[...]
    high = full.astype(jnp.bfloat16)
    pair_ref[:, :ry] = high
    pair_ref[:, ry:] = (full - high.astype(jnp.float32)).astype(jnp.bfloat16)

    pl.semaphore_wait(barrier, greeters)

    def whole_copy(k):
        return pltpu.make_async_remote_copy(
            src_ref=whole_ref, dst_ref=wholes_ref.at[k - 1],
            send_sem=whole_send.at[k - 1], recv_sem=whole_recv.at[k - 1],
            device_id=slab_peer(k), device_id_type=MESH)

    for k in range(reach, 0, -1):
        pl.when(slab + k < ns)(whole_copy(k).start)

    def halo_copy(src, dst, i, peer):
        return pltpu.make_async_remote_copy(
            src_ref=src, dst_ref=dst, send_sem=halo_send.at[i], recv_sem=halo_recv.at[i],
            device_id=peer, device_id_type=MESH)

    halos = [
        (halo_copy(grid_ref.at[:, depth - 1], zhalo_ref.at[0], 0, slab_peer(1)), slab < ns - 1, slab > 0),
        (halo_copy(grid_ref.at[:, 0], zhalo_ref.at[1], 1, slab_peer(ns - 1)), slab > 0, slab < ns - 1),
        (halo_copy(edge_ref.at[0], xhalo_ref.at[0], 2, tile_peer(1)), tile < nt - 1, tile > 0),
        (halo_copy(edge_ref.at[1], xhalo_ref.at[1], 3, tile_peer(nt - 1)), tile > 0, tile < nt - 1),
    ]
    for copy, sends, _ in halos:
        pl.when(sends)(copy.start)

    def part_copy(k, j):
        src, dst = (last_ref, far_ref) if k == reach else (own_ref, near_ref.at[k - 1])
        return pltpu.make_async_remote_copy(
            src_ref=src.at[j], dst_ref=dst.at[j],
            send_sem=part_send.at[k - 1, j], recv_sem=part_recv.at[k - 1, j],
            device_id=slab_peer(ns - k), device_id_type=MESH)

    y_ids = lax.broadcasted_iota(jnp.int32, (ry, chunk), 0).astype(jnp.float32).astype(jnp.bfloat16)
    row_ids = lax.broadcasted_iota(jnp.int32, (rows, chunk), 0)

    for copy in loads[channels:channels + 3]:
        copy.wait()
    for j in range(chunks):
        at = pl.ds(j * chunk, chunk)
        pix = pix_ref[:, at]
        start = start_ref[:, at]
        px = pix // ry
        py = (pix - px * ry).astype(jnp.float32).astype(jnp.bfloat16)
        length = jnp.clip((start - slab) * depth + count_ref[:, at], 0, depth)
        length = jnp.where(slab >= start, length, 0)
        row = jnp.where(length > 0, (length - 1) * rx + px, -1)
        row_ref[:, at] = row
        hot = jnp.where(y_ids == py, jnp.ones((), jnp.bfloat16), jnp.zeros((), jnp.bfloat16))
        onehot_ref[:, at] = hot
        mask = row_ids == row
        u = jnp.dot(pair_ref[:, :ry], hot, preferred_element_type=jnp.float32)
        u = u + jnp.dot(pair_ref[:, ry:], hot, preferred_element_type=jnp.float32)
        for c in range(4):
            picked = jnp.where(mask, u[c * rows:(c + 1) * rows], 0.0)
            part = jnp.sum(picked, axis=0, keepdims=True)
            if c == 3:
                part = jnp.where(row < 0, 1.0, part)
            own_ref[j, pl.ds(c, 1), :] = part
        for c in range(3):
            last_ref[j, c] = own_ref[j, pl.ds(c, 1), :] + BACKGROUND * part
        for k in range(1, reach + 1):
            pl.when(slab >= k)(part_copy(k, j).start)

    for copy, _, receives in halos:
        pl.when(receives)(copy.wait_recv)
    x_ids = lax.broadcasted_iota(jnp.int32, (rx, ry), 0)
    lane_ids = lax.broadcasted_iota(jnp.int32, (rx, ry), 1)
    first_x = tile == 0
    last_x = tile == nt - 1
    for c in range(channels):
        for z in range(depth):
            g = grid_ref[c, z]
            if z > 0:
                below = grid_ref[c, z - 1]
            else:
                below = jnp.where(slab > 0, zhalo_ref[0, c], g)
            if z < depth - 1:
                above = grid_ref[c, z + 1]
            else:
                above = jnp.where(slab < ns - 1, zhalo_ref[1, c], g)
            xl = jnp.broadcast_to(xhalo_ref[0, c, pl.ds(z, 1), :], (rx, ry))
            xh = jnp.broadcast_to(xhalo_ref[1, c, pl.ds(z, 1), :], (rx, ry))
            xl = jnp.where(first_x, g, xl)
            xh = jnp.where(last_x, g, xh)
            left = jnp.where(x_ids == 0, xl, pltpu.roll(g, 1, 0))
            right = jnp.where(x_ids == rx - 1, xh, pltpu.roll(g, rx - 1, 0))
            down = jnp.where(lane_ids == 0, g, pltpu.roll(g, 1, 1))
            up = jnp.where(lane_ids == ry - 1, g, pltpu.roll(g, ry - 1, 1))
            smooth = (g - below) + (g - above) + (g - left) + (g - right) + (g - down) + (g - up)
            grad_ref[c, z] = (2.0 * TV_WEIGHT) * smooth

    for k in range(1, reach + 1):
        pl.when(slab >= k)(whole_copy(k).wait_recv)
    folded = [[] for _ in range(4)]
    fold_t = jnp.ones((rx, ry), jnp.float32)
    fold_c = [jnp.zeros((rx, ry), jnp.float32)] * 3
    for k in range(1, reach + 1):
        there = slab >= k
        t = wholes_ref[k - 1, 3]
        fold_c = [jnp.where(there, wholes_ref[k - 1, c] + t * fold_c[c], 0.0) for c in range(3)]
        fold_t = jnp.where(there, t * fold_t, 0.0)
        for c in range(4):
            folded[c].append(fold_c[c] if c < 3 else fold_t)
    folds = jnp.concatenate([f for fs in folded for f in fs], axis=0)
    fold_high = folds.astype(jnp.bfloat16)
    fold_low = (folds - fold_high.astype(jnp.float32)).astype(jnp.bfloat16)
    step_rows = reach * rx
    step_ids = lax.broadcasted_iota(jnp.int32, (step_rows, chunk), 0)
    for j in range(chunks):
        at = pl.ds(j * chunk, chunk)
        hot = onehot_ref[:, at]
        behind = slab - start_ref[:, at]
        mask = step_ids == (behind - 1) * rx + pix_ref[:, at] // ry
        u = jnp.dot(fold_high, hot, preferred_element_type=jnp.float32)
        u = u + jnp.dot(fold_low, hot, preferred_element_type=jnp.float32)
        for c in range(4):
            picked = jnp.where(mask, u[c * step_rows:(c + 1) * step_rows], 0.0)
            value = jnp.sum(picked, axis=0, keepdims=True)
            if c == 3:
                value = jnp.where(behind <= 0, 1.0, value)
            front_ref[j, pl.ds(c, 1), :] = value

    loads[channels + 3].wait()
    row_ids16 = row_ids.astype(jnp.float32).astype(jnp.bfloat16)
    for j in range(chunks):
        for k in range(1, reach + 1):
            pl.when(slab + k < ns)(part_copy(k, j).wait_recv)
        if j == 0 and direct(ns, nt):
            for k in (-reach, reach):
                @pl.when(inside(slab + k))
                def _(k=k):
                    pl.semaphore_signal(
                        ready_sem, inc=1, device_id={"slab": slab + k}, device_id_type=MESH)
        at = pl.ds(j * chunk, chunk)
        front_c = front_ref[j, pl.ds(0, 3), :]
        front_t = front_ref[j, pl.ds(3, 1), :]
        beyond = jnp.concatenate([far_ref[j, c] for c in range(3)], axis=0)
        beyond = jnp.where(slab + reach < ns, beyond, BACKGROUND)
        for k in range(reach - 1, 0, -1):
            pc = near_ref[k - 1, j, pl.ds(0, 3), :]
            pt = near_ref[k - 1, j, pl.ds(3, 1), :]
            beyond = jnp.where(slab + k < ns, pc + pt * beyond, beyond)
        pc = own_ref[j, pl.ds(0, 3), :]
        pt = own_ref[j, pl.ds(3, 1), :]
        rendered = front_c + front_t * (pc + pt * beyond)
        residual = RENDER_WEIGHT * (rendered - target_ref[:, at])
        color_cot = front_t * residual
        trans_cot = front_t * jnp.sum(residual * beyond, axis=0, keepdims=True)
        hot = onehot_ref[:, at]
        mask = row_ids16 == row_ref[:, at].astype(jnp.float32).astype(jnp.bfloat16)
        none = jnp.zeros((), jnp.bfloat16)
        tops = []
        lows = []
        for c in range(4):
            cot = color_cot[c:c + 1] if c < 3 else trans_cot
            top = cot.astype(jnp.bfloat16)
            low = (cot - top.astype(jnp.float32)).astype(jnp.bfloat16)
            tops.append(jnp.where(mask, top, none))
            lows.append(jnp.where(mask, low, none))
        u = sum(
            lax.dot_general(
                jnp.concatenate(spread, axis=0), hot, (((1,), (1,)), ((), ())),
                preferred_element_type=jnp.float32)
            for spread in (tops, lows))
        if j == 0:
            table_ref[...] = u
        else:
            table_ref[...] += u

    zero = jnp.zeros((rx, ry), jnp.float32)
    suffix = [zero, zero, zero]
    later = zero
    squares = zero
    for z in range(depth - 1, -1, -1):
        w = weight_ref[z]
        after = trans_ref[z]
        later = later + after * table_ref[pl.ds(3 * rows + z * rx, rx), :]
        dw = zero
        for c in range(3):
            suffix[c] = suffix[c] + table_ref[pl.ds(c * rows + z * rx, rx), :]
            col = sig_ref[c + 1, z]
            dw = dw + col * suffix[c]
            out = grad_ref[c + 1, z] + w * suffix[c] * (col * (1.0 - col))
            grad_ref[c + 1, z] = out
            squares = squares + out * out
        dtau = after * dw - later
        later = later + w * dw
        out = grad_ref[0, z] + dtau * (sig_ref[0, z] * span)
        grad_ref[0, z] = out
        squares = squares + out * out

    local = jnp.sum(squares)

    def norm_copy(phase, slot, peer):
        return pltpu.make_async_remote_copy(
            src_ref=nsend_ref.at[phase], dst_ref=nrecv_ref.at[slot],
            send_sem=norm_send.at[slot], recv_sem=norm_recv.at[slot],
            device_id=peer, device_id_type=MESH)

    if direct(ns, nt):
        far = inside(slab - reach).astype(jnp.int32) + inside(slab + reach).astype(jnp.int32)
        pl.semaphore_wait(ready_sem, far)
    value = jnp.full((1, 128), local, jnp.float32)
    copies = []
    base = 0
    for phase, peers in enumerate(phases):
        nsend_ref[phase] = value
        group = [norm_copy(phase, base + i, peer) for i, peer in enumerate(peers)]
        for copy in group:
            copy.start()
        for i, copy in enumerate(group):
            copy.wait_recv()
            value = value + nrecv_ref[base + i]
        base += len(group)
        copies += group
    limit = CLIP_RMS * math.sqrt(4.0 * total_depth * (rx * nt) * ry)
    scale_ref[...] = limit / jnp.maximum(jnp.sqrt(value), limit)
    for copy in loads[channels + 4:]:
        copy.wait()
    for copy in copies:
        copy.wait_send()
    for copy, sends, _ in halos:
        pl.when(sends)(copy.wait_send)
    for j in range(chunks):
        for k in range(1, reach + 1):
            pl.when(slab >= k)(part_copy(k, j).wait_send)
    for k in range(1, reach + 1):
        pl.when(slab + k < ns)(whole_copy(k).wait_send)


def span_reach(ns):
    return max(ns // 2, 1)


def direct(ns, nt):
    return ns * nt <= DIRECT_LIMIT and nt % 2 == 0


def adam_kernel(
    grid_ref, first_ref, second_ref, grad_ref, scale_ref,
    grid_hbm, first_hbm, second_hbm, grid_out, first_out, second_out, sem,
):
    channels, depth, rx, ry = grid_ref.shape
    scale = jnp.broadcast_to(scale_ref[0:1, 0:1], (rx, ry))
    copies = []
    for c in range(channels):
        for z in range(depth):
            clipped = grad_ref[c, z] * scale
            first = BETA_ONE * first_ref[c, z] + (1.0 - BETA_ONE) * clipped
            second = BETA_TWO * second_ref[c, z] + (1.0 - BETA_TWO) * clipped * clipped
            first_out[c, z] = first
            second_out[c, z] = second
            first_hat = first * (1.0 / (1.0 - BETA_ONE**STEP))
            second_hat = second * (1.0 / (1.0 - BETA_TWO**STEP))
            grid_out[c, z] = grid_ref[c, z] - LEARN_RATE * first_hat / (
                jnp.sqrt(second_hat) + EPSILON)
        pairs = ((first_out, first_hbm), (second_out, second_hbm), (grid_out, grid_hbm))
        for i, (a, b) in enumerate(pairs):
            copy = pltpu.make_async_copy(a.at[c], b.at[c], sem.at[i, c])
            copy.start()
            copies.append(copy)
    for copy in copies:
        copy.wait()


def per_device(voxel_grid, first_moment, second_moment, pixel_index, start_slab, ray_count, target):
    ns = lax.axis_size("slab")
    nt = lax.axis_size("tile")
    channels, depth, rx, ry = voxel_grid.shape
    rays = pixel_index.shape[0]
    chunk = math.gcd(rays, CHUNK)
    chunks = rays // chunk
    rows = depth * rx
    reach = span_reach(ns)
    messages = ns * nt // 2 if direct(ns, nt) else nt + ns - 2
    f32 = jnp.float32
    vmem = pl.BlockSpec(memory_space=pltpu.VMEM)
    hbm = pl.BlockSpec(memory_space=pltpu.HBM)
    cells = jax.ShapeDtypeStruct(voxel_grid.shape, f32)
    staged = pl.pallas_call(
        functools.partial(kernel, ns, nt, chunk),
        out_shape=(cells, cells, cells, cells, jax.ShapeDtypeStruct((1, 128), f32)),
        in_specs=[hbm] * 7,
        out_specs=(vmem,) * 5,
        scratch_shapes=[
            pltpu.VMEM((1, rays), jnp.int32),
            pltpu.VMEM((1, rays), jnp.int32),
            pltpu.VMEM((1, rays), jnp.int32),
            pltpu.VMEM(target.shape, f32),
            pltpu.VMEM((channels * rows, 2 * ry), jnp.bfloat16),
            pltpu.VMEM((depth, rx, ry), f32),
            pltpu.VMEM((depth, rx, ry), f32),
            pltpu.VMEM((channels, depth, rx, ry), f32),
            pltpu.VMEM((ry, rays), jnp.bfloat16),
            pltpu.VMEM((1, rays), jnp.int32),
            pltpu.VMEM((channels * rows, ry), f32),
            pltpu.VMEM((4, rx, ry), f32),
            pltpu.VMEM((reach, 4, rx, ry), f32),
            pltpu.VMEM((chunks, 4, chunk), f32),
            pltpu.VMEM((chunks, 4, chunk), f32),
            pltpu.VMEM((chunks, 3, 1, chunk), f32),
            pltpu.VMEM((max(reach - 1, 1), chunks, 4, chunk), f32),
            pltpu.VMEM((chunks, 3, 1, chunk), f32),
            pltpu.VMEM((2, channels, depth, ry), f32),
            pltpu.VMEM((2, channels, depth, ry), f32),
            pltpu.VMEM((2, channels, rx, ry), f32),
            pltpu.VMEM((2, 1, 128), f32),
            pltpu.VMEM((messages, 1, 128), f32),
            pltpu.SemaphoreType.DMA((reach,)),
            pltpu.SemaphoreType.DMA((reach,)),
            pltpu.SemaphoreType.DMA((reach, chunks)),
            pltpu.SemaphoreType.DMA((reach, chunks)),
            pltpu.SemaphoreType.REGULAR,
            pltpu.SemaphoreType.DMA((4,)),
            pltpu.SemaphoreType.DMA((4,)),
            pltpu.SemaphoreType.DMA((messages,)),
            pltpu.SemaphoreType.DMA((messages,)),
            pltpu.SemaphoreType.DMA((channels + 6,)),
        ],
        compiler_params=pltpu.CompilerParams(
            collective_id=0, has_side_effects=True, vmem_limit_bytes=32 * 1024 * 1024
        ),
        name="render_step",
    )(*(pltpu.with_memory_space_constraint(a, pltpu.HBM) for a in (
        voxel_grid,
        first_moment,
        second_moment,
        pixel_index.reshape(1, rays),
        start_slab.reshape(1, rays),
        ray_count.reshape(1, rays),
        target,
    )))
    return pl.pallas_call(
        adam_kernel,
        out_shape=(cells, cells, cells),
        in_specs=[vmem] * 5,
        out_specs=(hbm, hbm, hbm),
        scratch_shapes=[
            pltpu.VMEM(voxel_grid.shape, f32),
            pltpu.VMEM(voxel_grid.shape, f32),
            pltpu.VMEM(voxel_grid.shape, f32),
            pltpu.SemaphoreType.DMA((3, channels)),
        ],
        compiler_params=pltpu.CompilerParams(vmem_limit_bytes=32 * 1024 * 1024),
        name="adam",
    )(*staged)


def solution(mesh):
    cells = P(None, "slab", "tile", None)
    return jax.shard_map(
        per_device,
        mesh=mesh,
        in_specs=(cells, cells, cells, P("tile"), P("tile"), P("tile"), P(None, "tile")),
        out_specs=(cells, cells, cells),
        check_vma=False,
    )
```

```python
import functools
import math

import jax
import jax.numpy as jnp
from jax import lax
from jax.experimental import pallas as pl
from jax.experimental.pallas import tpu as pltpu
from jax.sharding import PartitionSpec as P

STEP = 20
RENDER_WEIGHT = 1000.0
TV_WEIGHT = 0.05
BACKGROUND = 1.0
STEP_SPAN = 4.0
CLIP_RMS = 0.25
LEARN_RATE = 0.02
BETA_ONE = 0.9
BETA_TWO = 0.99
EPSILON = 1e-08
CHUNK = 512
WIDTH = 256
DIRECT_LIMIT = 64
MESH = pl.DeviceIdType.MESH


def kernel(
    ns, nt, chunk,
    grid_hbm, first_hbm, second_hbm, pix_hbm, start_hbm, count_hbm, target_hbm,
    grid_ref, first_ref, second_ref, grad_ref, scale_ref,
    pix_ref, start_ref, count_ref, target_ref,
    pair_ref, trans_ref, weight_ref, sig_ref, onehot_ref, row_ref, table_ref,
    whole_ref, wholes_ref, front_ref, own_ref, last_ref, near_ref, far_ref,
    edge_ref, xhalo_ref, zhalo_ref, nsend_ref, nrecv_ref,
    whole_send, whole_recv, part_send, part_recv, ready_sem, halo_send, halo_recv, norm_send, norm_recv, load_sem,
):
    channels, depth, rx, ry = grid_ref.shape
    rays = pix_ref.shape[1]
    chunks = rays // chunk
    total_depth = depth * ns
    reach = span_reach(ns)
    span = STEP_SPAN / total_depth
    rows = depth * rx
    slab = lax.axis_index("slab")
    tile = lax.axis_index("tile")

    def slab_peer(d):
        return {"slab": lax.rem(slab + d, ns)}

    def tile_peer(d):
        return {"tile": lax.rem(tile + d, nt)}

    if direct(ns, nt):
        pair = {"tile": tile + 1 - 2 * lax.rem(tile, 2)}
        half = nt // 2
        others = [
            {"slab": lax.rem(slab + k // half, ns), "tile": lax.rem(tile + 2 * (k % half), nt)}
            for k in range(1, ns * half)
        ]
        phases = [[pair], others]
        near = reach
    else:
        phases = [[tile_peer(d) for d in range(1, nt)], [slab_peer(d) for d in range(1, ns)]]
        near = ns - 1
    offsets = [k for k in range(-near, near + 1) if k]

    def inside(s):
        return (s >= 0) & (s < ns)

    loads = [
        pltpu.make_async_copy(grid_hbm.at[c], grid_ref.at[c], load_sem.at[c])
        for c in range(channels)
    ]
    rest = (
        (pix_hbm, pix_ref), (start_hbm, start_ref), (count_hbm, count_ref),
        (target_hbm, target_ref), (first_hbm, first_ref), (second_hbm, second_ref),
    )
    loads += [
        pltpu.make_async_copy(a, b, load_sem.at[channels + i]) for i, (a, b) in enumerate(rest)
    ]
    for copy in loads:
        copy.start()

    barrier = pltpu.get_barrier_semaphore()
    for d in range(1, nt):
        pl.semaphore_signal(barrier, inc=1, device_id=tile_peer(d), device_id_type=MESH)
    greeters = nt - 1
    for k in offsets:
        @pl.when(inside(slab + k))
        def _(k=k):
            pl.semaphore_signal(
                barrier, inc=1, device_id={"slab": slab + k}, device_id_type=MESH)
        greeters = greeters + inside(slab + k).astype(jnp.int32)

    for c in range(channels):
        loads[c].wait()
    edge_ref[0] = grid_ref[:, :, rx - 1, :]
    edge_ref[1] = grid_ref[:, :, 0, :]

    total = jnp.zeros((rx, ry), jnp.float32)
    before = jnp.ones((rx, ry), jnp.float32)
    sums = [jnp.zeros((rx, ry), jnp.float32) for _ in range(3)]
    for z in range(depth):
        s = grid_ref[0, z]
        e = jnp.exp(-jnp.abs(s))
        tau = (jnp.maximum(s, 0.0) + jnp.log1p(e)) * span
        sig_ref[0, z] = jnp.where(s >= 0, 1.0, e) / (1.0 + e)
        total = total + tau
        after = jnp.exp(-total)
        w = before * (1.0 - jnp.exp(-tau))
        before = after
        trans_ref[z] = after
        weight_ref[z] = w
        for c in range(3):
            col = 1.0 / (1.0 + jnp.exp(-grid_ref[c + 1, z]))
            sig_ref[c + 1, z] = col
            sums[c] = sums[c] + w * col
            table_ref[pl.ds(c * rows + z * rx, rx), :] = sums[c]
        table_ref[pl.ds(3 * rows + z * rx, rx), :] = after
    for c in range(3):
        whole_ref[c] = sums[c]
    whole_ref[3] = before
    full = table_ref[...]
    high = full.astype(jnp.bfloat16)
    pair_ref[:, :ry] = high
    pair_ref[:, ry:] = (full - high.astype(jnp.float32)).astype(jnp.bfloat16)

    pl.semaphore_wait(barrier, greeters)

    def whole_copy(k):
        return pltpu.make_async_remote_copy(
            src_ref=whole_ref, dst_ref=wholes_ref.at[k - 1],
            send_sem=whole_send.at[k - 1], recv_sem=whole_recv.at[k - 1],
            device_id=slab_peer(k), device_id_type=MESH)

    for k in range(reach, 0, -1):
        pl.when(slab + k < ns)(whole_copy(k).start)

    def halo_copy(src, dst, i, peer):
        return pltpu.make_async_remote_copy(
            src_ref=src, dst_ref=dst, send_sem=halo_send.at[i], recv_sem=halo_recv.at[i],
            device_id=peer, device_id_type=MESH)

    halos = [
        (halo_copy(grid_ref.at[:, depth - 1], zhalo_ref.at[0], 0, slab_peer(1)), slab < ns - 1, slab > 0),
        (halo_copy(grid_ref.at[:, 0], zhalo_ref.at[1], 1, slab_peer(ns - 1)), slab > 0, slab < ns - 1),
        (halo_copy(edge_ref.at[0], xhalo_ref.at[0], 2, tile_peer(1)), tile < nt - 1, tile > 0),
        (halo_copy(edge_ref.at[1], xhalo_ref.at[1], 3, tile_peer(nt - 1)), tile > 0, tile < nt - 1),
    ]
    for copy, sends, _ in halos:
        pl.when(sends)(copy.start)

    def part_copy(k, j):
        src, dst = (last_ref, far_ref) if k == reach else (own_ref, near_ref.at[k - 1])
        return pltpu.make_async_remote_copy(
            src_ref=src.at[j], dst_ref=dst.at[j],
            send_sem=part_send.at[k - 1, j], recv_sem=part_recv.at[k - 1, j],
            device_id=slab_peer(ns - k), device_id_type=MESH)

    y_ids = lax.broadcasted_iota(jnp.int32, (ry, chunk), 0).astype(jnp.float32).astype(jnp.bfloat16)
    row_ids = lax.broadcasted_iota(jnp.int32, (rows, chunk), 0)

    for copy in loads[channels:channels + 3]:
        copy.wait()
    units = range(chunk // WIDTH)

    def gather(*accs):
        banks = [[accs[(b * len(units) + q) * 4:][:4] for q in units] for b in range(2)]
        for j in range(chunks + 1):
            if j < chunks:
                at = pl.ds(j * chunk, chunk)
                pix = pix_ref[:, at]
                start = start_ref[:, at]
                px = pix // ry
                py = (pix - px * ry).astype(jnp.float32).astype(jnp.bfloat16)
                length = jnp.clip((start - slab) * depth + count_ref[:, at], 0, depth)
                length = jnp.where(slab >= start, length, 0)
                row_ref[:, at] = jnp.where(length > 0, (length - 1) * rx + px, -1)
                hot = jnp.where(y_ids == py, jnp.ones((), jnp.bfloat16), jnp.zeros((), jnp.bfloat16))
                onehot_ref[:, at] = hot
                for q in units:
                    pltpu.matmul_push_rhs(hot[:, q * WIDTH:(q + 1) * WIDTH], j % 2, q)
                for c in range(4):
                    block = pl.ds(c * rows, rows)
                    for half in range(2):
                        lhs = pair_ref[block, half * ry:(half + 1) * ry]
                        for q in units:
                            fresh = j % 2 if c == 0 and half == 0 else None
                            pltpu.matmul_acc_lhs(banks[j % 2][q][c], lhs, fresh)
            if j == 0:
                continue
            i = j - 1
            row = row_ref[:, pl.ds(i * chunk, chunk)]
            mask = row_ids == row
            for c in range(4):
                u = jnp.concatenate([pltpu.matmul_pop(banks[i % 2][q][c]) for q in units], axis=1)
                part = jnp.sum(jnp.where(mask, u, 0.0), axis=0, keepdims=True)
                if c == 3:
                    part = jnp.where(row < 0, 1.0, part)
                own_ref[i, pl.ds(c, 1), :] = part
            for c in range(3):
                last_ref[i, c] = own_ref[i, pl.ds(c, 1), :] + BACKGROUND * part
            for k in range(1, reach + 1):
                pl.when(slab >= k)(part_copy(k, i).start)

    pl.run_scoped(gather, *[
        pltpu.ACC(q)((rows, WIDTH), jnp.float32)
        for _ in range(2) for q in units for _ in range(4)
    ])

    for copy, _, receives in halos:
        pl.when(receives)(copy.wait_recv)
    x_ids = lax.broadcasted_iota(jnp.int32, (rx, ry), 0)
    lane_ids = lax.broadcasted_iota(jnp.int32, (rx, ry), 1)
    first_x = tile == 0
    last_x = tile == nt - 1
    for c in range(channels):
        for z in range(depth):
            g = grid_ref[c, z]
            if z > 0:
                below = grid_ref[c, z - 1]
            else:
                below = jnp.where(slab > 0, zhalo_ref[0, c], g)
            if z < depth - 1:
                above = grid_ref[c, z + 1]
            else:
                above = jnp.where(slab < ns - 1, zhalo_ref[1, c], g)
            xl = jnp.broadcast_to(xhalo_ref[0, c, pl.ds(z, 1), :], (rx, ry))
            xh = jnp.broadcast_to(xhalo_ref[1, c, pl.ds(z, 1), :], (rx, ry))
            xl = jnp.where(first_x, g, xl)
            xh = jnp.where(last_x, g, xh)
            left = jnp.where(x_ids == 0, xl, pltpu.roll(g, 1, 0))
            right = jnp.where(x_ids == rx - 1, xh, pltpu.roll(g, rx - 1, 0))
            down = jnp.where(lane_ids == 0, g, pltpu.roll(g, 1, 1))
            up = jnp.where(lane_ids == ry - 1, g, pltpu.roll(g, ry - 1, 1))
            smooth = (g - below) + (g - above) + (g - left) + (g - right) + (g - down) + (g - up)
            grad_ref[c, z] = (2.0 * TV_WEIGHT) * smooth

    for k in range(1, reach + 1):
        pl.when(slab >= k)(whole_copy(k).wait_recv)
    folded = [[] for _ in range(4)]
    fold_t = jnp.ones((rx, ry), jnp.float32)
    fold_c = [jnp.zeros((rx, ry), jnp.float32)] * 3
    for k in range(1, reach + 1):
        there = slab >= k
        t = wholes_ref[k - 1, 3]
        fold_c = [jnp.where(there, wholes_ref[k - 1, c] + t * fold_c[c], 0.0) for c in range(3)]
        fold_t = jnp.where(there, t * fold_t, 0.0)
        for c in range(4):
            folded[c].append(fold_c[c] if c < 3 else fold_t)
    folds = jnp.concatenate([f for fs in folded for f in fs], axis=0)
    fold_high = folds.astype(jnp.bfloat16)
    fold_low = (folds - fold_high.astype(jnp.float32)).astype(jnp.bfloat16)
    step_rows = reach * rx
    step_ids = lax.broadcasted_iota(jnp.int32, (step_rows, chunk), 0)
    row_ids16 = row_ids.astype(jnp.float32).astype(jnp.bfloat16)
    none = jnp.zeros((), jnp.bfloat16)
    lags = 4

    def scatter(*accs):
        sums_acc = [accs[q * 4:][:4] for q in units]
        accs = accs[4 * len(units):]
        steps = [[accs[b * len(units) + q] for q in units] for b in range(lags)]

        def columns(j, q):
            return onehot_ref[:, pl.ds(j * chunk + q * WIDTH, WIDTH)]

        for j in range(chunks):
            at = pl.ds(j * chunk, chunk)
            for q in units:
                pltpu.matmul_push_rhs(columns(j, q), j % 2, q)
            for half, lhs in enumerate((fold_high, fold_low)):
                for q in units:
                    pltpu.matmul_acc_lhs(steps[j % lags][q], lhs, None if half else j % 2)
            behind = slab - start_ref[:, at]
            mask = step_ids == (behind - 1) * rx + pix_ref[:, at] // ry
            u = jnp.concatenate([pltpu.matmul_pop(steps[j % lags][q]) for q in units], axis=1)
            for c in range(4):
                picked = jnp.where(mask, u[c * step_rows:(c + 1) * step_rows], 0.0)
                value = jnp.sum(picked, axis=0, keepdims=True)
                if c == 3:
                    value = jnp.where(behind <= 0, 1.0, value)
                front_ref[j, pl.ds(c, 1), :] = value

        loads[channels + 3].wait()
        for q in units:
            pltpu.matmul_push_rhs(columns(0, q), 0, q, transpose=True)
        for j in range(chunks):
            for k in range(1, reach + 1):
                pl.when(slab + k < ns)(part_copy(k, j).wait_recv)
            if j == 0 and direct(ns, nt):
                for k in (-reach, reach):
                    @pl.when(inside(slab + k))
                    def _(k=k):
                        pl.semaphore_signal(
                            ready_sem, inc=1, device_id={"slab": slab + k}, device_id_type=MESH)
            at = pl.ds(j * chunk, chunk)
            front_c = front_ref[j, pl.ds(0, 3), :]
            front_t = front_ref[j, pl.ds(3, 1), :]
            beyond = jnp.concatenate([far_ref[j, c] for c in range(3)], axis=0)
            beyond = jnp.where(slab + reach < ns, beyond, BACKGROUND)
            for k in range(reach - 1, 0, -1):
                pc = near_ref[k - 1, j, pl.ds(0, 3), :]
                pt = near_ref[k - 1, j, pl.ds(3, 1), :]
                beyond = jnp.where(slab + k < ns, pc + pt * beyond, beyond)
            pc = own_ref[j, pl.ds(0, 3), :]
            pt = own_ref[j, pl.ds(3, 1), :]
            rendered = front_c + front_t * (pc + pt * beyond)
            residual = RENDER_WEIGHT * (rendered - target_ref[:, at])
            color_cot = front_t * residual
            trans_cot = front_t * jnp.sum(residual * beyond, axis=0, keepdims=True)
            mask = row_ids16 == row_ref[:, at].astype(jnp.float32).astype(jnp.bfloat16)
            for c in range(4):
                cot = color_cot[c:c + 1] if c < 3 else trans_cot
                top = cot.astype(jnp.bfloat16)
                low = (cot - top.astype(jnp.float32)).astype(jnp.bfloat16)
                for half, part in enumerate((top, low)):
                    spread = jnp.where(mask, part, none)
                    for q in units:
                        fresh = j % 2 if c == 0 and half == 0 else None
                        pltpu.matmul_acc_lhs(
                            sums_acc[q][c], spread[:, q * WIDTH:(q + 1) * WIDTH], fresh)
            if j + 1 < chunks:
                for q in units:
                    pltpu.matmul_push_rhs(columns(j + 1, q), (j + 1) % 2, q, transpose=True)
        for c in range(4):
            table_ref[pl.ds(c * rows, rows), :] = sum(pltpu.matmul_pop(sums_acc[q][c]) for q in units)

    pl.run_scoped(scatter, *[
        pltpu.ACC(q)((rows, WIDTH), jnp.float32) for q in units for _ in range(4)
    ], *[
        pltpu.ACC(q)((4 * step_rows, WIDTH), jnp.float32) for _ in range(lags) for q in units
    ])

    zero = jnp.zeros((rx, ry), jnp.float32)
    suffix = [zero, zero, zero]
    later = zero
    squares = zero
    for z in range(depth - 1, -1, -1):
        w = weight_ref[z]
        after = trans_ref[z]
        later = later + after * table_ref[pl.ds(3 * rows + z * rx, rx), :]
        dw = zero
        for c in range(3):
            suffix[c] = suffix[c] + table_ref[pl.ds(c * rows + z * rx, rx), :]
            col = sig_ref[c + 1, z]
            dw = dw + col * suffix[c]
            out = grad_ref[c + 1, z] + w * suffix[c] * (col * (1.0 - col))
            grad_ref[c + 1, z] = out
            squares = squares + out * out
        dtau = after * dw - later
        later = later + w * dw
        out = grad_ref[0, z] + dtau * (sig_ref[0, z] * span)
        grad_ref[0, z] = out
        squares = squares + out * out

    local = jnp.sum(squares)

    def norm_copy(phase, slot, peer):
        return pltpu.make_async_remote_copy(
            src_ref=nsend_ref.at[phase], dst_ref=nrecv_ref.at[slot],
            send_sem=norm_send.at[slot], recv_sem=norm_recv.at[slot],
            device_id=peer, device_id_type=MESH)

    if direct(ns, nt):
        far = inside(slab - reach).astype(jnp.int32) + inside(slab + reach).astype(jnp.int32)
        pl.semaphore_wait(ready_sem, far)
    value = jnp.full((1, 128), local, jnp.float32)
    copies = []
    base = 0
    for phase, peers in enumerate(phases):
        nsend_ref[phase] = value
        group = [norm_copy(phase, base + i, peer) for i, peer in enumerate(peers)]
        for copy in group:
            copy.start()
        for i, copy in enumerate(group):
            copy.wait_recv()
            value = value + nrecv_ref[base + i]
        base += len(group)
        copies += group
    limit = CLIP_RMS * math.sqrt(4.0 * total_depth * (rx * nt) * ry)
    scale_ref[...] = limit / jnp.maximum(jnp.sqrt(value), limit)
    for copy in loads[channels + 4:]:
        copy.wait()
    for copy in copies:
        copy.wait_send()
    for copy, sends, _ in halos:
        pl.when(sends)(copy.wait_send)
    for j in range(chunks):
        for k in range(1, reach + 1):
            pl.when(slab >= k)(part_copy(k, j).wait_send)
    for k in range(1, reach + 1):
        pl.when(slab + k < ns)(whole_copy(k).wait_send)


def span_reach(ns):
    return max(ns // 2, 1)


def direct(ns, nt):
    return ns * nt <= DIRECT_LIMIT and nt % 2 == 0


def adam_kernel(
    grid_ref, first_ref, second_ref, grad_ref, scale_ref,
    grid_hbm, first_hbm, second_hbm, grid_out, first_out, second_out, sem,
):
    channels, depth, rx, ry = grid_ref.shape
    scale = jnp.broadcast_to(scale_ref[0:1, 0:1], (rx, ry))
    copies = []
    for c in range(channels):
        for z in range(depth):
            clipped = grad_ref[c, z] * scale
            first = BETA_ONE * first_ref[c, z] + (1.0 - BETA_ONE) * clipped
            second = BETA_TWO * second_ref[c, z] + (1.0 - BETA_TWO) * clipped * clipped
            first_out[c, z] = first
            second_out[c, z] = second
            first_hat = first * (1.0 / (1.0 - BETA_ONE**STEP))
            second_hat = second * (1.0 / (1.0 - BETA_TWO**STEP))
            grid_out[c, z] = grid_ref[c, z] - LEARN_RATE * first_hat / (
                jnp.sqrt(second_hat) + EPSILON)
        pairs = ((first_out, first_hbm), (second_out, second_hbm), (grid_out, grid_hbm))
        for i, (a, b) in enumerate(pairs):
            copy = pltpu.make_async_copy(a.at[c], b.at[c], sem.at[i, c])
            copy.start()
            copies.append(copy)
    for copy in copies:
        copy.wait()


def per_device(voxel_grid, first_moment, second_moment, pixel_index, start_slab, ray_count, target):
    ns = lax.axis_size("slab")
    nt = lax.axis_size("tile")
    channels, depth, rx, ry = voxel_grid.shape
    rays = pixel_index.shape[0]
    chunk = math.gcd(rays, CHUNK)
    chunks = rays // chunk
    rows = depth * rx
    reach = span_reach(ns)
    messages = ns * nt // 2 if direct(ns, nt) else nt + ns - 2
    f32 = jnp.float32
    vmem = pl.BlockSpec(memory_space=pltpu.VMEM)
    hbm = pl.BlockSpec(memory_space=pltpu.HBM)
    cells = jax.ShapeDtypeStruct(voxel_grid.shape, f32)
    staged = pl.pallas_call(
        functools.partial(kernel, ns, nt, chunk),
        out_shape=(cells, cells, cells, cells, jax.ShapeDtypeStruct((1, 128), f32)),
        in_specs=[hbm] * 7,
        out_specs=(vmem,) * 5,
        scratch_shapes=[
            pltpu.VMEM((1, rays), jnp.int32),
            pltpu.VMEM((1, rays), jnp.int32),
            pltpu.VMEM((1, rays), jnp.int32),
            pltpu.VMEM(target.shape, f32),
            pltpu.VMEM((channels * rows, 2 * ry), jnp.bfloat16),
            pltpu.VMEM((depth, rx, ry), f32),
            pltpu.VMEM((depth, rx, ry), f32),
            pltpu.VMEM((channels, depth, rx, ry), f32),
            pltpu.VMEM((ry, rays), jnp.bfloat16),
            pltpu.VMEM((1, rays), jnp.int32),
            pltpu.VMEM((channels * rows, ry), f32),
            pltpu.VMEM((4, rx, ry), f32),
            pltpu.VMEM((reach, 4, rx, ry), f32),
            pltpu.VMEM((chunks, 4, chunk), f32),
            pltpu.VMEM((chunks, 4, chunk), f32),
            pltpu.VMEM((chunks, 3, 1, chunk), f32),
            pltpu.VMEM((max(reach - 1, 1), chunks, 4, chunk), f32),
            pltpu.VMEM((chunks, 3, 1, chunk), f32),
            pltpu.VMEM((2, channels, depth, ry), f32),
            pltpu.VMEM((2, channels, depth, ry), f32),
            pltpu.VMEM((2, channels, rx, ry), f32),
            pltpu.VMEM((2, 1, 128), f32),
            pltpu.VMEM((messages, 1, 128), f32),
            pltpu.SemaphoreType.DMA((reach,)),
            pltpu.SemaphoreType.DMA((reach,)),
            pltpu.SemaphoreType.DMA((reach, chunks)),
            pltpu.SemaphoreType.DMA((reach, chunks)),
            pltpu.SemaphoreType.REGULAR,
            pltpu.SemaphoreType.DMA((4,)),
            pltpu.SemaphoreType.DMA((4,)),
            pltpu.SemaphoreType.DMA((messages,)),
            pltpu.SemaphoreType.DMA((messages,)),
            pltpu.SemaphoreType.DMA((channels + 6,)),
        ],
        compiler_params=pltpu.CompilerParams(
            collective_id=0, has_side_effects=True, vmem_limit_bytes=32 * 1024 * 1024
        ),
        name="render_step",
    )(*(pltpu.with_memory_space_constraint(a, pltpu.HBM) for a in (
        voxel_grid,
        first_moment,
        second_moment,
        pixel_index.reshape(1, rays),
        start_slab.reshape(1, rays),
        ray_count.reshape(1, rays),
        target,
    )))
    return pl.pallas_call(
        adam_kernel,
        out_shape=(cells, cells, cells),
        in_specs=[vmem] * 5,
        out_specs=(hbm, hbm, hbm),
        scratch_shapes=[
            pltpu.VMEM(voxel_grid.shape, f32),
            pltpu.VMEM(voxel_grid.shape, f32),
            pltpu.VMEM(voxel_grid.shape, f32),
            pltpu.SemaphoreType.DMA((3, channels)),
        ],
        compiler_params=pltpu.CompilerParams(vmem_limit_bytes=32 * 1024 * 1024),
        name="adam",
    )(*staged)


def solution(mesh):
    cells = P(None, "slab", "tile", None)
    return jax.shard_map(
        per_device,
        mesh=mesh,
        in_specs=(cells, cells, cells, P("tile"), P("tile"), P("tile"), P(None, "tile")),
        out_specs=(cells, cells, cells),
        check_vma=False,
    )
```

```python
import functools
import math

import jax
import jax.numpy as jnp
from jax import lax
from jax.experimental import pallas as pl
from jax.experimental.pallas import tpu as pltpu
from jax.sharding import PartitionSpec as P

STEP = 20
RENDER_WEIGHT = 1000.0
TV_WEIGHT = 0.05
BACKGROUND = 1.0
STEP_SPAN = 4.0
CLIP_RMS = 0.25
LEARN_RATE = 0.02
BETA_ONE = 0.9
BETA_TWO = 0.99
EPSILON = 1e-08
CHUNK = 512
WIDTH = 256
OPENING = 4
DIRECT_LIMIT = 64
MESH = pl.DeviceIdType.MESH


def kernel(
    ns, nt, chunk,
    grid_hbm, first_hbm, second_hbm, pix_hbm, start_hbm, count_hbm, target_hbm,
    grid_ref, first_ref, second_ref, grad_ref, scale_ref,
    pix_ref, start_ref, count_ref, target_ref,
    pair_ref, trans_ref, weight_ref, sig_ref, onehot_ref, row_ref, table_ref,
    whole_ref, wholes_ref, front_ref, own_ref, last_ref, near_ref, far_ref,
    edge_ref, xhalo_ref, zhalo_ref, nsend_ref, nrecv_ref,
    whole_send, whole_recv, part_send, part_recv, ready_sem, halo_send, halo_recv, norm_send, norm_recv, load_sem,
):
    channels, depth, rx, ry = grid_ref.shape
    rays = pix_ref.shape[1]
    chunks = rays // chunk
    total_depth = depth * ns
    reach = span_reach(ns)
    span = STEP_SPAN / total_depth
    rows = depth * rx
    slab = lax.axis_index("slab")
    tile = lax.axis_index("tile")

    def slab_peer(d):
        return {"slab": lax.rem(slab + d, ns)}

    def tile_peer(d):
        return {"tile": lax.rem(tile + d, nt)}

    if direct(ns, nt):
        pair = {"tile": tile + 1 - 2 * lax.rem(tile, 2)}
        half = nt // 2
        others = [
            {"slab": lax.rem(slab + k // half, ns), "tile": lax.rem(tile + 2 * (k % half), nt)}
            for k in range(1, ns * half)
        ]
        phases = [[pair], others]
        near = reach
    else:
        phases = [[tile_peer(d) for d in range(1, nt)], [slab_peer(d) for d in range(1, ns)]]
        near = ns - 1
    offsets = [k for k in range(-near, near + 1) if k]

    def inside(s):
        return (s >= 0) & (s < ns)

    loads = [
        pltpu.make_async_copy(grid_hbm.at[c], grid_ref.at[c], load_sem.at[c])
        for c in range(channels)
    ]
    rest = (
        (pix_hbm, pix_ref), (start_hbm, start_ref), (count_hbm, count_ref),
        (target_hbm, target_ref), (first_hbm, first_ref), (second_hbm, second_ref),
    )
    loads += [
        pltpu.make_async_copy(a, b, load_sem.at[channels + i]) for i, (a, b) in enumerate(rest)
    ]
    for copy in loads[:-2]:
        copy.start()

    barrier = pltpu.get_barrier_semaphore()
    for d in range(1, nt):
        pl.semaphore_signal(barrier, inc=1, device_id=tile_peer(d), device_id_type=MESH)
    greeters = nt - 1
    for k in offsets:
        @pl.when(inside(slab + k))
        def _(k=k):
            pl.semaphore_signal(
                barrier, inc=1, device_id={"slab": slab + k}, device_id_type=MESH)
        greeters = greeters + inside(slab + k).astype(jnp.int32)

    for c in range(channels):
        loads[c].wait()
    for copy in loads[-2:]:
        copy.start()
    edge_ref[0] = grid_ref[:, :, rx - 1, :]
    edge_ref[1] = grid_ref[:, :, 0, :]

    total = jnp.zeros((rx, ry), jnp.float32)
    before = jnp.ones((rx, ry), jnp.float32)
    sums = [jnp.zeros((rx, ry), jnp.float32) for _ in range(3)]
    for z in range(depth):
        s = grid_ref[0, z]
        e = jnp.exp(-jnp.abs(s))
        tau = (jnp.maximum(s, 0.0) + jnp.log1p(e)) * span
        sig_ref[0, z] = jnp.where(s >= 0, 1.0, e) / (1.0 + e)
        total = total + tau
        after = jnp.exp(-total)
        w = before * (1.0 - jnp.exp(-tau))
        before = after
        trans_ref[z] = after
        weight_ref[z] = w
        for c in range(3):
            col = 1.0 / (1.0 + jnp.exp(-grid_ref[c + 1, z]))
            sig_ref[c + 1, z] = col
            sums[c] = sums[c] + w * col
            table_ref[pl.ds(c * rows + z * rx, rx), :] = sums[c]
        table_ref[pl.ds(3 * rows + z * rx, rx), :] = after
    for c in range(3):
        whole_ref[c] = sums[c]
    whole_ref[3] = before
    full = table_ref[...]
    high = full.astype(jnp.bfloat16)
    pair_ref[:, :ry] = high
    pair_ref[:, ry:] = (full - high.astype(jnp.float32)).astype(jnp.bfloat16)

    def whole_copy(k):
        return pltpu.make_async_remote_copy(
            src_ref=whole_ref, dst_ref=wholes_ref.at[k - 1],
            send_sem=whole_send.at[k - 1], recv_sem=whole_recv.at[k - 1],
            device_id=slab_peer(k), device_id_type=MESH)

    def halo_copy(src, dst, i, peer):
        return pltpu.make_async_remote_copy(
            src_ref=src, dst_ref=dst, send_sem=halo_send.at[i], recv_sem=halo_recv.at[i],
            device_id=peer, device_id_type=MESH)

    halos = [
        (halo_copy(grid_ref.at[:, depth - 1], zhalo_ref.at[0], 0, slab_peer(1)), slab < ns - 1, slab > 0),
        (halo_copy(grid_ref.at[:, 0], zhalo_ref.at[1], 1, slab_peer(ns - 1)), slab > 0, slab < ns - 1),
        (halo_copy(edge_ref.at[0], xhalo_ref.at[0], 2, tile_peer(1)), tile < nt - 1, tile > 0),
        (halo_copy(edge_ref.at[1], xhalo_ref.at[1], 3, tile_peer(nt - 1)), tile > 0, tile < nt - 1),
    ]
    def part_copy(k, j):
        src, dst = (last_ref, far_ref) if k == reach else (own_ref, near_ref.at[k - 1])
        return pltpu.make_async_remote_copy(
            src_ref=src.at[j], dst_ref=dst.at[j],
            send_sem=part_send.at[k - 1, j], recv_sem=part_recv.at[k - 1, j],
            device_id=slab_peer(ns - k), device_id_type=MESH)

    y_ids = lax.broadcasted_iota(jnp.int32, (ry, chunk), 0).astype(jnp.float32).astype(jnp.bfloat16)
    row_ids = lax.broadcasted_iota(jnp.int32, (rows, chunk), 0)

    for copy in loads[channels:channels + 3]:
        copy.wait()
    units = range(chunk // WIDTH)

    def enter():
        pl.semaphore_wait(barrier, greeters)
        for k in range(reach, 0, -1):
            pl.when(slab + k < ns)(whole_copy(k).start)
        for copy, sends, _ in halos[2:]:
            pl.when(sends)(copy.start)

    opening = min(OPENING, chunks)

    def gather(*accs):
        banks = [[accs[(b * len(units) + q) * 4:][:4] for q in units] for b in range(2)]
        for j in range(chunks + 1):
            if j < chunks:
                at = pl.ds(j * chunk, chunk)
                pix = pix_ref[:, at]
                start = start_ref[:, at]
                px = pix // ry
                py = (pix - px * ry).astype(jnp.float32).astype(jnp.bfloat16)
                length = jnp.clip((start - slab) * depth + count_ref[:, at], 0, depth)
                length = jnp.where(slab >= start, length, 0)
                row_ref[:, at] = jnp.where(length > 0, (length - 1) * rx + px, -1)
                hot = jnp.where(y_ids == py, jnp.ones((), jnp.bfloat16), jnp.zeros((), jnp.bfloat16))
                onehot_ref[:, at] = hot
                for q in units:
                    pltpu.matmul_push_rhs(hot[:, q * WIDTH:(q + 1) * WIDTH], j % 2, q)
                for c in range(4):
                    block = pl.ds(c * rows, rows)
                    for half in range(2):
                        lhs = pair_ref[block, half * ry:(half + 1) * ry]
                        for q in units:
                            fresh = j % 2 if c == 0 and half == 0 else None
                            pltpu.matmul_acc_lhs(banks[j % 2][q][c], lhs, fresh)
            if j == 0:
                continue
            i = j - 1
            row = row_ref[:, pl.ds(i * chunk, chunk)]
            mask = row_ids == row
            for c in range(4):
                u = jnp.concatenate([pltpu.matmul_pop(banks[i % 2][q][c]) for q in units], axis=1)
                part = jnp.sum(jnp.where(mask, u, 0.0), axis=0, keepdims=True)
                if c == 3:
                    part = jnp.where(row < 0, 1.0, part)
                own_ref[i, pl.ds(c, 1), :] = part
            for c in range(3):
                last_ref[i, c] = own_ref[i, pl.ds(c, 1), :] + BACKGROUND * part
            if j < opening:
                continue
            if j == opening:
                enter()
            for n in range(0 if j == opening else i, j):
                for k in range(1, reach + 1):
                    pl.when(slab >= k)(part_copy(k, n).start)

    pl.run_scoped(gather, *[
        pltpu.ACC(q)((rows, WIDTH), jnp.float32)
        for _ in range(2) for q in units for _ in range(4)
    ])

    for copy, sends, _ in halos[:2]:
        pl.when(sends)(copy.start)
    x_ids = lax.broadcasted_iota(jnp.int32, (rx, ry), 0)
    lane_ids = lax.broadcasted_iota(jnp.int32, (rx, ry), 1)
    first_x = tile == 0
    last_x = tile == nt - 1
    def smooth_planes(c, planes):
        for z in planes:
            g = grid_ref[c, z]
            if z > 0:
                below = grid_ref[c, z - 1]
            else:
                below = jnp.where(slab > 0, zhalo_ref[0, c], g)
            if z < depth - 1:
                above = grid_ref[c, z + 1]
            else:
                above = jnp.where(slab < ns - 1, zhalo_ref[1, c], g)
            xl = jnp.broadcast_to(xhalo_ref[0, c, pl.ds(z, 1), :], (rx, ry))
            xh = jnp.broadcast_to(xhalo_ref[1, c, pl.ds(z, 1), :], (rx, ry))
            xl = jnp.where(first_x, g, xl)
            xh = jnp.where(last_x, g, xh)
            left = jnp.where(x_ids == 0, xl, pltpu.roll(g, 1, 0))
            right = jnp.where(x_ids == rx - 1, xh, pltpu.roll(g, rx - 1, 0))
            down = jnp.where(lane_ids == 0, g, pltpu.roll(g, 1, 1))
            up = jnp.where(lane_ids == ry - 1, g, pltpu.roll(g, ry - 1, 1))
            smooth = (g - below) + (g - above) + (g - left) + (g - right) + (g - down) + (g - up)
            grad_ref[c, z] = (2.0 * TV_WEIGHT) * smooth

    for k in range(1, reach + 1):
        pl.when(slab >= k)(whole_copy(k).wait_recv)
    folded = [[] for _ in range(4)]
    fold_t = jnp.ones((rx, ry), jnp.float32)
    fold_c = [jnp.zeros((rx, ry), jnp.float32)] * 3
    for k in range(1, reach + 1):
        there = slab >= k
        t = wholes_ref[k - 1, 3]
        fold_c = [jnp.where(there, wholes_ref[k - 1, c] + t * fold_c[c], 0.0) for c in range(3)]
        fold_t = jnp.where(there, t * fold_t, 0.0)
        for c in range(4):
            folded[c].append(fold_c[c] if c < 3 else fold_t)
    folds = jnp.concatenate([f for fs in folded for f in fs], axis=0)
    fold_high = folds.astype(jnp.bfloat16)
    fold_low = (folds - fold_high.astype(jnp.float32)).astype(jnp.bfloat16)
    step_rows = reach * rx
    step_ids = lax.broadcasted_iota(jnp.int32, (step_rows, chunk), 0)
    row_ids16 = row_ids.astype(jnp.float32).astype(jnp.bfloat16)
    none = jnp.zeros((), jnp.bfloat16)
    lags = 4
    inner = min(channels, chunks)

    def scatter(*accs):
        sums_acc = [accs[q * 4:][:4] for q in units]
        accs = accs[4 * len(units):]
        steps = [[accs[b * len(units) + q] for q in units] for b in range(lags)]

        def columns(j, q):
            return onehot_ref[:, pl.ds(j * chunk + q * WIDTH, WIDTH)]

        for j in range(chunks):
            at = pl.ds(j * chunk, chunk)
            for q in units:
                pltpu.matmul_push_rhs(columns(j, q), j % 2, q)
            for half, lhs in enumerate((fold_high, fold_low)):
                for q in units:
                    pltpu.matmul_acc_lhs(steps[j % lags][q], lhs, None if half else j % 2)
            behind = slab - start_ref[:, at]
            mask = step_ids == (behind - 1) * rx + pix_ref[:, at] // ry
            u = jnp.concatenate([pltpu.matmul_pop(steps[j % lags][q]) for q in units], axis=1)
            for c in range(4):
                picked = jnp.where(mask, u[c * step_rows:(c + 1) * step_rows], 0.0)
                value = jnp.sum(picked, axis=0, keepdims=True)
                if c == 3:
                    value = jnp.where(behind <= 0, 1.0, value)
                front_ref[j, pl.ds(c, 1), :] = value

        loads[channels + 3].wait()
        for q in units:
            pltpu.matmul_push_rhs(columns(0, q), 0, q, transpose=True)
        for j in range(chunks):
            for k in range(1, reach + 1):
                pl.when(slab + k < ns)(part_copy(k, j).wait_recv)
            if j == chunks - inner:
                for copy, _, receives in halos[2:]:
                    pl.when(receives)(copy.wait_recv)
            if j == 0 and direct(ns, nt):
                for k in (-reach, reach):
                    @pl.when(inside(slab + k))
                    def _(k=k):
                        pl.semaphore_signal(
                            ready_sem, inc=1, device_id={"slab": slab + k}, device_id_type=MESH)
            at = pl.ds(j * chunk, chunk)
            front_c = front_ref[j, pl.ds(0, 3), :]
            front_t = front_ref[j, pl.ds(3, 1), :]
            beyond = jnp.concatenate([far_ref[j, c] for c in range(3)], axis=0)
            beyond = jnp.where(slab + reach < ns, beyond, BACKGROUND)
            for k in range(reach - 1, 0, -1):
                pc = near_ref[k - 1, j, pl.ds(0, 3), :]
                pt = near_ref[k - 1, j, pl.ds(3, 1), :]
                beyond = jnp.where(slab + k < ns, pc + pt * beyond, beyond)
            pc = own_ref[j, pl.ds(0, 3), :]
            pt = own_ref[j, pl.ds(3, 1), :]
            rendered = front_c + front_t * (pc + pt * beyond)
            residual = RENDER_WEIGHT * (rendered - target_ref[:, at])
            color_cot = front_t * residual
            trans_cot = front_t * jnp.sum(residual * beyond, axis=0, keepdims=True)
            mask = row_ids16 == row_ref[:, at].astype(jnp.float32).astype(jnp.bfloat16)
            for c in range(4):
                cot = color_cot[c:c + 1] if c < 3 else trans_cot
                top = cot.astype(jnp.bfloat16)
                low = (cot - top.astype(jnp.float32)).astype(jnp.bfloat16)
                for half, part in enumerate((top, low)):
                    spread = jnp.where(mask, part, none)
                    for q in units:
                        fresh = j % 2 if c == 0 and half == 0 else None
                        pltpu.matmul_acc_lhs(
                            sums_acc[q][c], spread[:, q * WIDTH:(q + 1) * WIDTH], fresh)
            if j + 1 < chunks:
                for q in units:
                    pltpu.matmul_push_rhs(columns(j + 1, q), (j + 1) % 2, q, transpose=True)
            if j >= chunks - inner:
                for c in range((j - chunks + inner) * channels // inner, (j + 1 - chunks + inner) * channels // inner):
                    smooth_planes(c, range(1, depth - 1))
        for copy, _, receives in halos[:2]:
            pl.when(receives)(copy.wait_recv)
        for c in range(channels):
            smooth_planes(c, (0, depth - 1) if depth > 1 else (0,))
        for c in range(4):
            table_ref[pl.ds(c * rows, rows), :] = sum(pltpu.matmul_pop(sums_acc[q][c]) for q in units)

    pl.run_scoped(scatter, *[
        pltpu.ACC(q)((rows, WIDTH), jnp.float32) for q in units for _ in range(4)
    ], *[
        pltpu.ACC(q)((4 * step_rows, WIDTH), jnp.float32) for _ in range(lags) for q in units
    ])

    zero = jnp.zeros((rx, ry), jnp.float32)
    suffix = [zero, zero, zero]
    later = zero
    squares = zero
    for z in range(depth - 1, -1, -1):
        w = weight_ref[z]
        after = trans_ref[z]
        later = later + after * table_ref[pl.ds(3 * rows + z * rx, rx), :]
        dw = zero
        for c in range(3):
            suffix[c] = suffix[c] + table_ref[pl.ds(c * rows + z * rx, rx), :]
            col = sig_ref[c + 1, z]
            dw = dw + col * suffix[c]
            out = grad_ref[c + 1, z] + w * suffix[c] * (col * (1.0 - col))
            grad_ref[c + 1, z] = out
            squares = squares + out * out
        dtau = after * dw - later
        later = later + w * dw
        out = grad_ref[0, z] + dtau * (sig_ref[0, z] * span)
        grad_ref[0, z] = out
        squares = squares + out * out

    local = jnp.sum(squares)

    def norm_copy(phase, slot, peer):
        return pltpu.make_async_remote_copy(
            src_ref=nsend_ref.at[phase], dst_ref=nrecv_ref.at[slot],
            send_sem=norm_send.at[slot], recv_sem=norm_recv.at[slot],
            device_id=peer, device_id_type=MESH)

    if direct(ns, nt):
        far = inside(slab - reach).astype(jnp.int32) + inside(slab + reach).astype(jnp.int32)
        pl.semaphore_wait(ready_sem, far)
    value = jnp.full((1, 128), local, jnp.float32)
    copies = []
    base = 0
    for phase, peers in enumerate(phases):
        nsend_ref[phase] = value
        group = [norm_copy(phase, base + i, peer) for i, peer in enumerate(peers)]
        for copy in group:
            copy.start()
        for i, copy in enumerate(group):
            copy.wait_recv()
            value = value + nrecv_ref[base + i]
        base += len(group)
        copies += group
    limit = CLIP_RMS * math.sqrt(4.0 * total_depth * (rx * nt) * ry)
    scale_ref[...] = limit / jnp.maximum(jnp.sqrt(value), limit)
    for copy in loads[channels + 4:]:
        copy.wait()
    for copy in copies:
        copy.wait_send()
    for copy, sends, _ in halos:
        pl.when(sends)(copy.wait_send)
    for j in range(chunks):
        for k in range(1, reach + 1):
            pl.when(slab >= k)(part_copy(k, j).wait_send)
    for k in range(1, reach + 1):
        pl.when(slab + k < ns)(whole_copy(k).wait_send)


def span_reach(ns):
    return max(ns // 2, 1)


def direct(ns, nt):
    return ns * nt <= DIRECT_LIMIT and nt % 2 == 0


def adam_kernel(
    grid_ref, first_ref, second_ref, grad_ref, scale_ref,
    grid_hbm, first_hbm, second_hbm, grid_out, first_out, second_out, sem,
):
    channels, depth, rx, ry = grid_ref.shape
    scale = jnp.broadcast_to(scale_ref[0:1, 0:1], (rx, ry))
    copies = []
    for c in range(channels):
        for z in range(depth):
            clipped = grad_ref[c, z] * scale
            first = BETA_ONE * first_ref[c, z] + (1.0 - BETA_ONE) * clipped
            second = BETA_TWO * second_ref[c, z] + (1.0 - BETA_TWO) * clipped * clipped
            first_out[c, z] = first
            second_out[c, z] = second
            first_hat = first * (1.0 / (1.0 - BETA_ONE**STEP))
            second_hat = second * (1.0 / (1.0 - BETA_TWO**STEP))
            grid_out[c, z] = grid_ref[c, z] - LEARN_RATE * first_hat / (
                jnp.sqrt(second_hat) + EPSILON)
        pairs = ((first_out, first_hbm), (second_out, second_hbm), (grid_out, grid_hbm))
        for i, (a, b) in enumerate(pairs):
            copy = pltpu.make_async_copy(a.at[c], b.at[c], sem.at[i, c])
            copy.start()
            copies.append(copy)
    for copy in copies:
        copy.wait()


def per_device(voxel_grid, first_moment, second_moment, pixel_index, start_slab, ray_count, target):
    ns = lax.axis_size("slab")
    nt = lax.axis_size("tile")
    channels, depth, rx, ry = voxel_grid.shape
    rays = pixel_index.shape[0]
    chunk = math.gcd(rays, CHUNK)
    chunks = rays // chunk
    rows = depth * rx
    reach = span_reach(ns)
    messages = ns * nt // 2 if direct(ns, nt) else nt + ns - 2
    f32 = jnp.float32
    vmem = pl.BlockSpec(memory_space=pltpu.VMEM)
    hbm = pl.BlockSpec(memory_space=pltpu.HBM)
    cells = jax.ShapeDtypeStruct(voxel_grid.shape, f32)
    staged = pl.pallas_call(
        functools.partial(kernel, ns, nt, chunk),
        out_shape=(cells, cells, cells, cells, jax.ShapeDtypeStruct((1, 128), f32)),
        in_specs=[hbm] * 7,
        out_specs=(vmem,) * 5,
        scratch_shapes=[
            pltpu.VMEM((1, rays), jnp.int32),
            pltpu.VMEM((1, rays), jnp.int32),
            pltpu.VMEM((1, rays), jnp.int32),
            pltpu.VMEM(target.shape, f32),
            pltpu.VMEM((channels * rows, 2 * ry), jnp.bfloat16),
            pltpu.VMEM((depth, rx, ry), f32),
            pltpu.VMEM((depth, rx, ry), f32),
            pltpu.VMEM((channels, depth, rx, ry), f32),
            pltpu.VMEM((ry, rays), jnp.bfloat16),
            pltpu.VMEM((1, rays), jnp.int32),
            pltpu.VMEM((channels * rows, ry), f32),
            pltpu.VMEM((4, rx, ry), f32),
            pltpu.VMEM((reach, 4, rx, ry), f32),
            pltpu.VMEM((chunks, 4, chunk), f32),
            pltpu.VMEM((chunks, 4, chunk), f32),
            pltpu.VMEM((chunks, 3, 1, chunk), f32),
            pltpu.VMEM((max(reach - 1, 1), chunks, 4, chunk), f32),
            pltpu.VMEM((chunks, 3, 1, chunk), f32),
            pltpu.VMEM((2, channels, depth, ry), f32),
            pltpu.VMEM((2, channels, depth, ry), f32),
            pltpu.VMEM((2, channels, rx, ry), f32),
            pltpu.VMEM((2, 1, 128), f32),
            pltpu.VMEM((messages, 1, 128), f32),
            pltpu.SemaphoreType.DMA((reach,)),
            pltpu.SemaphoreType.DMA((reach,)),
            pltpu.SemaphoreType.DMA((reach, chunks)),
            pltpu.SemaphoreType.DMA((reach, chunks)),
            pltpu.SemaphoreType.REGULAR,
            pltpu.SemaphoreType.DMA((4,)),
            pltpu.SemaphoreType.DMA((4,)),
            pltpu.SemaphoreType.DMA((messages,)),
            pltpu.SemaphoreType.DMA((messages,)),
            pltpu.SemaphoreType.DMA((channels + 6,)),
        ],
        compiler_params=pltpu.CompilerParams(
            collective_id=0, has_side_effects=True, vmem_limit_bytes=32 * 1024 * 1024
        ),
        name="render_step",
    )(*(pltpu.with_memory_space_constraint(a, pltpu.HBM) for a in (
        voxel_grid,
        first_moment,
        second_moment,
        pixel_index.reshape(1, rays),
        start_slab.reshape(1, rays),
        ray_count.reshape(1, rays),
        target,
    )))
    return pl.pallas_call(
        adam_kernel,
        out_shape=(cells, cells, cells),
        in_specs=[vmem] * 5,
        out_specs=(hbm, hbm, hbm),
        scratch_shapes=[
            pltpu.VMEM(voxel_grid.shape, f32),
            pltpu.VMEM(voxel_grid.shape, f32),
            pltpu.VMEM(voxel_grid.shape, f32),
            pltpu.SemaphoreType.DMA((3, channels)),
        ],
        compiler_params=pltpu.CompilerParams(vmem_limit_bytes=32 * 1024 * 1024),
        name="adam",
    )(*staged)


def solution(mesh):
    cells = P(None, "slab", "tile", None)
    return jax.shard_map(
        per_device,
        mesh=mesh,
        in_specs=(cells, cells, cells, P("tile"), P("tile"), P("tile"), P(None, "tile")),
        out_specs=(cells, cells, cells),
        check_vma=False,
    )
```

```python
import functools
import math

import jax
import jax.numpy as jnp
from jax import lax
from jax.experimental import pallas as pl
from jax.experimental.pallas import tpu as pltpu
from jax.sharding import PartitionSpec as P

STEP = 20
RENDER_WEIGHT = 1000.0
TV_WEIGHT = 0.05
BACKGROUND = 1.0
STEP_SPAN = 4.0
CLIP_RMS = 0.25
LEARN_RATE = 0.02
BETA_ONE = 0.9
BETA_TWO = 0.99
EPSILON = 1e-08
CHUNK = 512
WIDTH = 256
OPENING = 1
DIRECT_LIMIT = 64
MESH = pl.DeviceIdType.MESH


def kernel(
    ns, nt, chunk,
    grid_hbm, first_hbm, second_hbm, pix_hbm, start_hbm, count_hbm, target_hbm,
    grid_ref, first_ref, second_ref, grad_ref, scale_ref,
    pix_ref, start_ref, count_ref, target_ref,
    pair_ref, trans_ref, weight_ref, sig_ref, onehot_ref, row_ref, table_ref,
    whole_ref, wholes_ref, front_ref, own_ref, last_ref, near_ref, far_ref,
    edge_ref, xhalo_ref, zhalo_ref, nsend_ref, nrecv_ref,
    whole_send, whole_recv, part_send, part_recv, ready_sem, halo_send, halo_recv, norm_send, norm_recv, load_sem,
):
    channels, depth, rx, ry = grid_ref.shape
    rays = pix_ref.shape[1]
    chunks = rays // chunk
    total_depth = depth * ns
    reach = span_reach(ns)
    span = STEP_SPAN / total_depth
    rows = depth * rx
    slab = lax.axis_index("slab")
    tile = lax.axis_index("tile")

    def slab_peer(d):
        return {"slab": lax.rem(slab + d, ns)}

    def tile_peer(d):
        return {"tile": lax.rem(tile + d, nt)}

    if direct(ns, nt):
        phases = [[
            {"slab": lax.rem(slab + k // nt, ns), "tile": lax.rem(tile + k % nt, nt)}
            for k in range(1, ns * nt)
        ]]
        near = reach
    else:
        phases = [[tile_peer(d) for d in range(1, nt)], [slab_peer(d) for d in range(1, ns)]]
        near = ns - 1
    offsets = [k for k in range(-near, near + 1) if k]

    def inside(s):
        return (s >= 0) & (s < ns)

    loads = [
        pltpu.make_async_copy(grid_hbm.at[c], grid_ref.at[c], load_sem.at[c])
        for c in range(channels)
    ]
    rest = (
        (pix_hbm, pix_ref), (start_hbm, start_ref), (count_hbm, count_ref),
        (target_hbm, target_ref), (first_hbm, first_ref), (second_hbm, second_ref),
    )
    loads += [
        pltpu.make_async_copy(a, b, load_sem.at[channels + i]) for i, (a, b) in enumerate(rest)
    ]
    for copy in loads[:-2]:
        copy.start()

    barrier = pltpu.get_barrier_semaphore()
    for d in range(1, nt):
        pl.semaphore_signal(barrier, inc=1, device_id=tile_peer(d), device_id_type=MESH)
    greeters = nt - 1
    for k in offsets:
        @pl.when(inside(slab + k))
        def _(k=k):
            pl.semaphore_signal(
                barrier, inc=1, device_id={"slab": slab + k}, device_id_type=MESH)
        greeters = greeters + inside(slab + k).astype(jnp.int32)

    for c in range(channels):
        loads[c].wait()
    for copy in loads[-2:]:
        copy.start()
    edge_ref[0] = grid_ref[:, :, rx - 1, :]
    edge_ref[1] = grid_ref[:, :, 0, :]

    total = jnp.zeros((rx, ry), jnp.float32)
    before = jnp.ones((rx, ry), jnp.float32)
    sums = [jnp.zeros((rx, ry), jnp.float32) for _ in range(3)]
    for z in range(depth):
        s = grid_ref[0, z]
        e = jnp.exp(-jnp.abs(s))
        tau = (jnp.maximum(s, 0.0) + jnp.log1p(e)) * span
        sig_ref[0, z] = jnp.where(s >= 0, 1.0, e) / (1.0 + e)
        total = total + tau
        after = jnp.exp(-total)
        w = before * (1.0 - jnp.exp(-tau))
        before = after
        trans_ref[z] = after
        weight_ref[z] = w
        for c in range(3):
            col = 1.0 / (1.0 + jnp.exp(-grid_ref[c + 1, z]))
            sig_ref[c + 1, z] = col
            sums[c] = sums[c] + w * col
            table_ref[pl.ds(c * rows + z * rx, rx), :] = sums[c]
        table_ref[pl.ds(3 * rows + z * rx, rx), :] = after
    for c in range(3):
        whole_ref[c] = sums[c]
    whole_ref[3] = before
    full = table_ref[...]
    high = full.astype(jnp.bfloat16)
    pair_ref[:, :ry] = high
    pair_ref[:, ry:] = (full - high.astype(jnp.float32)).astype(jnp.bfloat16)

    def whole_copy(k):
        return pltpu.make_async_remote_copy(
            src_ref=whole_ref, dst_ref=wholes_ref.at[k - 1],
            send_sem=whole_send.at[k - 1], recv_sem=whole_recv.at[k - 1],
            device_id=slab_peer(k), device_id_type=MESH)

    def halo_copy(src, dst, i, peer):
        return pltpu.make_async_remote_copy(
            src_ref=src, dst_ref=dst, send_sem=halo_send.at[i], recv_sem=halo_recv.at[i],
            device_id=peer, device_id_type=MESH)

    halos = [
        (halo_copy(grid_ref.at[:, depth - 1], zhalo_ref.at[0], 0, slab_peer(1)), slab < ns - 1, slab > 0),
        (halo_copy(grid_ref.at[:, 0], zhalo_ref.at[1], 1, slab_peer(ns - 1)), slab > 0, slab < ns - 1),
        (halo_copy(edge_ref.at[0], xhalo_ref.at[0], 2, tile_peer(1)), tile < nt - 1, tile > 0),
        (halo_copy(edge_ref.at[1], xhalo_ref.at[1], 3, tile_peer(nt - 1)), tile > 0, tile < nt - 1),
    ]
    def part_copy(k, j):
        src, dst = (last_ref, far_ref) if k == reach else (own_ref, near_ref.at[k - 1])
        return pltpu.make_async_remote_copy(
            src_ref=src.at[j], dst_ref=dst.at[j],
            send_sem=part_send.at[k - 1, j], recv_sem=part_recv.at[k - 1, j],
            device_id=slab_peer(ns - k), device_id_type=MESH)

    y_ids = lax.broadcasted_iota(jnp.int32, (ry, chunk), 0).astype(jnp.float32).astype(jnp.bfloat16)
    row_ids = lax.broadcasted_iota(jnp.int32, (rows, chunk), 0)

    for copy in loads[channels:channels + 3]:
        copy.wait()
    units = range(chunk // WIDTH)

    def enter():
        pl.semaphore_wait(barrier, greeters)
        for k in range(reach, 0, -1):
            pl.when(slab + k < ns)(whole_copy(k).start)
        for copy, sends, _ in halos[2:]:
            pl.when(sends)(copy.start)

    opening = min(OPENING, chunks)

    def gather(*accs):
        banks = [[accs[(b * len(units) + q) * 4:][:4] for q in units] for b in range(2)]
        for j in range(chunks + 1):
            if j < chunks:
                at = pl.ds(j * chunk, chunk)
                pix = pix_ref[:, at]
                start = start_ref[:, at]
                px = pix // ry
                py = (pix - px * ry).astype(jnp.float32).astype(jnp.bfloat16)
                length = jnp.clip((start - slab) * depth + count_ref[:, at], 0, depth)
                length = jnp.where(slab >= start, length, 0)
                row_ref[:, at] = jnp.where(length > 0, (length - 1) * rx + px, -1)
                hot = jnp.where(y_ids == py, jnp.ones((), jnp.bfloat16), jnp.zeros((), jnp.bfloat16))
                onehot_ref[:, at] = hot
                for q in units:
                    pltpu.matmul_push_rhs(hot[:, q * WIDTH:(q + 1) * WIDTH], j % 2, q)
                for c in range(4):
                    block = pl.ds(c * rows, rows)
                    for half in range(2):
                        lhs = pair_ref[block, half * ry:(half + 1) * ry]
                        for q in units:
                            fresh = j % 2 if c == 0 and half == 0 else None
                            pltpu.matmul_acc_lhs(banks[j % 2][q][c], lhs, fresh)
            if j == 0:
                continue
            i = j - 1
            row = row_ref[:, pl.ds(i * chunk, chunk)]
            mask = row_ids == row
            for c in range(4):
                u = jnp.concatenate([pltpu.matmul_pop(banks[i % 2][q][c]) for q in units], axis=1)
                part = jnp.sum(jnp.where(mask, u, 0.0), axis=0, keepdims=True)
                if c == 3:
                    part = jnp.where(row < 0, 1.0, part)
                own_ref[i, pl.ds(c, 1), :] = part
            for c in range(3):
                last_ref[i, c] = own_ref[i, pl.ds(c, 1), :] + BACKGROUND * part
            if j < opening:
                continue
            if j == opening:
                enter()
            for n in range(0 if j == opening else i, j):
                for k in range(1, reach + 1):
                    pl.when(slab >= k)(part_copy(k, n).start)

    pl.run_scoped(gather, *[
        pltpu.ACC(q)((rows, WIDTH), jnp.float32)
        for _ in range(2) for q in units for _ in range(4)
    ])

    for copy, sends, _ in halos[:2]:
        pl.when(sends)(copy.start)
    x_ids = lax.broadcasted_iota(jnp.int32, (rx, ry), 0)
    lane_ids = lax.broadcasted_iota(jnp.int32, (rx, ry), 1)
    first_x = tile == 0
    last_x = tile == nt - 1
    def smooth_planes(c, planes):
        for z in planes:
            g = grid_ref[c, z]
            if z > 0:
                below = grid_ref[c, z - 1]
            else:
                below = jnp.where(slab > 0, zhalo_ref[0, c], g)
            if z < depth - 1:
                above = grid_ref[c, z + 1]
            else:
                above = jnp.where(slab < ns - 1, zhalo_ref[1, c], g)
            xl = jnp.broadcast_to(xhalo_ref[0, c, pl.ds(z, 1), :], (rx, ry))
            xh = jnp.broadcast_to(xhalo_ref[1, c, pl.ds(z, 1), :], (rx, ry))
            xl = jnp.where(first_x, g, xl)
            xh = jnp.where(last_x, g, xh)
            left = jnp.where(x_ids == 0, xl, pltpu.roll(g, 1, 0))
            right = jnp.where(x_ids == rx - 1, xh, pltpu.roll(g, rx - 1, 0))
            down = jnp.where(lane_ids == 0, g, pltpu.roll(g, 1, 1))
            up = jnp.where(lane_ids == ry - 1, g, pltpu.roll(g, ry - 1, 1))
            smooth = (g - below) + (g - above) + (g - left) + (g - right) + (g - down) + (g - up)
            grad_ref[c, z] = (2.0 * TV_WEIGHT) * smooth

    for k in range(1, reach + 1):
        pl.when(slab >= k)(whole_copy(k).wait_recv)
    folded = [[] for _ in range(4)]
    fold_t = jnp.ones((rx, ry), jnp.float32)
    fold_c = [jnp.zeros((rx, ry), jnp.float32)] * 3
    for k in range(1, reach + 1):
        there = slab >= k
        t = wholes_ref[k - 1, 3]
        fold_c = [jnp.where(there, wholes_ref[k - 1, c] + t * fold_c[c], 0.0) for c in range(3)]
        fold_t = jnp.where(there, t * fold_t, 0.0)
        for c in range(4):
            folded[c].append(fold_c[c] if c < 3 else fold_t)
    folds = jnp.concatenate([f for fs in folded for f in fs], axis=0)
    fold_high = folds.astype(jnp.bfloat16)
    fold_low = (folds - fold_high.astype(jnp.float32)).astype(jnp.bfloat16)
    step_rows = reach * rx
    step_ids = lax.broadcasted_iota(jnp.int32, (step_rows, chunk), 0)
    row_ids16 = row_ids.astype(jnp.float32).astype(jnp.bfloat16)
    none = jnp.zeros((), jnp.bfloat16)
    lags = 4
    inner = min(channels, chunks)

    def scatter(*accs):
        sums_acc = [accs[q * 4:][:4] for q in units]
        accs = accs[4 * len(units):]
        steps = [[accs[b * len(units) + q] for q in units] for b in range(lags)]

        def columns(j, q):
            return onehot_ref[:, pl.ds(j * chunk + q * WIDTH, WIDTH)]

        for j in range(chunks):
            at = pl.ds(j * chunk, chunk)
            for q in units:
                pltpu.matmul_push_rhs(columns(j, q), j % 2, q)
            for half, lhs in enumerate((fold_high, fold_low)):
                for q in units:
                    pltpu.matmul_acc_lhs(steps[j % lags][q], lhs, None if half else j % 2)
            behind = slab - start_ref[:, at]
            mask = step_ids == (behind - 1) * rx + pix_ref[:, at] // ry
            u = jnp.concatenate([pltpu.matmul_pop(steps[j % lags][q]) for q in units], axis=1)
            for c in range(4):
                picked = jnp.where(mask, u[c * step_rows:(c + 1) * step_rows], 0.0)
                value = jnp.sum(picked, axis=0, keepdims=True)
                if c == 3:
                    value = jnp.where(behind <= 0, 1.0, value)
                front_ref[j, pl.ds(c, 1), :] = value

        loads[channels + 3].wait()
        for q in units:
            pltpu.matmul_push_rhs(columns(0, q), 0, q, transpose=True)
        for j in range(chunks):
            for k in range(1, reach + 1):
                pl.when(slab + k < ns)(part_copy(k, j).wait_recv)
            if j == chunks - inner:
                for copy, _, receives in halos[2:]:
                    pl.when(receives)(copy.wait_recv)
            if j == 0 and direct(ns, nt):
                for k in (-reach, reach):
                    @pl.when(inside(slab + k))
                    def _(k=k):
                        pl.semaphore_signal(
                            ready_sem, inc=1, device_id={"slab": slab + k}, device_id_type=MESH)
            at = pl.ds(j * chunk, chunk)
            front_c = front_ref[j, pl.ds(0, 3), :]
            front_t = front_ref[j, pl.ds(3, 1), :]
            beyond = jnp.concatenate([far_ref[j, c] for c in range(3)], axis=0)
            beyond = jnp.where(slab + reach < ns, beyond, BACKGROUND)
            for k in range(reach - 1, 0, -1):
                pc = near_ref[k - 1, j, pl.ds(0, 3), :]
                pt = near_ref[k - 1, j, pl.ds(3, 1), :]
                beyond = jnp.where(slab + k < ns, pc + pt * beyond, beyond)
            pc = own_ref[j, pl.ds(0, 3), :]
            pt = own_ref[j, pl.ds(3, 1), :]
            rendered = front_c + front_t * (pc + pt * beyond)
            residual = RENDER_WEIGHT * (rendered - target_ref[:, at])
            color_cot = front_t * residual
            trans_cot = front_t * jnp.sum(residual * beyond, axis=0, keepdims=True)
            mask = row_ids16 == row_ref[:, at].astype(jnp.float32).astype(jnp.bfloat16)
            for c in range(4):
                cot = color_cot[c:c + 1] if c < 3 else trans_cot
                top = cot.astype(jnp.bfloat16)
                low = (cot - top.astype(jnp.float32)).astype(jnp.bfloat16)
                for half, part in enumerate((top, low)):
                    spread = jnp.where(mask, part, none)
                    for q in units:
                        fresh = j % 2 if c == 0 and half == 0 else None
                        pltpu.matmul_acc_lhs(
                            sums_acc[q][c], spread[:, q * WIDTH:(q + 1) * WIDTH], fresh)
            if j + 1 < chunks:
                for q in units:
                    pltpu.matmul_push_rhs(columns(j + 1, q), (j + 1) % 2, q, transpose=True)
            if j >= chunks - inner:
                for c in range((j - chunks + inner) * channels // inner, (j + 1 - chunks + inner) * channels // inner):
                    smooth_planes(c, range(1, depth - 1))
        for copy, _, receives in halos[:2]:
            pl.when(receives)(copy.wait_recv)
        for c in range(channels):
            smooth_planes(c, (0, depth - 1) if depth > 1 else (0,))
        for c in range(4):
            table_ref[pl.ds(c * rows, rows), :] = sum(pltpu.matmul_pop(sums_acc[q][c]) for q in units)

    pl.run_scoped(scatter, *[
        pltpu.ACC(q)((rows, WIDTH), jnp.float32) for q in units for _ in range(4)
    ], *[
        pltpu.ACC(q)((4 * step_rows, WIDTH), jnp.float32) for _ in range(lags) for q in units
    ])

    zero = jnp.zeros((rx, ry), jnp.float32)
    suffix = [zero, zero, zero]
    later = zero
    squares = zero
    for z in range(depth - 1, -1, -1):
        w = weight_ref[z]
        after = trans_ref[z]
        later = later + after * table_ref[pl.ds(3 * rows + z * rx, rx), :]
        dw = zero
        for c in range(3):
            suffix[c] = suffix[c] + table_ref[pl.ds(c * rows + z * rx, rx), :]
            col = sig_ref[c + 1, z]
            dw = dw + col * suffix[c]
            out = grad_ref[c + 1, z] + w * suffix[c] * (col * (1.0 - col))
            grad_ref[c + 1, z] = out
            squares = squares + out * out
        dtau = after * dw - later
        later = later + w * dw
        out = grad_ref[0, z] + dtau * (sig_ref[0, z] * span)
        grad_ref[0, z] = out
        squares = squares + out * out

    local = jnp.sum(squares)

    def norm_copy(phase, slots, peer=None):
        src = nsend_ref.at[pl.ds(phase, 1)] if peer else nrecv_ref.at[slots]
        return pltpu.make_async_remote_copy(
            src_ref=src, dst_ref=nrecv_ref.at[slots],
            send_sem=norm_send.at[phase], recv_sem=norm_recv.at[phase],
            device_id=peer or tile_peer(1), device_id_type=MESH)

    if direct(ns, nt):
        far = inside(slab - reach).astype(jnp.int32) + inside(slab + reach).astype(jnp.int32)
        pl.semaphore_wait(ready_sem, far)
    value = jnp.full((1, 128), local, jnp.float32)
    base = 0
    for phase, peers in enumerate(phases):
        nsend_ref[phase] = value
        for i, peer in enumerate(peers):
            norm_copy(phase, pl.ds(base + i, 1), peer).start()
        if phase == 0:
            for copy in loads[-2:]:
                copy.wait()
            first_ref[...] = BETA_ONE * first_ref[...]
            second_ref[...] = BETA_TWO * second_ref[...]
        norm_copy(phase, pl.ds(base, len(peers))).wait_recv()
        value = value + jnp.sum(nrecv_ref[pl.ds(base, len(peers)), 0, :], axis=0, keepdims=True)
        base += len(peers)
    limit = CLIP_RMS * math.sqrt(4.0 * total_depth * (rx * nt) * ry)
    scale_ref[...] = limit / jnp.maximum(jnp.sqrt(value), limit)
    base = 0
    for phase, peers in enumerate(phases):
        norm_copy(phase, pl.ds(base, len(peers))).wait_send()
        base += len(peers)
    for copy, sends, _ in halos:
        pl.when(sends)(copy.wait_send)
    for j in range(chunks):
        for k in range(1, reach + 1):
            pl.when(slab >= k)(part_copy(k, j).wait_send)
    for k in range(1, reach + 1):
        pl.when(slab + k < ns)(whole_copy(k).wait_send)


def span_reach(ns):
    return max(ns // 2, 1)


def direct(ns, nt):
    return ns * nt <= DIRECT_LIMIT


def adam_kernel(
    grid_ref, first_ref, second_ref, grad_ref, scale_ref,
    grid_hbm, first_hbm, second_hbm, grid_out, first_out, second_out, sem,
):
    channels, depth, rx, ry = grid_ref.shape
    gain = (1.0 - BETA_ONE**STEP) / LEARN_RATE
    slope = gain / math.sqrt(1.0 - BETA_TWO**STEP)
    offset = gain * EPSILON
    scale = jnp.broadcast_to(scale_ref[0:1, 0:1], (rx, ry))
    linear = (1.0 - BETA_ONE) * scale
    square = (1.0 - BETA_TWO) * scale * scale
    copies = []
    pieces = 2 if depth % 2 == 0 else 1
    for c in range(channels):
        for p in range(pieces):
            planes = range(p * depth // pieces, (p + 1) * depth // pieces)
            for z in planes:
                g = grad_ref[c, z]
                first = first_ref[c, z] + linear * g
                second = second_ref[c, z] + square * g * g
                first_out[c, z] = first
                second_out[c, z] = second
                root = second * lax.rsqrt(second)
                grid_out[c, z] = grid_ref[c, z] - first / (root * slope + offset)
            at = pl.ds(p * depth // pieces, depth // pieces)
            pairs = ((first_out, first_hbm), (second_out, second_hbm), (grid_out, grid_hbm))
            for i, (a, b) in enumerate(pairs):
                copy = pltpu.make_async_copy(a.at[c, at], b.at[c, at], sem.at[i, c, p])
                copy.start()
                copies.append(copy)
    for copy in copies:
        copy.wait()


def per_device(voxel_grid, first_moment, second_moment, pixel_index, start_slab, ray_count, target):
    ns = lax.axis_size("slab")
    nt = lax.axis_size("tile")
    channels, depth, rx, ry = voxel_grid.shape
    rays = pixel_index.shape[0]
    chunk = math.gcd(rays, CHUNK)
    chunks = rays // chunk
    rows = depth * rx
    reach = span_reach(ns)
    messages = ns * nt - 1 if direct(ns, nt) else nt + ns - 2
    f32 = jnp.float32
    vmem = pl.BlockSpec(memory_space=pltpu.VMEM)
    hbm = pl.BlockSpec(memory_space=pltpu.HBM)
    cells = jax.ShapeDtypeStruct(voxel_grid.shape, f32)
    staged = pl.pallas_call(
        functools.partial(kernel, ns, nt, chunk),
        out_shape=(cells, cells, cells, cells, jax.ShapeDtypeStruct((1, 128), f32)),
        in_specs=[hbm] * 7,
        out_specs=(vmem,) * 5,
        scratch_shapes=[
            pltpu.VMEM((1, rays), jnp.int32),
            pltpu.VMEM((1, rays), jnp.int32),
            pltpu.VMEM((1, rays), jnp.int32),
            pltpu.VMEM(target.shape, f32),
            pltpu.VMEM((channels * rows, 2 * ry), jnp.bfloat16),
            pltpu.VMEM((depth, rx, ry), f32),
            pltpu.VMEM((depth, rx, ry), f32),
            pltpu.VMEM((channels, depth, rx, ry), f32),
            pltpu.VMEM((ry, rays), jnp.bfloat16),
            pltpu.VMEM((1, rays), jnp.int32),
            pltpu.VMEM((channels * rows, ry), f32),
            pltpu.VMEM((4, rx, ry), f32),
            pltpu.VMEM((reach, 4, rx, ry), f32),
            pltpu.VMEM((chunks, 4, chunk), f32),
            pltpu.VMEM((chunks, 4, chunk), f32),
            pltpu.VMEM((chunks, 3, 1, chunk), f32),
            pltpu.VMEM((max(reach - 1, 1), chunks, 4, chunk), f32),
            pltpu.VMEM((chunks, 3, 1, chunk), f32),
            pltpu.VMEM((2, channels, depth, ry), f32),
            pltpu.VMEM((2, channels, depth, ry), f32),
            pltpu.VMEM((2, channels, rx, ry), f32),
            pltpu.VMEM((2, 1, 128), f32),
            pltpu.VMEM((messages, 1, 128), f32),
            pltpu.SemaphoreType.DMA((reach,)),
            pltpu.SemaphoreType.DMA((reach,)),
            pltpu.SemaphoreType.DMA((reach, chunks)),
            pltpu.SemaphoreType.DMA((reach, chunks)),
            pltpu.SemaphoreType.REGULAR,
            pltpu.SemaphoreType.DMA((4,)),
            pltpu.SemaphoreType.DMA((4,)),
            pltpu.SemaphoreType.DMA((2,)),
            pltpu.SemaphoreType.DMA((2,)),
            pltpu.SemaphoreType.DMA((channels + 6,)),
        ],
        compiler_params=pltpu.CompilerParams(
            collective_id=0, has_side_effects=True, vmem_limit_bytes=32 * 1024 * 1024
        ),
        name="render_step",
    )(*(pltpu.with_memory_space_constraint(a, pltpu.HBM) for a in (
        voxel_grid,
        first_moment,
        second_moment,
        pixel_index.reshape(1, rays),
        start_slab.reshape(1, rays),
        ray_count.reshape(1, rays),
        target,
    )))
    return pl.pallas_call(
        adam_kernel,
        out_shape=(cells, cells, cells),
        in_specs=[vmem] * 5,
        out_specs=(hbm, hbm, hbm),
        scratch_shapes=[
            pltpu.VMEM(voxel_grid.shape, f32),
            pltpu.VMEM(voxel_grid.shape, f32),
            pltpu.VMEM(voxel_grid.shape, f32),
            pltpu.SemaphoreType.DMA((3, channels, 2)),
        ],
        compiler_params=pltpu.CompilerParams(vmem_limit_bytes=32 * 1024 * 1024),
        name="adam",
    )(*staged)


def solution(mesh):
    cells = P(None, "slab", "tile", None)
    return jax.shard_map(
        per_device,
        mesh=mesh,
        in_specs=(cells, cells, cells, P("tile"), P("tile"), P("tile"), P(None, "tile")),
        out_specs=(cells, cells, cells),
        check_vma=False,
    )
```

```python
import functools
import math

import jax
import jax.numpy as jnp
from jax import lax
from jax.experimental import pallas as pl
from jax.experimental.pallas import tpu as pltpu
from jax.sharding import PartitionSpec as P

STEP = 20
RENDER_WEIGHT = 1000.0
TV_WEIGHT = 0.05
BACKGROUND = 1.0
STEP_SPAN = 4.0
CLIP_RMS = 0.25
LEARN_RATE = 0.02
BETA_ONE = 0.9
BETA_TWO = 0.99
EPSILON = 1e-08
CHUNK = 512
WIDTH = 256
OPENING = 1
PIECES = 4
DIRECT_LIMIT = 64
MESH = pl.DeviceIdType.MESH


def kernel(
    ns, nt, chunk,
    grid_hbm, first_hbm, second_hbm, pix_hbm, start_hbm, count_hbm, target_hbm,
    grid_ref, first_ref, second_ref, grad_ref, scale_ref,
    ints_ref, target_ref,
    pair_ref, trans_ref, weight_ref, sig_ref, onehot_ref, row_ref, table_ref,
    whole_ref, wholes_ref, front_ref, own_ref, last_ref, far_ref,
    edge_ref, xhalo_ref, zhalo_ref, nsend_ref, nrecv_ref,
    whole_sem, part_send, part_recv, ready_sem, halo_send, halo_recv, norm_send, norm_recv, load_sem,
):
    channels, depth, rx, ry = grid_ref.shape
    rays = ints_ref.shape[2]
    pix_ref, start_ref, count_ref = (ints_ref.at[i] for i in range(3))
    chunks = rays // chunk
    total_depth = depth * ns
    reach = span_reach(ns)
    span = STEP_SPAN / total_depth
    rows = depth * rx
    slab = lax.axis_index("slab")
    tile = lax.axis_index("tile")

    def slab_peer(d):
        return {"slab": lax.rem(slab + d, ns)}

    def tile_peer(d):
        return {"tile": lax.rem(tile + d, nt)}

    if direct(ns, nt):
        phases = [[
            {"slab": lax.rem(slab + k // nt, ns), "tile": lax.rem(tile + k % nt, nt)}
            for k in range(1, ns * nt)
        ]]
        near = reach
    else:
        phases = [[tile_peer(d) for d in range(1, nt)], [slab_peer(d) for d in range(1, ns)]]
        near = ns - 1
    offsets = [k for k in range(-near, near + 1) if k]

    def inside(s):
        return (s >= 0) & (s < ns)

    pieces = split(depth)
    step = depth // pieces
    grid_load = pltpu.make_async_copy(grid_hbm, grid_ref, load_sem.at[0])
    for c in range(channels):
        for p in range(pieces):
            at = pl.ds(p * step, step)
            pltpu.make_async_copy(grid_hbm.at[c, at], grid_ref.at[c, at], load_sem.at[0]).start()
    for i, a in enumerate((pix_hbm, start_hbm, count_hbm)):
        pltpu.make_async_copy(a, ints_ref.at[i], load_sem.at[1]).start()
    ints_load = pltpu.make_async_copy(ints_ref, ints_ref, load_sem.at[1])
    target_load = pltpu.make_async_copy(target_hbm, target_ref, load_sem.at[2])
    target_load.start()
    moment_loads = [
        pltpu.make_async_copy(first_hbm, first_ref, load_sem.at[3]),
        pltpu.make_async_copy(second_hbm, second_ref, load_sem.at[4]),
    ]

    barrier = pltpu.get_barrier_semaphore()
    for d in range(1, nt):
        pl.semaphore_signal(barrier, inc=1, device_id=tile_peer(d), device_id_type=MESH)
    greeters = nt - 1
    for k in offsets:
        @pl.when(inside(slab + k))
        def _(k=k):
            pl.semaphore_signal(
                barrier, inc=1, device_id={"slab": slab + k}, device_id_type=MESH)
        greeters = greeters + inside(slab + k).astype(jnp.int32)

    grid_load.wait()
    for copy in moment_loads:
        copy.start()
    edge_ref[0] = grid_ref[:, :, rx - 1, :]
    edge_ref[1] = grid_ref[:, :, 0, :]

    total = jnp.zeros((rx, ry), jnp.float32)
    before = jnp.ones((rx, ry), jnp.float32)
    sums = [jnp.zeros((rx, ry), jnp.float32) for _ in range(3)]
    for z in range(depth):
        s = grid_ref[0, z]
        e = jnp.exp(-jnp.abs(s))
        tau = (jnp.maximum(s, 0.0) + jnp.log1p(e)) * span
        sig_ref[0, z] = jnp.where(s >= 0, 1.0, e) / (1.0 + e)
        total = total + tau
        after = jnp.exp(-total)
        w = before * (1.0 - jnp.exp(-tau))
        before = after
        trans_ref[z] = after
        weight_ref[z] = w
        for c in range(3):
            col = 1.0 / (1.0 + jnp.exp(-grid_ref[c + 1, z]))
            sig_ref[c + 1, z] = col
            sums[c] = sums[c] + w * col
            table_ref[pl.ds(c * rows + z * rx, rx), :] = sums[c]
        table_ref[pl.ds(3 * rows + z * rx, rx), :] = after
    for c in range(3):
        whole_ref[c] = sums[c]
    whole_ref[3] = before
    full = table_ref[...]
    high = full.astype(jnp.bfloat16)
    pair_ref[:, :ry] = high
    pair_ref[:, ry:] = (full - high.astype(jnp.float32)).astype(jnp.bfloat16)

    def waiter(ref, sem):
        return pltpu.make_async_remote_copy(
            src_ref=ref, dst_ref=ref, send_sem=sem, recv_sem=sem,
            device_id=tile_peer(1), device_id_type=MESH)

    def wait_sent(ref, sem, count, most):
        for n in range(1, most + 1):
            pl.when(count == n)(waiter(ref.at[pl.ds(0, n)], sem).wait_send)

    def wait_received(ref, sem, count, most):
        for n in range(1, most + 1):
            pl.when(count == n)(waiter(ref.at[pl.ds(0, n)], sem).wait_recv)

    behind_count = jnp.minimum(slab, reach)
    ahead_count = jnp.minimum(ns - 1 - slab, reach)
    beside_count = (tile < nt - 1).astype(jnp.int32) + (tile > 0).astype(jnp.int32)
    level_count = (slab < ns - 1).astype(jnp.int32) + (slab > 0).astype(jnp.int32)

    def whole_copy(k):
        return pltpu.make_async_remote_copy(
            src_ref=whole_ref, dst_ref=wholes_ref.at[k - 1],
            send_sem=whole_sem.at[0], recv_sem=whole_sem.at[1],
            device_id=slab_peer(k), device_id_type=MESH)

    def halo_copy(src, dst, i, peer):
        return pltpu.make_async_remote_copy(
            src_ref=src, dst_ref=dst, send_sem=halo_send.at[i // 2], recv_sem=halo_recv.at[i // 2],
            device_id=peer, device_id_type=MESH)

    halos = [
        (halo_copy(grid_ref.at[:, depth - 1], zhalo_ref.at[0], 0, slab_peer(1)), slab < ns - 1),
        (halo_copy(grid_ref.at[:, 0], zhalo_ref.at[1], 1, slab_peer(ns - 1)), slab > 0),
        (halo_copy(edge_ref.at[0], xhalo_ref.at[0], 2, tile_peer(1)), tile < nt - 1),
        (halo_copy(edge_ref.at[1], xhalo_ref.at[1], 3, tile_peer(nt - 1)), tile > 0),
    ]
    def part_copy(k, j):
        src = last_ref if k == reach else own_ref
        return pltpu.make_async_remote_copy(
            src_ref=src.at[j], dst_ref=far_ref.at[j, pl.ds(4 * (k - 1), src.shape[1])],
            send_sem=part_send.at[k - 1], recv_sem=part_recv.at[j],
            device_id=slab_peer(ns - k), device_id_type=MESH)

    y_ids = lax.broadcasted_iota(jnp.int32, (ry, chunk), 0).astype(jnp.float32).astype(jnp.bfloat16)
    row_ids = lax.broadcasted_iota(jnp.int32, (rows, chunk), 0)

    ints_load.wait()
    units = range(chunk // WIDTH)

    def enter():
        pl.semaphore_wait(barrier, greeters)
        for k in range(reach, 0, -1):
            pl.when(slab + k < ns)(whole_copy(k).start)
        for copy, sends in halos[2:]:
            pl.when(sends)(copy.start)

    opening = min(OPENING, chunks)

    def gather(*accs):
        banks = [[accs[(b * len(units) + q) * 4:][:4] for q in units] for b in range(2)]
        for j in range(chunks + 1):
            if j < chunks:
                at = pl.ds(j * chunk, chunk)
                pix = pix_ref[:, at]
                start = start_ref[:, at]
                px = pix // ry
                py = (pix - px * ry).astype(jnp.float32).astype(jnp.bfloat16)
                length = jnp.clip((start - slab) * depth + count_ref[:, at], 0, depth)
                length = jnp.where(slab >= start, length, 0)
                row_ref[:, at] = jnp.where(length > 0, (length - 1) * rx + px, -1)
                hot = jnp.where(y_ids == py, jnp.ones((), jnp.bfloat16), jnp.zeros((), jnp.bfloat16))
                onehot_ref[:, at] = hot
                for q in units:
                    pltpu.matmul_push_rhs(hot[:, q * WIDTH:(q + 1) * WIDTH], j % 2, q)
                for c in range(4):
                    block = pl.ds(c * rows, rows)
                    for half in range(2):
                        lhs = pair_ref[block, half * ry:(half + 1) * ry]
                        for q in units:
                            fresh = j % 2 if c == 0 and half == 0 else None
                            pltpu.matmul_acc_lhs(banks[j % 2][q][c], lhs, fresh)
            if j == 0:
                continue
            i = j - 1
            row = row_ref[:, pl.ds(i * chunk, chunk)]
            mask = row_ids == row
            for c in range(4):
                u = jnp.concatenate([pltpu.matmul_pop(banks[i % 2][q][c]) for q in units], axis=1)
                part = jnp.sum(jnp.where(mask, u, 0.0), axis=0, keepdims=True)
                if c == 3:
                    part = jnp.where(row < 0, 1.0, part)
                own_ref[i, c] = part
            for c in range(3):
                last_ref[i, c] = own_ref[i, c] + BACKGROUND * part
            if j < opening:
                continue
            if j == opening:
                enter()
            for n in range(0 if j == opening else i, j):
                for k in range(1, reach + 1):
                    pl.when(slab >= k)(part_copy(k, n).start)

    pl.run_scoped(gather, *[
        pltpu.ACC(q)((rows, WIDTH), jnp.float32)
        for _ in range(2) for q in units for _ in range(4)
    ])

    for copy, sends in halos[:2]:
        pl.when(sends)(copy.start)
    x_ids = lax.broadcasted_iota(jnp.int32, (rx, ry), 0)
    lane_ids = lax.broadcasted_iota(jnp.int32, (rx, ry), 1)
    first_x = tile == 0
    last_x = tile == nt - 1
    def smooth_planes(c, planes):
        for z in planes:
            g = grid_ref[c, z]
            if z > 0:
                below = grid_ref[c, z - 1]
            else:
                below = jnp.where(slab > 0, zhalo_ref[0, c], g)
            if z < depth - 1:
                above = grid_ref[c, z + 1]
            else:
                above = jnp.where(slab < ns - 1, zhalo_ref[1, c], g)
            xl = jnp.broadcast_to(xhalo_ref[0, c, pl.ds(z, 1), :], (rx, ry))
            xh = jnp.broadcast_to(xhalo_ref[1, c, pl.ds(z, 1), :], (rx, ry))
            xl = jnp.where(first_x, g, xl)
            xh = jnp.where(last_x, g, xh)
            left = jnp.where(x_ids == 0, xl, pltpu.roll(g, 1, 0))
            right = jnp.where(x_ids == rx - 1, xh, pltpu.roll(g, rx - 1, 0))
            down = jnp.where(lane_ids == 0, g, pltpu.roll(g, 1, 1))
            up = jnp.where(lane_ids == ry - 1, g, pltpu.roll(g, ry - 1, 1))
            smooth = (g - below) + (g - above) + (g - left) + (g - right) + (g - down) + (g - up)
            grad_ref[c, z] = (2.0 * TV_WEIGHT) * smooth

    wait_received(wholes_ref, whole_sem.at[1], behind_count, reach)
    folded = [[] for _ in range(4)]
    fold_t = jnp.ones((rx, ry), jnp.float32)
    fold_c = [jnp.zeros((rx, ry), jnp.float32)] * 3
    for k in range(1, reach + 1):
        there = slab >= k
        t = wholes_ref[k - 1, 3]
        fold_c = [jnp.where(there, wholes_ref[k - 1, c] + t * fold_c[c], 0.0) for c in range(3)]
        fold_t = jnp.where(there, t * fold_t, 0.0)
        for c in range(4):
            folded[c].append(fold_c[c] if c < 3 else fold_t)
    folds = jnp.concatenate([f for fs in folded for f in fs], axis=0)
    fold_high = folds.astype(jnp.bfloat16)
    fold_low = (folds - fold_high.astype(jnp.float32)).astype(jnp.bfloat16)
    step_rows = reach * rx
    step_ids = lax.broadcasted_iota(jnp.int32, (step_rows, chunk), 0)
    row_ids16 = row_ids.astype(jnp.float32).astype(jnp.bfloat16)
    none = jnp.zeros((), jnp.bfloat16)
    lags = 4
    inner = min(channels, chunks)

    def scatter(*accs):
        sums_acc = [accs[q * 4:][:4] for q in units]
        accs = accs[4 * len(units):]
        steps = [[accs[b * len(units) + q] for q in units] for b in range(lags)]

        def columns(j, q):
            return onehot_ref[:, pl.ds(j * chunk + q * WIDTH, WIDTH)]

        for j in range(chunks):
            at = pl.ds(j * chunk, chunk)
            for q in units:
                pltpu.matmul_push_rhs(columns(j, q), j % 2, q)
            for half, lhs in enumerate((fold_high, fold_low)):
                for q in units:
                    pltpu.matmul_acc_lhs(steps[j % lags][q], lhs, None if half else j % 2)
            behind = slab - start_ref[:, at]
            mask = step_ids == (behind - 1) * rx + pix_ref[:, at] // ry
            u = jnp.concatenate([pltpu.matmul_pop(steps[j % lags][q]) for q in units], axis=1)
            for c in range(4):
                picked = jnp.where(mask, u[c * step_rows:(c + 1) * step_rows], 0.0)
                value = jnp.sum(picked, axis=0, keepdims=True)
                if c == 3:
                    value = jnp.where(behind <= 0, 1.0, value)
                front_ref[j, pl.ds(c, 1), :] = value

        target_load.wait()
        for q in units:
            pltpu.matmul_push_rhs(columns(0, q), 0, q, transpose=True)
        for j in range(chunks):
            for n in range(1, reach + 1):
                size = far_ref.shape[1] if n == reach else 4 * n
                pl.when(ahead_count == n)(waiter(far_ref.at[j, pl.ds(0, size)], part_recv.at[j]).wait_recv)
            if j == chunks - inner:
                wait_received(xhalo_ref, halo_recv.at[1], beside_count, 2)
            if j == 0 and direct(ns, nt):
                for k in (-reach, reach):
                    @pl.when(inside(slab + k))
                    def _(k=k):
                        pl.semaphore_signal(
                            ready_sem, inc=1, device_id={"slab": slab + k}, device_id_type=MESH)
            at = pl.ds(j * chunk, chunk)
            front_c = front_ref[j, pl.ds(0, 3), :]
            front_t = front_ref[j, pl.ds(3, 1), :]
            beyond = far_ref[j, pl.ds(4 * (reach - 1), 3), 0, :]
            beyond = jnp.where(slab + reach < ns, beyond, BACKGROUND)
            for k in range(reach - 1, 0, -1):
                pc = far_ref[j, pl.ds(4 * (k - 1), 3), 0, :]
                pt = far_ref[j, 4 * k - 1]
                beyond = jnp.where(slab + k < ns, pc + pt * beyond, beyond)
            pc = own_ref[j, pl.ds(0, 3), 0, :]
            pt = own_ref[j, 3]
            rendered = front_c + front_t * (pc + pt * beyond)
            residual = RENDER_WEIGHT * (rendered - target_ref[:, at])
            color_cot = front_t * residual
            trans_cot = front_t * jnp.sum(residual * beyond, axis=0, keepdims=True)
            mask = row_ids16 == row_ref[:, at].astype(jnp.float32).astype(jnp.bfloat16)
            for c in range(4):
                cot = color_cot[c:c + 1] if c < 3 else trans_cot
                top = cot.astype(jnp.bfloat16)
                low = (cot - top.astype(jnp.float32)).astype(jnp.bfloat16)
                for half, part in enumerate((top, low)):
                    spread = jnp.where(mask, part, none)
                    for q in units:
                        fresh = j % 2 if c == 0 and half == 0 else None
                        pltpu.matmul_acc_lhs(
                            sums_acc[q][c], spread[:, q * WIDTH:(q + 1) * WIDTH], fresh)
            if j + 1 < chunks:
                for q in units:
                    pltpu.matmul_push_rhs(columns(j + 1, q), (j + 1) % 2, q, transpose=True)
            if j >= chunks - inner:
                for c in range((j - chunks + inner) * channels // inner, (j + 1 - chunks + inner) * channels // inner):
                    smooth_planes(c, range(1, depth - 1))
        wait_received(zhalo_ref, halo_recv.at[0], level_count, 2)
        for c in range(channels):
            smooth_planes(c, (0, depth - 1) if depth > 1 else (0,))
        for c in range(4):
            table_ref[pl.ds(c * rows, rows), :] = sum(pltpu.matmul_pop(sums_acc[q][c]) for q in units)

    pl.run_scoped(scatter, *[
        pltpu.ACC(q)((rows, WIDTH), jnp.float32) for q in units for _ in range(4)
    ], *[
        pltpu.ACC(q)((4 * step_rows, WIDTH), jnp.float32) for _ in range(lags) for q in units
    ])

    zero = jnp.zeros((rx, ry), jnp.float32)
    suffix = [zero, zero, zero]
    later = zero
    squares = zero
    for z in range(depth - 1, -1, -1):
        w = weight_ref[z]
        after = trans_ref[z]
        later = later + after * table_ref[pl.ds(3 * rows + z * rx, rx), :]
        dw = zero
        for c in range(3):
            suffix[c] = suffix[c] + table_ref[pl.ds(c * rows + z * rx, rx), :]
            col = sig_ref[c + 1, z]
            dw = dw + col * suffix[c]
            out = grad_ref[c + 1, z] + w * suffix[c] * (col * (1.0 - col))
            grad_ref[c + 1, z] = out
            squares = squares + out * out
        dtau = after * dw - later
        later = later + w * dw
        out = grad_ref[0, z] + dtau * (sig_ref[0, z] * span)
        grad_ref[0, z] = out
        squares = squares + out * out

    local = jnp.sum(squares)

    def norm_copy(phase, slots, peer=None):
        src = nsend_ref.at[pl.ds(phase, 1)] if peer else nrecv_ref.at[slots]
        return pltpu.make_async_remote_copy(
            src_ref=src, dst_ref=nrecv_ref.at[slots],
            send_sem=norm_send.at[phase], recv_sem=norm_recv.at[phase],
            device_id=peer or tile_peer(1), device_id_type=MESH)

    if direct(ns, nt):
        far = inside(slab - reach).astype(jnp.int32) + inside(slab + reach).astype(jnp.int32)
        pl.semaphore_wait(ready_sem, far)
    value = jnp.full((1, 128), local, jnp.float32)
    base = 0
    for phase, peers in enumerate(phases):
        nsend_ref[phase] = value
        for i, peer in enumerate(peers):
            norm_copy(phase, pl.ds(base + i, 1), peer).start()
        if phase == 0:
            for copy in moment_loads:
                copy.wait()
            first_ref[...] = BETA_ONE * first_ref[...]
            second_ref[...] = BETA_TWO * second_ref[...]
            wait_sent(zhalo_ref, halo_send.at[0], level_count, 2)
            wait_sent(edge_ref, halo_send.at[1], beside_count, 2)
            wait_sent(wholes_ref, whole_sem.at[0], ahead_count, reach)
            for k in range(1, reach + 1):
                src = last_ref if k == reach else own_ref
                pl.when(slab >= k)(waiter(src, part_send.at[k - 1]).wait_send)
        norm_copy(phase, pl.ds(base, len(peers))).wait_recv()
        value = value + jnp.sum(nrecv_ref[pl.ds(base, len(peers)), 0, :], axis=0, keepdims=True)
        base += len(peers)
    limit = CLIP_RMS * math.sqrt(4.0 * total_depth * (rx * nt) * ry)
    scale_ref[...] = limit / jnp.maximum(jnp.sqrt(value), limit)
    base = 0
    for phase, peers in enumerate(phases):
        norm_copy(phase, pl.ds(base, len(peers))).wait_send()
        base += len(peers)


def split(depth):
    return math.gcd(depth, PIECES)


def span_reach(ns):
    return max(ns // 2, 1)


def direct(ns, nt):
    return ns * nt <= DIRECT_LIMIT


def adam_kernel(
    grid_ref, first_ref, second_ref, grad_ref, scale_ref,
    grid_hbm, first_hbm, second_hbm, grid_out, first_out, second_out, sem,
):
    channels, depth, rx, ry = grid_ref.shape
    gain = (1.0 - BETA_ONE**STEP) / LEARN_RATE
    slope = gain / math.sqrt(1.0 - BETA_TWO**STEP)
    offset = gain * EPSILON
    scale = jnp.broadcast_to(scale_ref[0:1, 0:1], (rx, ry))
    linear = (1.0 - BETA_ONE) * scale
    square = (1.0 - BETA_TWO) * scale * scale
    pairs = ((first_out, first_hbm), (second_out, second_hbm), (grid_out, grid_hbm))
    pieces = split(depth)
    for c in range(channels):
        for p in range(pieces):
            planes = range(p * depth // pieces, (p + 1) * depth // pieces)
            for z in planes:
                g = grad_ref[c, z]
                first = first_ref[c, z] + linear * g
                second = second_ref[c, z] + square * g * g
                first_out[c, z] = first
                second_out[c, z] = second
                root = second * lax.rsqrt(second)
                grid_out[c, z] = grid_ref[c, z] - first / (root * slope + offset)
            at = pl.ds(p * depth // pieces, depth // pieces)
            for i, (a, b) in enumerate(pairs):
                pltpu.make_async_copy(a.at[c, at], b.at[c, at], sem.at[i]).start()
    for i, (a, b) in enumerate(pairs):
        pltpu.make_async_copy(a, b, sem.at[i]).wait()


def per_device(voxel_grid, first_moment, second_moment, pixel_index, start_slab, ray_count, target):
    ns = lax.axis_size("slab")
    nt = lax.axis_size("tile")
    channels, depth, rx, ry = voxel_grid.shape
    rays = pixel_index.shape[0]
    chunk = math.gcd(rays, CHUNK)
    chunks = rays // chunk
    rows = depth * rx
    reach = span_reach(ns)
    phases = 1 if direct(ns, nt) else 2
    messages = ns * nt - 1 if direct(ns, nt) else nt + ns - 2
    f32 = jnp.float32
    vmem = pl.BlockSpec(memory_space=pltpu.VMEM)
    hbm = pl.BlockSpec(memory_space=pltpu.HBM)
    cells = jax.ShapeDtypeStruct(voxel_grid.shape, f32)
    staged = pl.pallas_call(
        functools.partial(kernel, ns, nt, chunk),
        out_shape=(cells, cells, cells, cells, jax.ShapeDtypeStruct((1, 128), f32)),
        in_specs=[hbm] * 7,
        out_specs=(vmem,) * 5,
        scratch_shapes=[
            pltpu.VMEM((3, 1, rays), jnp.int32),
            pltpu.VMEM(target.shape, f32),
            pltpu.VMEM((channels * rows, 2 * ry), jnp.bfloat16),
            pltpu.VMEM((depth, rx, ry), f32),
            pltpu.VMEM((depth, rx, ry), f32),
            pltpu.VMEM((channels, depth, rx, ry), f32),
            pltpu.VMEM((ry, rays), jnp.bfloat16),
            pltpu.VMEM((1, rays), jnp.int32),
            pltpu.VMEM((channels * rows, ry), f32),
            pltpu.VMEM((4, rx, ry), f32),
            pltpu.VMEM((reach, 4, rx, ry), f32),
            pltpu.VMEM((chunks, 4, chunk), f32),
            pltpu.VMEM((chunks, 4, 1, chunk), f32),
            pltpu.VMEM((chunks, 3, 1, chunk), f32),
            pltpu.VMEM((chunks, 4 * reach - 1, 1, chunk), f32),
            pltpu.VMEM((2, channels, depth, ry), f32),
            pltpu.VMEM((2, channels, depth, ry), f32),
            pltpu.VMEM((2, channels, rx, ry), f32),
            pltpu.VMEM((2, 1, 128), f32),
            pltpu.VMEM((messages, 1, 128), f32),
            pltpu.SemaphoreType.DMA((2,)),
            pltpu.SemaphoreType.DMA((reach,)),
            pltpu.SemaphoreType.DMA((chunks,)),
            pltpu.SemaphoreType.REGULAR,
            pltpu.SemaphoreType.DMA((2,)),
            pltpu.SemaphoreType.DMA((2,)),
            pltpu.SemaphoreType.DMA((phases,)),
            pltpu.SemaphoreType.DMA((phases,)),
            pltpu.SemaphoreType.DMA((5,)),
        ],
        compiler_params=pltpu.CompilerParams(
            collective_id=0, has_side_effects=True, vmem_limit_bytes=32 * 1024 * 1024
        ),
        name="render_step",
    )(*(pltpu.with_memory_space_constraint(a, pltpu.HBM) for a in (
        voxel_grid,
        first_moment,
        second_moment,
        pixel_index.reshape(1, rays),
        start_slab.reshape(1, rays),
        ray_count.reshape(1, rays),
        target,
    )))
    return pl.pallas_call(
        adam_kernel,
        out_shape=(cells, cells, cells),
        in_specs=[vmem] * 5,
        out_specs=(hbm, hbm, hbm),
        scratch_shapes=[
            pltpu.VMEM(voxel_grid.shape, f32),
            pltpu.VMEM(voxel_grid.shape, f32),
            pltpu.VMEM(voxel_grid.shape, f32),
            pltpu.SemaphoreType.DMA((3,)),
        ],
        compiler_params=pltpu.CompilerParams(vmem_limit_bytes=32 * 1024 * 1024),
        name="adam",
    )(*staged)


def solution(mesh):
    cells = P(None, "slab", "tile", None)
    return jax.shard_map(
        per_device,
        mesh=mesh,
        in_specs=(cells, cells, cells, P("tile"), P("tile"), P("tile"), P(None, "tile")),
        out_specs=(cells, cells, cells),
        check_vma=False,
    )
```

```python
import functools
import math

import jax
import jax.numpy as jnp
from jax import lax
from jax.experimental import pallas as pl
from jax.experimental.pallas import tpu as pltpu
from jax.sharding import PartitionSpec as P

STEP = 20
RENDER_WEIGHT = 1000.0
TV_WEIGHT = 0.05
BACKGROUND = 1.0
STEP_SPAN = 4.0
CLIP_RMS = 0.25
LEARN_RATE = 0.02
BETA_ONE = 0.9
BETA_TWO = 0.99
EPSILON = 1e-08
CHUNK = 512
WIDTH = 256
OPENING = 1
FINE = jnp.float8_e4m3fn
TABLE_SCALE = 65536.0
COTANGENT_SCALE = 32.0
PIECES = 4
DIRECT_LIMIT = 64
MESH = pl.DeviceIdType.MESH


def kernel(
    ns, nt, chunk,
    grid_hbm, first_hbm, second_hbm, pix_hbm, start_hbm, count_hbm, target_hbm,
    grid_ref, first_ref, second_ref, grad_ref, scale_ref,
    ints_ref, target_ref,
    high_ref, low_ref, trans_ref, weight_ref, sig_ref, onehot_ref, row_ref, table_ref,
    whole_ref, wholes_ref, front_ref, own_ref, last_ref, far_ref,
    edge_ref, xhalo_ref, zhalo_ref, nsend_ref, nrecv_ref,
    whole_sem, part_send, part_recv, ready_sem, halo_send, halo_recv, norm_send, norm_recv, load_sem,
):
    channels, depth, rx, ry = grid_ref.shape
    rays = ints_ref.shape[2]
    pix_ref, start_ref, count_ref = (ints_ref.at[i] for i in range(3))
    chunks = rays // chunk
    total_depth = depth * ns
    reach = span_reach(ns)
    span = STEP_SPAN / total_depth
    rows = depth * rx
    slab = lax.axis_index("slab")
    tile = lax.axis_index("tile")

    def slab_peer(d):
        return {"slab": lax.rem(slab + d, ns)}

    def tile_peer(d):
        return {"tile": lax.rem(tile + d, nt)}

    if direct(ns, nt):
        phases = [[
            {"slab": lax.rem(slab + k // nt, ns), "tile": lax.rem(tile + k % nt, nt)}
            for k in range(1, ns * nt)
        ]]
        near = reach
    else:
        phases = [[tile_peer(d) for d in range(1, nt)], [slab_peer(d) for d in range(1, ns)]]
        near = ns - 1
    offsets = [k for k in range(-near, near + 1) if k]

    def inside(s):
        return (s >= 0) & (s < ns)

    pieces = split(depth)
    step = depth // pieces
    grid_load = pltpu.make_async_copy(grid_hbm, grid_ref, load_sem.at[0])
    for c in range(channels):
        for p in range(pieces):
            at = pl.ds(p * step, step)
            pltpu.make_async_copy(grid_hbm.at[c, at], grid_ref.at[c, at], load_sem.at[0]).start()
    for i, a in enumerate((pix_hbm, start_hbm, count_hbm)):
        pltpu.make_async_copy(a, ints_ref.at[i], load_sem.at[1]).start()
    ints_load = pltpu.make_async_copy(ints_ref, ints_ref, load_sem.at[1])
    target_load = pltpu.make_async_copy(target_hbm, target_ref, load_sem.at[2])
    target_load.start()
    moment_loads = [
        pltpu.make_async_copy(first_hbm, first_ref, load_sem.at[3]),
        pltpu.make_async_copy(second_hbm, second_ref, load_sem.at[4]),
    ]

    barrier = pltpu.get_barrier_semaphore()
    for d in range(1, nt):
        pl.semaphore_signal(barrier, inc=1, device_id=tile_peer(d), device_id_type=MESH)
    greeters = nt - 1
    for k in offsets:
        @pl.when(inside(slab + k))
        def _(k=k):
            pl.semaphore_signal(
                barrier, inc=1, device_id={"slab": slab + k}, device_id_type=MESH)
        greeters = greeters + inside(slab + k).astype(jnp.int32)

    grid_load.wait()
    for copy in moment_loads:
        copy.start()
    edge_ref[0] = grid_ref[:, :, rx - 1, :]
    edge_ref[1] = grid_ref[:, :, 0, :]

    total = jnp.zeros((rx, ry), jnp.float32)
    before = jnp.ones((rx, ry), jnp.float32)
    sums = [jnp.zeros((rx, ry), jnp.float32) for _ in range(3)]
    for z in range(depth):
        s = grid_ref[0, z]
        e = jnp.exp(-jnp.abs(s))
        tau = (jnp.maximum(s, 0.0) + jnp.log1p(e)) * span
        sig_ref[0, z] = jnp.where(s >= 0, 1.0, e) / (1.0 + e)
        total = total + tau
        after = jnp.exp(-total)
        w = before * (1.0 - jnp.exp(-tau))
        before = after
        trans_ref[z] = after
        weight_ref[z] = w
        for c in range(3):
            col = 1.0 / (1.0 + jnp.exp(-grid_ref[c + 1, z]))
            sig_ref[c + 1, z] = col
            sums[c] = sums[c] + w * col
            table_ref[pl.ds(c * rows + z * rx, rx), :] = sums[c]
        table_ref[pl.ds(3 * rows + z * rx, rx), :] = after
    for c in range(3):
        whole_ref[c] = sums[c]
    whole_ref[3] = before
    full = TABLE_SCALE * table_ref[...]
    high = full.astype(jnp.bfloat16)
    high_ref[...] = high
    low_ref[...] = (full - high.astype(jnp.float32)).astype(FINE)

    def waiter(ref, sem):
        return pltpu.make_async_remote_copy(
            src_ref=ref, dst_ref=ref, send_sem=sem, recv_sem=sem,
            device_id=tile_peer(1), device_id_type=MESH)

    def wait_sent(ref, sem, count, most):
        for n in range(1, most + 1):
            pl.when(count == n)(waiter(ref.at[pl.ds(0, n)], sem).wait_send)

    def wait_received(ref, sem, count, most):
        for n in range(1, most + 1):
            pl.when(count == n)(waiter(ref.at[pl.ds(0, n)], sem).wait_recv)

    behind_count = jnp.minimum(slab, reach)
    ahead_count = jnp.minimum(ns - 1 - slab, reach)
    beside_count = (tile < nt - 1).astype(jnp.int32) + (tile > 0).astype(jnp.int32)
    level_count = (slab < ns - 1).astype(jnp.int32) + (slab > 0).astype(jnp.int32)

    def whole_copy(k):
        return pltpu.make_async_remote_copy(
            src_ref=whole_ref, dst_ref=wholes_ref.at[k - 1],
            send_sem=whole_sem.at[0], recv_sem=whole_sem.at[1],
            device_id=slab_peer(k), device_id_type=MESH)

    def halo_copy(src, dst, i, peer):
        return pltpu.make_async_remote_copy(
            src_ref=src, dst_ref=dst, send_sem=halo_send.at[i // 2], recv_sem=halo_recv.at[i // 2],
            device_id=peer, device_id_type=MESH)

    halos = [
        (halo_copy(grid_ref.at[:, depth - 1], zhalo_ref.at[0], 0, slab_peer(1)), slab < ns - 1),
        (halo_copy(grid_ref.at[:, 0], zhalo_ref.at[1], 1, slab_peer(ns - 1)), slab > 0),
        (halo_copy(edge_ref.at[0], xhalo_ref.at[0], 2, tile_peer(1)), tile < nt - 1),
        (halo_copy(edge_ref.at[1], xhalo_ref.at[1], 3, tile_peer(nt - 1)), tile > 0),
    ]
    def part_copy(k, j):
        src = last_ref if k == reach else own_ref
        return pltpu.make_async_remote_copy(
            src_ref=src.at[j], dst_ref=far_ref.at[j, pl.ds(4 * (k - 1), src.shape[1])],
            send_sem=part_send.at[k - 1], recv_sem=part_recv.at[j],
            device_id=slab_peer(ns - k), device_id_type=MESH)

    y_ids = lax.broadcasted_iota(jnp.int32, (ry, chunk), 0).astype(jnp.float32).astype(jnp.bfloat16)
    row_ids = lax.broadcasted_iota(jnp.int32, (rows, chunk), 0)

    ints_load.wait()
    units = range(chunk // WIDTH)

    def enter():
        pl.semaphore_wait(barrier, greeters)
        for k in range(reach, 0, -1):
            pl.when(slab + k < ns)(whole_copy(k).start)
        for copy, sends in halos[2:]:
            pl.when(sends)(copy.start)

    opening = min(OPENING, chunks)

    def gather(*accs):
        banks = [[accs[(b * len(units) + q) * 4:][:4] for q in units] for b in range(2)]
        for j in range(chunks + 1):
            if j < chunks:
                at = pl.ds(j * chunk, chunk)
                pix = pix_ref[:, at]
                start = start_ref[:, at]
                px = pix // ry
                py = (pix - px * ry).astype(jnp.float32).astype(jnp.bfloat16)
                length = jnp.clip((start - slab) * depth + count_ref[:, at], 0, depth)
                length = jnp.where(slab >= start, length, 0)
                row_ref[:, at] = jnp.where(length > 0, (length - 1) * rx + px, -1)
                hot = jnp.where(y_ids == py, jnp.ones((), jnp.bfloat16), jnp.zeros((), jnp.bfloat16))
                hot = hot.astype(FINE)
                onehot_ref[:, at] = hot
                for q in units:
                    for half in range(2):
                        pltpu.matmul_push_rhs(hot[:, q * WIDTH:(q + 1) * WIDTH], half, q)
                for half, side in enumerate((high_ref, low_ref)):
                    for c in range(4):
                        lhs = side[pl.ds(c * rows, rows), :]
                        for q in units:
                            pltpu.matmul_acc_lhs(banks[j % 2][q][c], lhs, None if c else half)
            if j == 0:
                continue
            i = j - 1
            row = row_ref[:, pl.ds(i * chunk, chunk)]
            mask = row_ids == row
            for c in range(4):
                u = jnp.concatenate([pltpu.matmul_pop(banks[i % 2][q][c]) for q in units], axis=1)
                part = jnp.sum(jnp.where(mask, u, 0.0), axis=0, keepdims=True)
                part = part * (1.0 / TABLE_SCALE)
                if c == 3:
                    part = jnp.where(row < 0, 1.0, part)
                own_ref[i, c] = part
            for c in range(3):
                last_ref[i, c] = own_ref[i, c] + BACKGROUND * part
            if j < opening:
                continue
            if j == opening:
                enter()
            for n in range(0 if j == opening else i, j):
                for k in range(1, reach + 1):
                    pl.when(slab >= k)(part_copy(k, n).start)

    pl.run_scoped(gather, *[
        pltpu.ACC(q)((rows, WIDTH), jnp.float32)
        for _ in range(2) for q in units for _ in range(4)
    ])

    for copy, sends in halos[:2]:
        pl.when(sends)(copy.start)
    x_ids = lax.broadcasted_iota(jnp.int32, (rx, ry), 0)
    lane_ids = lax.broadcasted_iota(jnp.int32, (rx, ry), 1)
    first_x = tile == 0
    last_x = tile == nt - 1
    def smooth_planes(c, planes):
        for z in planes:
            g = grid_ref[c, z]
            if z > 0:
                below = grid_ref[c, z - 1]
            else:
                below = jnp.where(slab > 0, zhalo_ref[0, c], g)
            if z < depth - 1:
                above = grid_ref[c, z + 1]
            else:
                above = jnp.where(slab < ns - 1, zhalo_ref[1, c], g)
            xl = jnp.broadcast_to(xhalo_ref[0, c, pl.ds(z, 1), :], (rx, ry))
            xh = jnp.broadcast_to(xhalo_ref[1, c, pl.ds(z, 1), :], (rx, ry))
            xl = jnp.where(first_x, g, xl)
            xh = jnp.where(last_x, g, xh)
            left = jnp.where(x_ids == 0, xl, pltpu.roll(g, 1, 0))
            right = jnp.where(x_ids == rx - 1, xh, pltpu.roll(g, rx - 1, 0))
            down = jnp.where(lane_ids == 0, g, pltpu.roll(g, 1, 1))
            up = jnp.where(lane_ids == ry - 1, g, pltpu.roll(g, ry - 1, 1))
            smooth = (g - below) + (g - above) + (g - left) + (g - right) + (g - down) + (g - up)
            grad_ref[c, z] = (2.0 * TV_WEIGHT) * smooth

    wait_received(wholes_ref, whole_sem.at[1], behind_count, reach)
    folded = [[] for _ in range(4)]
    fold_t = jnp.ones((rx, ry), jnp.float32)
    fold_c = [jnp.zeros((rx, ry), jnp.float32)] * 3
    for k in range(1, reach + 1):
        there = slab >= k
        t = wholes_ref[k - 1, 3]
        fold_c = [jnp.where(there, wholes_ref[k - 1, c] + t * fold_c[c], 0.0) for c in range(3)]
        fold_t = jnp.where(there, t * fold_t, 0.0)
        for c in range(4):
            folded[c].append(fold_c[c] if c < 3 else fold_t)
    folds = jnp.concatenate([f for fs in folded for f in fs], axis=0)
    fold_high = folds.astype(jnp.bfloat16)
    fold_low = (folds - fold_high.astype(jnp.float32)).astype(jnp.bfloat16)
    step_rows = reach * rx
    step_ids = lax.broadcasted_iota(jnp.int32, (step_rows, chunk), 0)
    row_ids16 = row_ids.astype(jnp.float32).astype(jnp.bfloat16)
    none = jnp.zeros((), jnp.bfloat16)
    lags = 4
    inner = min(channels, chunks)

    def scatter(*accs):
        sums_acc = [accs[q * 4:][:4] for q in units]
        accs = accs[4 * len(units):]
        steps = [[accs[b * len(units) + q] for q in units] for b in range(lags)]

        def columns(j, q):
            return onehot_ref[:, pl.ds(j * chunk + q * WIDTH, WIDTH)]

        for j in range(chunks):
            at = pl.ds(j * chunk, chunk)
            for q in units:
                pltpu.matmul_push_rhs(columns(j, q), j % 2, q)
            for half, lhs in enumerate((fold_high, fold_low)):
                for q in units:
                    pltpu.matmul_acc_lhs(steps[j % lags][q], lhs, None if half else j % 2)
            behind = slab - start_ref[:, at]
            mask = step_ids == (behind - 1) * rx + pix_ref[:, at] // ry
            u = jnp.concatenate([pltpu.matmul_pop(steps[j % lags][q]) for q in units], axis=1)
            for c in range(4):
                picked = jnp.where(mask, u[c * step_rows:(c + 1) * step_rows], 0.0)
                value = jnp.sum(picked, axis=0, keepdims=True)
                if c == 3:
                    value = jnp.where(behind <= 0, 1.0, value)
                front_ref[j, pl.ds(c, 1), :] = value

        target_load.wait()
        for q in units:
            for half in range(2):
                pltpu.matmul_push_rhs(columns(0, q), half, q, transpose=True)
        for j in range(chunks):
            for n in range(1, reach + 1):
                size = far_ref.shape[1] if n == reach else 4 * n
                pl.when(ahead_count == n)(waiter(far_ref.at[j, pl.ds(0, size)], part_recv.at[j]).wait_recv)
            if j == chunks - inner:
                wait_received(xhalo_ref, halo_recv.at[1], beside_count, 2)
            if j == 0 and direct(ns, nt):
                for k in (-reach, reach):
                    @pl.when(inside(slab + k))
                    def _(k=k):
                        pl.semaphore_signal(
                            ready_sem, inc=1, device_id={"slab": slab + k}, device_id_type=MESH)
            at = pl.ds(j * chunk, chunk)
            front_c = front_ref[j, pl.ds(0, 3), :]
            front_t = front_ref[j, pl.ds(3, 1), :]
            beyond = far_ref[j, pl.ds(4 * (reach - 1), 3), 0, :]
            beyond = jnp.where(slab + reach < ns, beyond, BACKGROUND)
            for k in range(reach - 1, 0, -1):
                pc = far_ref[j, pl.ds(4 * (k - 1), 3), 0, :]
                pt = far_ref[j, 4 * k - 1]
                beyond = jnp.where(slab + k < ns, pc + pt * beyond, beyond)
            pc = own_ref[j, pl.ds(0, 3), 0, :]
            pt = own_ref[j, 3]
            rendered = front_c + front_t * (pc + pt * beyond)
            residual = (COTANGENT_SCALE * RENDER_WEIGHT) * (rendered - target_ref[:, at])
            color_cot = front_t * residual
            trans_cot = front_t * jnp.sum(residual * beyond, axis=0, keepdims=True)
            mask = row_ids16 == row_ref[:, at].astype(jnp.float32).astype(jnp.bfloat16)
            cots = [color_cot[c:c + 1] for c in range(3)] + [trans_cot]
            tops = [cot.astype(jnp.bfloat16) for cot in cots]
            lows = [(cot - top.astype(jnp.float32)).astype(jnp.bfloat16) for cot, top in zip(cots, tops)]
            for half, side in enumerate((tops, lows)):
                for c in range(4):
                    spread = jnp.where(mask, side[c], none)
                    if half:
                        spread = spread.astype(FINE)
                    for q in units:
                        pltpu.matmul_acc_lhs(
                            sums_acc[q][c], spread[:, q * WIDTH:(q + 1) * WIDTH], None if c else half)
            if j + 1 < chunks:
                for q in units:
                    for half in range(2):
                        pltpu.matmul_push_rhs(columns(j + 1, q), half, q, transpose=True)
            if j >= chunks - inner:
                for c in range((j - chunks + inner) * channels // inner, (j + 1 - chunks + inner) * channels // inner):
                    smooth_planes(c, range(1, depth - 1))
        wait_received(zhalo_ref, halo_recv.at[0], level_count, 2)
        for c in range(channels):
            smooth_planes(c, (0, depth - 1) if depth > 1 else (0,))
        for c in range(4):
            gathered = sum(pltpu.matmul_pop(sums_acc[q][c]) for q in units)
            table_ref[pl.ds(c * rows, rows), :] = (1.0 / COTANGENT_SCALE) * gathered

    pl.run_scoped(scatter, *[
        pltpu.ACC(q)((rows, WIDTH), jnp.float32) for q in units for _ in range(4)
    ], *[
        pltpu.ACC(q)((4 * step_rows, WIDTH), jnp.float32) for _ in range(lags) for q in units
    ])

    zero = jnp.zeros((rx, ry), jnp.float32)
    suffix = [zero, zero, zero]
    later = zero
    squares = zero
    for z in range(depth - 1, -1, -1):
        w = weight_ref[z]
        after = trans_ref[z]
        later = later + after * table_ref[pl.ds(3 * rows + z * rx, rx), :]
        dw = zero
        for c in range(3):
            suffix[c] = suffix[c] + table_ref[pl.ds(c * rows + z * rx, rx), :]
            col = sig_ref[c + 1, z]
            dw = dw + col * suffix[c]
            out = grad_ref[c + 1, z] + w * suffix[c] * (col * (1.0 - col))
            grad_ref[c + 1, z] = out
            squares = squares + out * out
        dtau = after * dw - later
        later = later + w * dw
        out = grad_ref[0, z] + dtau * (sig_ref[0, z] * span)
        grad_ref[0, z] = out
        squares = squares + out * out

    local = jnp.sum(squares)

    def norm_copy(phase, slots, peer=None):
        src = nsend_ref.at[pl.ds(phase, 1)] if peer else nrecv_ref.at[slots]
        return pltpu.make_async_remote_copy(
            src_ref=src, dst_ref=nrecv_ref.at[slots],
            send_sem=norm_send.at[phase], recv_sem=norm_recv.at[phase],
            device_id=peer or tile_peer(1), device_id_type=MESH)

    if direct(ns, nt):
        far = inside(slab - reach).astype(jnp.int32) + inside(slab + reach).astype(jnp.int32)
        pl.semaphore_wait(ready_sem, far)
    value = jnp.full((1, 128), local, jnp.float32)
    base = 0
    for phase, peers in enumerate(phases):
        nsend_ref[phase] = value
        for i, peer in enumerate(peers):
            norm_copy(phase, pl.ds(base + i, 1), peer).start()
        if phase == 0:
            for copy in moment_loads:
                copy.wait()
            first_ref[...] = BETA_ONE * first_ref[...]
            second_ref[...] = BETA_TWO * second_ref[...]
            wait_sent(zhalo_ref, halo_send.at[0], level_count, 2)
            wait_sent(edge_ref, halo_send.at[1], beside_count, 2)
            wait_sent(wholes_ref, whole_sem.at[0], ahead_count, reach)
            for k in range(1, reach + 1):
                src = last_ref if k == reach else own_ref
                pl.when(slab >= k)(waiter(src, part_send.at[k - 1]).wait_send)
        norm_copy(phase, pl.ds(base, len(peers))).wait_recv()
        value = value + jnp.sum(nrecv_ref[pl.ds(base, len(peers)), 0, :], axis=0, keepdims=True)
        base += len(peers)
    limit = CLIP_RMS * math.sqrt(4.0 * total_depth * (rx * nt) * ry)
    scale_ref[...] = limit / jnp.maximum(jnp.sqrt(value), limit)
    base = 0
    for phase, peers in enumerate(phases):
        norm_copy(phase, pl.ds(base, len(peers))).wait_send()
        base += len(peers)


def split(depth):
    return math.gcd(depth, PIECES)


def span_reach(ns):
    return max(ns // 2, 1)


def direct(ns, nt):
    return ns * nt <= DIRECT_LIMIT


def adam_kernel(
    grid_ref, first_ref, second_ref, grad_ref, scale_ref,
    grid_hbm, first_hbm, second_hbm, grid_out, first_out, second_out, sem,
):
    channels, depth, rx, ry = grid_ref.shape
    gain = (1.0 - BETA_ONE**STEP) / LEARN_RATE
    slope = gain / math.sqrt(1.0 - BETA_TWO**STEP)
    offset = gain * EPSILON
    scale = jnp.broadcast_to(scale_ref[0:1, 0:1], (rx, ry))
    linear = (1.0 - BETA_ONE) * scale
    square = (1.0 - BETA_TWO) * scale * scale
    pairs = ((first_out, first_hbm), (second_out, second_hbm), (grid_out, grid_hbm))
    pieces = split(depth)
    for c in range(channels):
        for p in range(pieces):
            planes = range(p * depth // pieces, (p + 1) * depth // pieces)
            for z in planes:
                g = grad_ref[c, z]
                first = first_ref[c, z] + linear * g
                second = second_ref[c, z] + square * g * g
                first_out[c, z] = first
                second_out[c, z] = second
                root = second * lax.rsqrt(second)
                grid_out[c, z] = grid_ref[c, z] - first / (root * slope + offset)
            at = pl.ds(p * depth // pieces, depth // pieces)
            for i, (a, b) in enumerate(pairs):
                pltpu.make_async_copy(a.at[c, at], b.at[c, at], sem.at[i]).start()
    for i, (a, b) in enumerate(pairs):
        pltpu.make_async_copy(a, b, sem.at[i]).wait()


def per_device(voxel_grid, first_moment, second_moment, pixel_index, start_slab, ray_count, target):
    ns = lax.axis_size("slab")
    nt = lax.axis_size("tile")
    channels, depth, rx, ry = voxel_grid.shape
    rays = pixel_index.shape[0]
    chunk = math.gcd(rays, CHUNK)
    chunks = rays // chunk
    rows = depth * rx
    reach = span_reach(ns)
    phases = 1 if direct(ns, nt) else 2
    messages = ns * nt - 1 if direct(ns, nt) else nt + ns - 2
    f32 = jnp.float32
    vmem = pl.BlockSpec(memory_space=pltpu.VMEM)
    hbm = pl.BlockSpec(memory_space=pltpu.HBM)
    cells = jax.ShapeDtypeStruct(voxel_grid.shape, f32)
    staged = pl.pallas_call(
        functools.partial(kernel, ns, nt, chunk),
        out_shape=(cells, cells, cells, cells, jax.ShapeDtypeStruct((1, 128), f32)),
        in_specs=[hbm] * 7,
        out_specs=(vmem,) * 5,
        scratch_shapes=[
            pltpu.VMEM((3, 1, rays), jnp.int32),
            pltpu.VMEM(target.shape, f32),
            pltpu.VMEM((channels * rows, ry), jnp.bfloat16),
            pltpu.VMEM((channels * rows, ry), FINE),
            pltpu.VMEM((depth, rx, ry), f32),
            pltpu.VMEM((depth, rx, ry), f32),
            pltpu.VMEM((channels, depth, rx, ry), f32),
            pltpu.VMEM((ry, rays), FINE),
            pltpu.VMEM((1, rays), jnp.int32),
            pltpu.VMEM((channels * rows, ry), f32),
            pltpu.VMEM((4, rx, ry), f32),
            pltpu.VMEM((reach, 4, rx, ry), f32),
            pltpu.VMEM((chunks, 4, chunk), f32),
            pltpu.VMEM((chunks, 4, 1, chunk), f32),
            pltpu.VMEM((chunks, 3, 1, chunk), f32),
            pltpu.VMEM((chunks, 4 * reach - 1, 1, chunk), f32),
            pltpu.VMEM((2, channels, depth, ry), f32),
            pltpu.VMEM((2, channels, depth, ry), f32),
            pltpu.VMEM((2, channels, rx, ry), f32),
            pltpu.VMEM((2, 1, 128), f32),
            pltpu.VMEM((messages, 1, 128), f32),
            pltpu.SemaphoreType.DMA((2,)),
            pltpu.SemaphoreType.DMA((reach,)),
            pltpu.SemaphoreType.DMA((chunks,)),
            pltpu.SemaphoreType.REGULAR,
            pltpu.SemaphoreType.DMA((2,)),
            pltpu.SemaphoreType.DMA((2,)),
            pltpu.SemaphoreType.DMA((phases,)),
            pltpu.SemaphoreType.DMA((phases,)),
            pltpu.SemaphoreType.DMA((5,)),
        ],
        compiler_params=pltpu.CompilerParams(
            collective_id=0, has_side_effects=True, vmem_limit_bytes=32 * 1024 * 1024
        ),
        name="render_step",
    )(*(pltpu.with_memory_space_constraint(a, pltpu.HBM) for a in (
        voxel_grid,
        first_moment,
        second_moment,
        pixel_index.reshape(1, rays),
        start_slab.reshape(1, rays),
        ray_count.reshape(1, rays),
        target,
    )))
    return pl.pallas_call(
        adam_kernel,
        out_shape=(cells, cells, cells),
        in_specs=[vmem] * 5,
        out_specs=(hbm, hbm, hbm),
        scratch_shapes=[
            pltpu.VMEM(voxel_grid.shape, f32),
            pltpu.VMEM(voxel_grid.shape, f32),
            pltpu.VMEM(voxel_grid.shape, f32),
            pltpu.SemaphoreType.DMA((3,)),
        ],
        compiler_params=pltpu.CompilerParams(vmem_limit_bytes=32 * 1024 * 1024),
        name="adam",
    )(*staged)


def solution(mesh):
    cells = P(None, "slab", "tile", None)
    return jax.shard_map(
        per_device,
        mesh=mesh,
        in_specs=(cells, cells, cells, P("tile"), P("tile"), P("tile"), P(None, "tile")),
        out_specs=(cells, cells, cells),
        check_vma=False,
    )
```

```python
import functools
import math

import jax
import jax.numpy as jnp
from jax import lax
from jax.experimental import pallas as pl
from jax.experimental.pallas import tpu as pltpu
from jax.sharding import PartitionSpec as P

STEP = 20
RENDER_WEIGHT = 1000.0
TV_WEIGHT = 0.05
BACKGROUND = 1.0
STEP_SPAN = 4.0
CLIP_RMS = 0.25
LEARN_RATE = 0.02
BETA_ONE = 0.9
BETA_TWO = 0.99
EPSILON = 1e-08
CHUNK = 512
WIDTH = 256
OPENING = 1
FINE = jnp.float8_e4m3fn
TABLE_SCALE = 65536.0
COTANGENT_SCALE = 32.0
PIECES = 4
DIRECT_LIMIT = 64
MESH = pl.DeviceIdType.MESH


def kernel(
    ns, nt, chunk,
    grid_hbm, first_hbm, second_hbm, pix_hbm, start_hbm, count_hbm, target_hbm,
    grid_ref, first_ref, second_ref, grad_ref, scale_ref,
    ints_ref, target_ref,
    high_ref, low_ref, trans_ref, weight_ref, sig_ref, onehot_ref, row_ref, step_ref, table_ref,
    whole_ref, wholes_ref, front_ref, own_ref, last_ref, far_ref,
    edge_ref, xhalo_ref, zhalo_ref, nsend_ref, nrecv_ref,
    whole_sem, part_send, part_recv, ready_sem, halo_send, halo_recv, norm_send, norm_recv, load_sem,
):
    channels, depth, rx, ry = grid_ref.shape
    rays = ints_ref.shape[2]
    pix_ref, start_ref, count_ref = (ints_ref.at[i] for i in range(3))
    chunks = rays // chunk
    total_depth = depth * ns
    reach = span_reach(ns)
    span = STEP_SPAN / total_depth
    rows = depth * rx
    slab = lax.axis_index("slab")
    tile = lax.axis_index("tile")

    def slab_peer(d):
        return {"slab": lax.rem(slab + d, ns)}

    def tile_peer(d):
        return {"tile": lax.rem(tile + d, nt)}

    if direct(ns, nt):
        phases = [[
            {"slab": lax.rem(slab + k // nt, ns), "tile": lax.rem(tile + k % nt, nt)}
            for k in [*range(nt, ns * nt), *range(1, nt)]
        ]]
        near = reach
    else:
        phases = [[tile_peer(d) for d in range(1, nt)], [slab_peer(d) for d in range(1, ns)]]
        near = ns - 1
    offsets = [k for k in range(-near, near + 1) if k]

    def inside(s):
        return (s >= 0) & (s < ns)

    pieces = split(depth)
    step = depth // pieces
    for i, a in enumerate((pix_hbm, start_hbm, count_hbm)):
        pltpu.make_async_copy(a, ints_ref.at[i], load_sem.at[1]).start()
    ints_load = pltpu.make_async_copy(ints_ref, ints_ref, load_sem.at[1])
    grid_load = pltpu.make_async_copy(grid_hbm, grid_ref, load_sem.at[0])
    for c in range(channels):
        for p in range(pieces):
            at = pl.ds(p * step, step)
            pltpu.make_async_copy(grid_hbm.at[c, at], grid_ref.at[c, at], load_sem.at[0]).start()
    target_load = pltpu.make_async_copy(target_hbm, target_ref, load_sem.at[2])
    target_load.start()
    moment_loads = [
        pltpu.make_async_copy(first_hbm, first_ref, load_sem.at[0]),
        pltpu.make_async_copy(second_hbm, second_ref, load_sem.at[1]),
    ]

    barrier = pltpu.get_barrier_semaphore()
    for d in range(1, nt):
        pl.semaphore_signal(barrier, inc=1, device_id=tile_peer(d), device_id_type=MESH)
    greeters = nt - 1
    for k in offsets:
        @pl.when(inside(slab + k))
        def _(k=k):
            pl.semaphore_signal(
                barrier, inc=1, device_id={"slab": slab + k}, device_id_type=MESH)
        greeters = greeters + inside(slab + k).astype(jnp.int32)

    ints_load.wait()
    y_ids = lax.broadcasted_iota(jnp.int32, (ry, chunk), 0).astype(jnp.float32).astype(jnp.bfloat16)
    for j in range(chunks):
        at = pl.ds(j * chunk, chunk)
        pix = pix_ref[:, at]
        start = start_ref[:, at]
        px = pix // ry
        py = (pix - px * ry).astype(jnp.float32).astype(jnp.bfloat16)
        length = jnp.clip((start - slab) * depth + count_ref[:, at], 0, depth)
        length = jnp.where(slab >= start, length, 0)
        row_ref[:, at] = jnp.where(length > 0, (length - 1) * rx + px, -1)
        step_ref[:, at] = (slab - start - 1) * rx + px
        hot = jnp.where(y_ids == py, jnp.ones((), jnp.bfloat16), jnp.zeros((), jnp.bfloat16))
        hot = hot.astype(FINE)
        onehot_ref[:, at] = hot

    grid_load.wait()
    for copy in moment_loads:
        copy.start()
    edge_ref[0] = grid_ref[:, :, rx - 1, :]
    edge_ref[1] = grid_ref[:, :, 0, :]

    total = jnp.zeros((rx, ry), jnp.float32)
    before = jnp.ones((rx, ry), jnp.float32)
    sums = [jnp.zeros((rx, ry), jnp.float32) for _ in range(3)]
    for z in range(depth):
        s = grid_ref[0, z]
        e = jnp.exp(-jnp.abs(s))
        tau = (jnp.maximum(s, 0.0) + jnp.log(1.0 + e)) * span
        sig_ref[0, z] = jnp.where(s >= 0, 1.0, e) / (1.0 + e)
        total = total + tau
        after = jnp.exp(-total)
        w = before * (1.0 - jnp.exp(-tau))
        before = after
        trans_ref[z] = after
        weight_ref[z] = w
        for c in range(3):
            col = 1.0 / (1.0 + jnp.exp(-grid_ref[c + 1, z]))
            sig_ref[c + 1, z] = col
            sums[c] = sums[c] + w * col
            table_ref[pl.ds(c * rows + z * rx, rx), :] = sums[c]
        table_ref[pl.ds(3 * rows + z * rx, rx), :] = after
    for c in range(3):
        whole_ref[c] = sums[c]
    whole_ref[3] = before
    full = TABLE_SCALE * table_ref[...]
    high = full.astype(jnp.bfloat16)
    high_ref[...] = high
    low_ref[...] = (full - high.astype(jnp.float32)).astype(FINE)

    def waiter(ref, sem):
        return pltpu.make_async_remote_copy(
            src_ref=ref, dst_ref=ref, send_sem=sem, recv_sem=sem,
            device_id=tile_peer(1), device_id_type=MESH)

    def wait_sent(ref, sem, count, most):
        for n in range(1, most + 1):
            pl.when(count == n)(waiter(ref.at[pl.ds(0, n)], sem).wait_send)

    def wait_received(ref, sem, count, most):
        for n in range(1, most + 1):
            pl.when(count == n)(waiter(ref.at[pl.ds(0, n)], sem).wait_recv)

    behind_count = jnp.minimum(slab, reach)
    ahead_count = jnp.minimum(ns - 1 - slab, reach)
    beside_count = (tile < nt - 1).astype(jnp.int32) + (tile > 0).astype(jnp.int32)
    level_count = (slab < ns - 1).astype(jnp.int32) + (slab > 0).astype(jnp.int32)

    def whole_copy(k):
        return pltpu.make_async_remote_copy(
            src_ref=whole_ref, dst_ref=wholes_ref.at[k - 1],
            send_sem=whole_sem.at[0], recv_sem=whole_sem.at[1],
            device_id=slab_peer(k), device_id_type=MESH)

    def halo_copy(src, dst, i, peer):
        return pltpu.make_async_remote_copy(
            src_ref=src, dst_ref=dst, send_sem=halo_send.at[i // 2], recv_sem=halo_recv.at[i // 2],
            device_id=peer, device_id_type=MESH)

    halos = [
        (halo_copy(grid_ref.at[:, depth - 1], zhalo_ref.at[0], 0, slab_peer(1)), slab < ns - 1),
        (halo_copy(grid_ref.at[:, 0], zhalo_ref.at[1], 1, slab_peer(ns - 1)), slab > 0),
        (halo_copy(edge_ref.at[0], xhalo_ref.at[0], 2, tile_peer(1)), tile < nt - 1),
        (halo_copy(edge_ref.at[1], xhalo_ref.at[1], 3, tile_peer(nt - 1)), tile > 0),
    ]
    def part_copy(k, j):
        src = last_ref if k == reach else own_ref
        return pltpu.make_async_remote_copy(
            src_ref=src.at[j], dst_ref=far_ref.at[j, pl.ds(4 * (k - 1), src.shape[1])],
            send_sem=part_send.at[k - 1], recv_sem=part_recv.at[lot_of(j, chunks)],
            device_id=slab_peer(ns - k), device_id_type=MESH)

    row_ids = lax.broadcasted_iota(jnp.int32, (rows, chunk), 0)

    units = range(chunk // WIDTH)

    def enter():
        pl.semaphore_wait(barrier, greeters)
        for k in range(reach, 0, -1):
            pl.when(slab + k < ns)(whole_copy(k).start)
        for copy, sends in halos[2:]:
            pl.when(sends)(copy.start)

    opening = min(OPENING, chunks)

    def gather(*accs):
        banks = [[accs[(b * len(units) + q) * 4:][:4] for q in units] for b in range(2)]
        for j in range(chunks + 1):
            if j < chunks:
                hot = onehot_ref[:, pl.ds(j * chunk, chunk)]
                for q in units:
                    for half in range(2):
                        pltpu.matmul_push_rhs(hot[:, q * WIDTH:(q + 1) * WIDTH], half, q)
                for half, side in enumerate((high_ref, low_ref)):
                    for c in range(4):
                        lhs = side[pl.ds(c * rows, rows), :]
                        for q in units:
                            pltpu.matmul_acc_lhs(banks[j % 2][q][c], lhs, None if c else half)
            if j == 0:
                continue
            i = j - 1
            row = row_ref[:, pl.ds(i * chunk, chunk)]
            mask = row_ids == row
            for c in range(4):
                u = jnp.concatenate([pltpu.matmul_pop(banks[i % 2][q][c]) for q in units], axis=1)
                part = jnp.sum(jnp.where(mask, u, 0.0), axis=0, keepdims=True)
                part = part * (1.0 / TABLE_SCALE)
                if c == 3:
                    part = jnp.where(row < 0, 1.0, part)
                own_ref[i, c] = part
            for c in range(3):
                last_ref[i, c] = own_ref[i, c] + BACKGROUND * part
            if j < opening:
                continue
            if j == opening:
                enter()
            for n in range(0 if j == opening else i, j):
                for k in range(1, reach + 1):
                    pl.when(slab >= k)(part_copy(k, n).start)

    pl.run_scoped(gather, *[
        pltpu.ACC(q)((rows, WIDTH), jnp.float32)
        for _ in range(2) for q in units for _ in range(4)
    ])

    for copy, sends in halos[:2]:
        pl.when(sends)(copy.start)
    x_ids = lax.broadcasted_iota(jnp.int32, (rx, ry), 0)
    lane_ids = lax.broadcasted_iota(jnp.int32, (rx, ry), 1)
    first_x = tile == 0
    last_x = tile == nt - 1
    def smooth_planes(c, planes):
        for z in planes:
            g = grid_ref[c, z]
            if z > 0:
                below = grid_ref[c, z - 1]
            else:
                below = jnp.where(slab > 0, zhalo_ref[0, c], g)
            if z < depth - 1:
                above = grid_ref[c, z + 1]
            else:
                above = jnp.where(slab < ns - 1, zhalo_ref[1, c], g)
            xl = jnp.broadcast_to(xhalo_ref[0, c, pl.ds(z, 1), :], (rx, ry))
            xh = jnp.broadcast_to(xhalo_ref[1, c, pl.ds(z, 1), :], (rx, ry))
            xl = jnp.where(first_x, g, xl)
            xh = jnp.where(last_x, g, xh)
            left = jnp.where(x_ids == 0, xl, pltpu.roll(g, 1, 0))
            right = jnp.where(x_ids == rx - 1, xh, pltpu.roll(g, rx - 1, 0))
            down = jnp.where(lane_ids == 0, g, pltpu.roll(g, 1, 1))
            up = jnp.where(lane_ids == ry - 1, g, pltpu.roll(g, ry - 1, 1))
            smooth = (g - below) + (g - above) + (g - left) + (g - right) + (g - down) + (g - up)
            grad_ref[c, z] = (2.0 * TV_WEIGHT) * smooth

    wait_received(wholes_ref, whole_sem.at[1], behind_count, reach)
    folded = [[] for _ in range(4)]
    fold_t = jnp.ones((rx, ry), jnp.float32)
    fold_c = [jnp.zeros((rx, ry), jnp.float32)] * 3
    for k in range(1, reach + 1):
        there = slab >= k
        t = wholes_ref[k - 1, 3]
        fold_c = [jnp.where(there, wholes_ref[k - 1, c] + t * fold_c[c], 0.0) for c in range(3)]
        fold_t = jnp.where(there, t * fold_t, 0.0)
        for c in range(4):
            folded[c].append(fold_c[c] if c < 3 else fold_t)
    folds = jnp.concatenate([f for fs in folded for f in fs], axis=0)
    fold_high = folds.astype(jnp.bfloat16)
    fold_low = (folds - fold_high.astype(jnp.float32)).astype(jnp.bfloat16)
    step_rows = reach * rx
    step_ids = lax.broadcasted_iota(jnp.int32, (step_rows, chunk), 0)
    row_ids16 = row_ids.astype(jnp.float32).astype(jnp.bfloat16)
    none = jnp.zeros((), jnp.bfloat16)
    lags = 4
    inner = min(channels, chunks)

    def scatter(*accs):
        sums_acc = [accs[q * 4:][:4] for q in units]
        accs = accs[4 * len(units):]
        steps = [[accs[b * len(units) + q] for q in units] for b in range(lags)]

        def columns(j, q):
            return onehot_ref[:, pl.ds(j * chunk + q * WIDTH, WIDTH)]

        def front_start(j):
            for q in units:
                pltpu.matmul_push_rhs(columns(j, q), 0, q)
            for half, lhs in enumerate((fold_high, fold_low)):
                for q in units:
                    pltpu.matmul_acc_lhs(steps[j % lags][q], lhs, None if half else 0)

        def front_end(j):
            at_step = step_ref[:, pl.ds(j * chunk, chunk)]
            mask = step_ids == at_step
            u = jnp.concatenate([pltpu.matmul_pop(steps[j % lags][q]) for q in units], axis=1)
            for c in range(4):
                picked = jnp.where(mask, u[c * step_rows:(c + 1) * step_rows], 0.0)
                value = jnp.sum(picked, axis=0, keepdims=True)
                if c == 3:
                    value = jnp.where(at_step < 0, 1.0, value)
                front_ref[j, pl.ds(c, 1), :] = value

        for j in range(min(2, chunks)):
            front_start(j)
        for j in range(min(2, chunks)):
            front_end(j)

        target_load.wait()
        for j in range(chunks):
            lot = [i for i in range(chunks) if lot_of(i, chunks) == lot_of(j, chunks)]
            for n in range(1, reach + 1 if j == lot[0] else 0):
                size = far_ref.shape[1] if n == reach else 4 * n
                part = far_ref.at[pl.ds(j, len(lot)), pl.ds(0, size)]
                pl.when(ahead_count == n)(waiter(part, part_recv.at[lot_of(j, chunks)]).wait_recv)
            if j == chunks - inner:
                wait_received(xhalo_ref, halo_recv.at[1], beside_count, 2)
            if j == 0 and direct(ns, nt):
                for k in (-reach, reach):
                    @pl.when(inside(slab + k))
                    def _(k=k):
                        pl.semaphore_signal(
                            ready_sem, inc=1, device_id={"slab": slab + k}, device_id_type=MESH)
            at = pl.ds(j * chunk, chunk)
            if j + 2 < chunks:
                front_start(j + 2)
            for q in units:
                for half in range(2):
                    pltpu.matmul_push_rhs(columns(j, q), 1 - half, q, transpose=True)
            front_c = front_ref[j, pl.ds(0, 3), :]
            front_t = front_ref[j, pl.ds(3, 1), :]
            beyond = far_ref[j, pl.ds(4 * (reach - 1), 3), 0, :]
            beyond = jnp.where(slab + reach < ns, beyond, BACKGROUND)
            for k in range(reach - 1, 0, -1):
                pc = far_ref[j, pl.ds(4 * (k - 1), 3), 0, :]
                pt = far_ref[j, 4 * k - 1]
                beyond = jnp.where(slab + k < ns, pc + pt * beyond, beyond)
            pc = own_ref[j, pl.ds(0, 3), 0, :]
            pt = own_ref[j, 3]
            rendered = front_c + front_t * (pc + pt * beyond)
            residual = (COTANGENT_SCALE * RENDER_WEIGHT) * (rendered - target_ref[:, at])
            color_cot = front_t * residual
            trans_cot = front_t * jnp.sum(residual * beyond, axis=0, keepdims=True)
            mask = row_ids16 == row_ref[:, at].astype(jnp.float32).astype(jnp.bfloat16)
            cots = [color_cot[c:c + 1] for c in range(3)] + [trans_cot]
            tops = [cot.astype(jnp.bfloat16) for cot in cots]
            lows = [(cot - top.astype(jnp.float32)).astype(jnp.bfloat16) for cot, top in zip(cots, tops)]
            for half, side in enumerate((tops, lows)):
                for c in range(4):
                    spread = jnp.where(mask, side[c], none)
                    if half:
                        spread = spread.astype(FINE)
                    for q in units:
                        pltpu.matmul_acc_lhs(
                            sums_acc[q][c], spread[:, q * WIDTH:(q + 1) * WIDTH], None if c else 1 - half)
            if j + 2 < chunks:
                front_end(j + 2)
            if j >= chunks - inner:
                for c in range((j - chunks + inner) * channels // inner, (j + 1 - chunks + inner) * channels // inner):
                    smooth_planes(c, range(1, depth - 1))
        wait_received(zhalo_ref, halo_recv.at[0], level_count, 2)
        for c in range(channels):
            smooth_planes(c, (0, depth - 1) if depth > 1 else (0,))
        for c in range(4):
            gathered = sum(pltpu.matmul_pop(sums_acc[q][c]) for q in units)
            table_ref[pl.ds(c * rows, rows), :] = (1.0 / COTANGENT_SCALE) * gathered

    pl.run_scoped(scatter, *[
        pltpu.ACC(q)((rows, WIDTH), jnp.float32) for q in units for _ in range(4)
    ], *[
        pltpu.ACC(q)((4 * step_rows, WIDTH), jnp.float32) for _ in range(lags) for q in units
    ])

    zero = jnp.zeros((rx, ry), jnp.float32)
    suffix = [zero, zero, zero]
    later = zero
    squares = zero
    for z in range(depth - 1, -1, -1):
        w = weight_ref[z]
        after = trans_ref[z]
        later = later + after * table_ref[pl.ds(3 * rows + z * rx, rx), :]
        dw = zero
        for c in range(3):
            suffix[c] = suffix[c] + table_ref[pl.ds(c * rows + z * rx, rx), :]
            col = sig_ref[c + 1, z]
            dw = dw + col * suffix[c]
            out = grad_ref[c + 1, z] + w * suffix[c] * (col * (1.0 - col))
            grad_ref[c + 1, z] = out
            squares = squares + out * out
        dtau = after * dw - later
        later = later + w * dw
        out = grad_ref[0, z] + dtau * (sig_ref[0, z] * span)
        grad_ref[0, z] = out
        squares = squares + out * out

    lanes = jnp.sum(squares, axis=0, keepdims=True)
    lanes = sum(lanes[:, i * 128:(i + 1) * 128] for i in range(ry // 128))

    def norm_copy(phase, slots, peer=None):
        src = nsend_ref.at[pl.ds(phase, 1)] if peer else nrecv_ref.at[slots]
        return pltpu.make_async_remote_copy(
            src_ref=src, dst_ref=nrecv_ref.at[slots],
            send_sem=norm_send.at[phase], recv_sem=norm_recv.at[phase],
            device_id=peer or tile_peer(1), device_id_type=MESH)

    if direct(ns, nt):
        far = inside(slab - reach).astype(jnp.int32) + inside(slab + reach).astype(jnp.int32)
        pl.semaphore_wait(ready_sem, far)
    value = lanes
    base = 0
    for phase, peers in enumerate(phases):
        nsend_ref[phase] = value
        for i, peer in enumerate(peers):
            norm_copy(phase, pl.ds(base + i, 1), peer).start()
        if phase == 0:
            for copy in moment_loads:
                copy.wait()
            first_ref[...] = BETA_ONE * first_ref[...]
            second_ref[...] = BETA_TWO * second_ref[...]
            wait_sent(zhalo_ref, halo_send.at[0], level_count, 2)
            wait_sent(edge_ref, halo_send.at[1], beside_count, 2)
            wait_sent(wholes_ref, whole_sem.at[0], ahead_count, reach)
            for k in range(1, reach + 1):
                src = last_ref if k == reach else own_ref
                pl.when(slab >= k)(waiter(src, part_send.at[k - 1]).wait_send)
        norm_copy(phase, pl.ds(base, len(peers))).wait_recv()
        value = value + jnp.sum(nrecv_ref[pl.ds(base, len(peers)), 0, :], axis=0, keepdims=True)
        base += len(peers)
    limit = CLIP_RMS * math.sqrt(4.0 * total_depth * (rx * nt) * ry)
    total_square = jnp.sum(value, axis=1, keepdims=True)
    scale_ref[...] = jnp.broadcast_to(limit / jnp.maximum(jnp.sqrt(total_square), limit), (1, 128))
    base = 0
    for phase, peers in enumerate(phases):
        norm_copy(phase, pl.ds(base, len(peers))).wait_send()
        base += len(peers)


def split(depth):
    return math.gcd(depth, PIECES)


def lot_of(j, chunks):
    return j // 2 if j < chunks - 1 else (chunks - 1) // 2 + 1


def span_reach(ns):
    return max(ns // 2, 1)


def direct(ns, nt):
    return ns * nt <= DIRECT_LIMIT


def adam_kernel(
    grid_ref, first_ref, second_ref, grad_ref, scale_ref,
    grid_hbm, first_hbm, second_hbm, grid_out, first_out, second_out, sem,
):
    channels, depth, rx, ry = grid_ref.shape
    gain = (1.0 - BETA_ONE**STEP) / LEARN_RATE
    slope = gain / math.sqrt(1.0 - BETA_TWO**STEP)
    offset = gain * EPSILON
    scale = jnp.broadcast_to(scale_ref[0:1, 0:1], (rx, ry))
    linear = (1.0 - BETA_ONE) * scale
    square = (1.0 - BETA_TWO) * scale * scale
    pairs = ((first_out, first_hbm), (second_out, second_hbm), (grid_out, grid_hbm))
    pieces = split(depth)
    for c in range(channels):
        for p in range(pieces):
            planes = range(p * depth // pieces, (p + 1) * depth // pieces)
            for z in planes:
                g = grad_ref[c, z]
                first = first_ref[c, z] + linear * g
                second = second_ref[c, z] + square * g * g
                first_out[c, z] = first
                second_out[c, z] = second
                root = second * lax.rsqrt(second)
                grid_out[c, z] = grid_ref[c, z] - first / (root * slope + offset)
            at = pl.ds(p * depth // pieces, depth // pieces)
            for i, (a, b) in enumerate(pairs):
                pltpu.make_async_copy(a.at[c, at], b.at[c, at], sem.at[i]).start()
    for i, (a, b) in enumerate(pairs):
        pltpu.make_async_copy(a, b, sem.at[i]).wait()


def per_device(voxel_grid, first_moment, second_moment, pixel_index, start_slab, ray_count, target):
    ns = lax.axis_size("slab")
    nt = lax.axis_size("tile")
    channels, depth, rx, ry = voxel_grid.shape
    rays = pixel_index.shape[0]
    chunk = math.gcd(rays, CHUNK)
    chunks = rays // chunk
    rows = depth * rx
    reach = span_reach(ns)
    phases = 1 if direct(ns, nt) else 2
    messages = ns * nt - 1 if direct(ns, nt) else nt + ns - 2
    f32 = jnp.float32
    vmem = pl.BlockSpec(memory_space=pltpu.VMEM)
    hbm = pl.BlockSpec(memory_space=pltpu.HBM)
    cells = jax.ShapeDtypeStruct(voxel_grid.shape, f32)
    staged = pl.pallas_call(
        functools.partial(kernel, ns, nt, chunk),
        out_shape=(cells, cells, cells, cells, jax.ShapeDtypeStruct((1, 128), f32)),
        in_specs=[hbm] * 7,
        out_specs=(vmem,) * 5,
        scratch_shapes=[
            pltpu.VMEM((3, 1, rays), jnp.int32),
            pltpu.VMEM(target.shape, f32),
            pltpu.VMEM((channels * rows, ry), jnp.bfloat16),
            pltpu.VMEM((channels * rows, ry), FINE),
            pltpu.VMEM((depth, rx, ry), f32),
            pltpu.VMEM((depth, rx, ry), f32),
            pltpu.VMEM((channels, depth, rx, ry), f32),
            pltpu.VMEM((ry, rays), FINE),
            pltpu.VMEM((1, rays), jnp.int32),
            pltpu.VMEM((1, rays), jnp.int32),
            pltpu.VMEM((channels * rows, ry), f32),
            pltpu.VMEM((4, rx, ry), f32),
            pltpu.VMEM((reach, 4, rx, ry), f32),
            pltpu.VMEM((chunks, 4, chunk), f32),
            pltpu.VMEM((chunks, 4, 1, chunk), f32),
            pltpu.VMEM((chunks, 3, 1, chunk), f32),
            pltpu.VMEM((chunks, 4 * reach - 1, 1, chunk), f32),
            pltpu.VMEM((2, channels, depth, ry), f32),
            pltpu.VMEM((2, channels, depth, ry), f32),
            pltpu.VMEM((2, channels, rx, ry), f32),
            pltpu.VMEM((2, 1, 128), f32),
            pltpu.VMEM((messages, 1, 128), f32),
            pltpu.SemaphoreType.DMA((2,)),
            pltpu.SemaphoreType.DMA((reach,)),
            pltpu.SemaphoreType.DMA((lot_of(chunks - 1, chunks) + 1,)),
            pltpu.SemaphoreType.REGULAR,
            pltpu.SemaphoreType.DMA((2,)),
            pltpu.SemaphoreType.DMA((2,)),
            pltpu.SemaphoreType.DMA((phases,)),
            pltpu.SemaphoreType.DMA((phases,)),
            pltpu.SemaphoreType.DMA((3,)),
        ],
        compiler_params=pltpu.CompilerParams(
            collective_id=0, has_side_effects=True, vmem_limit_bytes=32 * 1024 * 1024
        ),
        name="render_step",
    )(*(pltpu.with_memory_space_constraint(a, pltpu.HBM) for a in (
        voxel_grid,
        first_moment,
        second_moment,
        pixel_index.reshape(1, rays),
        start_slab.reshape(1, rays),
        ray_count.reshape(1, rays),
        target,
    )))
    return pl.pallas_call(
        adam_kernel,
        out_shape=(cells, cells, cells),
        in_specs=[vmem] * 5,
        out_specs=(hbm, hbm, hbm),
        scratch_shapes=[
            pltpu.VMEM(voxel_grid.shape, f32),
            pltpu.VMEM(voxel_grid.shape, f32),
            pltpu.VMEM(voxel_grid.shape, f32),
            pltpu.SemaphoreType.DMA((3,)),
        ],
        compiler_params=pltpu.CompilerParams(vmem_limit_bytes=32 * 1024 * 1024),
        name="adam",
    )(*staged)


def solution(mesh):
    cells = P(None, "slab", "tile", None)
    return jax.shard_map(
        per_device,
        mesh=mesh,
        in_specs=(cells, cells, cells, P("tile"), P("tile"), P("tile"), P(None, "tile")),
        out_specs=(cells, cells, cells),
        check_vma=False,
    )
```

```python
import functools
import math

import jax
import jax.numpy as jnp
from jax import lax
from jax.experimental import pallas as pl
from jax.experimental.pallas import tpu as pltpu
from jax.sharding import PartitionSpec as P

STEP = 20
RENDER_WEIGHT = 1000.0
TV_WEIGHT = 0.05
BACKGROUND = 1.0
STEP_SPAN = 4.0
CLIP_RMS = 0.25
LEARN_RATE = 0.02
BETA_ONE = 0.9
BETA_TWO = 0.99
EPSILON = 1e-08
CHUNK = 512
WIDTH = 256
FINE = jnp.float8_e4m3fn
TABLE_SCALE = 65536.0
COTANGENT_SCALE = 32.0
PIECES = 4
DIRECT_LIMIT = 64
MESH = pl.DeviceIdType.MESH


def kernel(
    ns, nt, chunk,
    grid_hbm, first_hbm, second_hbm, pix_hbm, start_hbm, count_hbm, target_hbm,
    grid_ref, first_ref, second_ref, grad_ref, scale_ref,
    ints_ref, target_ref,
    high_ref, low_ref, trans_ref, weight_ref, sig_ref, onehot_ref, row_ref, step_ref, table_ref,
    whole_ref, wholes_ref, front_ref, own_ref, last_ref, far_ref,
    edge_ref, xhalo_ref, zhalo_ref, nsend_ref, nrecv_ref,
    whole_sem, part_send, part_recv, ready_sem, halo_send, halo_recv, norm_send, norm_recv, load_sem,
):
    channels, depth, rx, ry = grid_ref.shape
    rays = ints_ref.shape[2]
    pix_ref, start_ref, count_ref = (ints_ref.at[i] for i in range(3))
    chunks = rays // chunk
    total_depth = depth * ns
    reach = span_reach(ns)
    span = STEP_SPAN / total_depth
    rows = depth * rx
    slab = lax.axis_index("slab")
    tile = lax.axis_index("tile")

    def slab_peer(d):
        return {"slab": lax.rem(slab + d, ns)}

    def tile_peer(d):
        return {"tile": lax.rem(tile + d, nt)}

    if direct(ns, nt):
        phases = [[
            {"slab": lax.rem(slab + k // nt, ns), "tile": lax.rem(tile + k % nt, nt)}
            for k in [*range(nt, ns * nt), *range(1, nt)]
        ]]
        near = reach
    else:
        phases = [[tile_peer(d) for d in range(1, nt)], [slab_peer(d) for d in range(1, ns)]]
        near = ns - 1
    offsets = [k for k in range(-near, near + 1) if k]

    def inside(s):
        return (s >= 0) & (s < ns)

    pieces = split(depth)
    step = depth // pieces
    for i, a in enumerate((pix_hbm, start_hbm, count_hbm)):
        pltpu.make_async_copy(a, ints_ref.at[i], load_sem.at[1]).start()
    ints_load = pltpu.make_async_copy(ints_ref, ints_ref, load_sem.at[1])
    grid_load = pltpu.make_async_copy(grid_hbm, grid_ref, load_sem.at[0])
    for c in range(channels):
        for p in range(pieces):
            at = pl.ds(p * step, step)
            pltpu.make_async_copy(grid_hbm.at[c, at], grid_ref.at[c, at], load_sem.at[0]).start()
    target_load = pltpu.make_async_copy(target_hbm, target_ref, load_sem.at[2])
    target_load.start()
    moment_loads = [
        pltpu.make_async_copy(first_hbm, first_ref, load_sem.at[0]),
        pltpu.make_async_copy(second_hbm, second_ref, load_sem.at[1]),
    ]

    barrier = pltpu.get_barrier_semaphore()
    for d in range(1, nt):
        pl.semaphore_signal(barrier, inc=1, device_id=tile_peer(d), device_id_type=MESH)
    greeters = nt - 1
    for k in offsets:
        @pl.when(inside(slab + k))
        def _(k=k):
            pl.semaphore_signal(
                barrier, inc=1, device_id={"slab": slab + k}, device_id_type=MESH)
        greeters = greeters + inside(slab + k).astype(jnp.int32)

    ints_load.wait()
    y_ids = lax.broadcasted_iota(jnp.int32, (ry, chunk), 0).astype(jnp.float32).astype(jnp.bfloat16)
    for j in range(chunks):
        at = pl.ds(j * chunk, chunk)
        pix = pix_ref[:, at]
        start = start_ref[:, at]
        px = pix // ry
        py = (pix - px * ry).astype(jnp.float32).astype(jnp.bfloat16)
        length = jnp.clip((start - slab) * depth + count_ref[:, at], 0, depth)
        length = jnp.where(slab >= start, length, 0)
        row_ref[:, at] = jnp.where(length > 0, (length - 1) * rx + px, -1)
        step_ref[:, at] = (slab - start - 1) * rx + px
        hot = jnp.where(y_ids == py, jnp.ones((), jnp.bfloat16), jnp.zeros((), jnp.bfloat16))
        hot = hot.astype(FINE)
        onehot_ref[:, at] = hot

    grid_load.wait()
    for copy in moment_loads:
        copy.start()
    edge_ref[0] = grid_ref[:, :, rx - 1, :]
    edge_ref[1] = grid_ref[:, :, 0, :]

    total = jnp.zeros((rx, ry), jnp.float32)
    before = jnp.ones((rx, ry), jnp.float32)
    sums = [jnp.zeros((rx, ry), jnp.float32) for _ in range(3)]
    for z in range(depth):
        s = grid_ref[0, z]
        e = jnp.exp(-jnp.abs(s))
        tau = (jnp.maximum(s, 0.0) + jnp.log(1.0 + e)) * span
        sig_ref[0, z] = jnp.where(s >= 0, 1.0, e) / (1.0 + e)
        total = total + tau
        after = jnp.exp(-total)
        w = before * (1.0 - jnp.exp(-tau))
        before = after
        trans_ref[z] = after
        weight_ref[z] = w
        for c in range(3):
            col = 1.0 / (1.0 + jnp.exp(-grid_ref[c + 1, z]))
            sig_ref[c + 1, z] = col
            sums[c] = sums[c] + w * col
            table_ref[pl.ds(c * rows + z * rx, rx), :] = sums[c]
        table_ref[pl.ds(3 * rows + z * rx, rx), :] = after
    for c in range(3):
        whole_ref[c] = sums[c]
    whole_ref[3] = before
    full = TABLE_SCALE * table_ref[...]
    high = full.astype(jnp.bfloat16)
    high_ref[...] = high
    low_ref[...] = (full - high.astype(jnp.float32)).astype(FINE)

    def waiter(ref, sem):
        return pltpu.make_async_remote_copy(
            src_ref=ref, dst_ref=ref, send_sem=sem, recv_sem=sem,
            device_id=tile_peer(1), device_id_type=MESH)

    def wait_sent(ref, sem, count, most):
        for n in range(1, most + 1):
            pl.when(count == n)(waiter(ref.at[pl.ds(0, n)], sem).wait_send)

    def wait_received(ref, sem, count, most):
        for n in range(1, most + 1):
            pl.when(count == n)(waiter(ref.at[pl.ds(0, n)], sem).wait_recv)

    behind_count = jnp.minimum(slab, reach)
    ahead_count = jnp.minimum(ns - 1 - slab, reach)
    beside_count = (tile < nt - 1).astype(jnp.int32) + (tile > 0).astype(jnp.int32)
    level_count = (slab < ns - 1).astype(jnp.int32) + (slab > 0).astype(jnp.int32)

    def whole_copy(k):
        return pltpu.make_async_remote_copy(
            src_ref=whole_ref, dst_ref=wholes_ref.at[k - 1],
            send_sem=whole_sem.at[0], recv_sem=whole_sem.at[1],
            device_id=slab_peer(k), device_id_type=MESH)

    def halo_copy(src, dst, i, peer):
        return pltpu.make_async_remote_copy(
            src_ref=src, dst_ref=dst, send_sem=halo_send.at[i // 2], recv_sem=halo_recv.at[i // 2],
            device_id=peer, device_id_type=MESH)

    halos = [
        (halo_copy(grid_ref.at[:, depth - 1], zhalo_ref.at[0], 0, slab_peer(1)), slab < ns - 1),
        (halo_copy(grid_ref.at[:, 0], zhalo_ref.at[1], 1, slab_peer(ns - 1)), slab > 0),
        (halo_copy(edge_ref.at[0], xhalo_ref.at[0], 2, tile_peer(1)), tile < nt - 1),
        (halo_copy(edge_ref.at[1], xhalo_ref.at[1], 3, tile_peer(nt - 1)), tile > 0),
    ]
    def part_copy(k, j):
        src = last_ref if k == reach else own_ref
        return pltpu.make_async_remote_copy(
            src_ref=src.at[j], dst_ref=far_ref.at[j, pl.ds(4 * (k - 1), src.shape[1])],
            send_sem=part_send.at[k - 1], recv_sem=part_recv.at[lot_of(j, chunks)],
            device_id=slab_peer(ns - k), device_id_type=MESH)

    row_ids = lax.broadcasted_iota(jnp.int32, (rows, chunk), 0)

    units = range(chunk // WIDTH)

    def enter():
        pl.semaphore_wait(barrier, greeters)
        for k in range(1, min(reach, ns - 1) + 1):
            pl.when(slab == 0)(whole_copy(k).start)
        for k in range(reach, 0, -1):
            pl.when((slab > 0) & (slab + k < ns))(whole_copy(k).start)
        for copy, sends in halos[2:]:
            pl.when(sends)(copy.start)

    def gather(*accs):
        banks = [[accs[(b * len(units) + q) * 4:][:4] for q in units] for b in range(2)]
        for j in range(chunks + 1):
            if j < chunks:
                hot = onehot_ref[:, pl.ds(j * chunk, chunk)]
                for q in units:
                    for half in range(2):
                        pltpu.matmul_push_rhs(hot[:, q * WIDTH:(q + 1) * WIDTH], half, q)
                for half, side in enumerate((low_ref, high_ref)):
                    for c in range(4):
                        lhs = side[pl.ds(c * rows, rows), :]
                        for q in units:
                            pltpu.matmul_acc_lhs(banks[j % 2][q][c], lhs, None if c else half)
            if j == 0:
                continue
            i = j - 1
            row = row_ref[:, pl.ds(i * chunk, chunk)]
            mask = row_ids == row
            for c in range(4):
                u = jnp.concatenate([pltpu.matmul_pop(banks[i % 2][q][c]) for q in units], axis=1)
                part = jnp.sum(jnp.where(mask, u, 0.0), axis=0, keepdims=True)
                part = part * (1.0 / TABLE_SCALE)
                if c == 3:
                    part = jnp.where(row < 0, 1.0, part)
                own_ref[i, c] = part
            for c in range(3):
                last_ref[i, c] = own_ref[i, c] + BACKGROUND * part
            lot = [n for n in range(chunks) if lot_of(n, chunks) == lot_of(i, chunks)]
            if i != lot[-1]:
                continue
            if lot[0] == 0:
                enter()
            for n in lot:
                for k in range(1, reach + 1):
                    pl.when(slab >= k)(part_copy(k, n).start)

    pl.run_scoped(gather, *[
        pltpu.ACC(q)((rows, WIDTH), jnp.float32)
        for _ in range(2) for q in units for _ in range(4)
    ])

    for copy, sends in halos[:2]:
        pl.when(sends)(copy.start)
    x_ids = lax.broadcasted_iota(jnp.int32, (rx, ry), 0)
    lane_ids = lax.broadcasted_iota(jnp.int32, (rx, ry), 1)
    first_x = tile == 0
    last_x = tile == nt - 1
    def smooth_planes(c, planes):
        for z in planes:
            g = grid_ref[c, z]
            if z > 0:
                below = grid_ref[c, z - 1]
            else:
                below = jnp.where(slab > 0, zhalo_ref[0, c], g)
            if z < depth - 1:
                above = grid_ref[c, z + 1]
            else:
                above = jnp.where(slab < ns - 1, zhalo_ref[1, c], g)
            xl = jnp.broadcast_to(xhalo_ref[0, c, pl.ds(z, 1), :], (rx, ry))
            xh = jnp.broadcast_to(xhalo_ref[1, c, pl.ds(z, 1), :], (rx, ry))
            xl = jnp.where(first_x, g, xl)
            xh = jnp.where(last_x, g, xh)
            left = jnp.where(x_ids == 0, xl, pltpu.roll(g, 1, 0))
            right = jnp.where(x_ids == rx - 1, xh, pltpu.roll(g, rx - 1, 0))
            down = jnp.where(lane_ids == 0, g, pltpu.roll(g, 1, 1))
            up = jnp.where(lane_ids == ry - 1, g, pltpu.roll(g, ry - 1, 1))
            smooth = (g - below) + (g - above) + (g - left) + (g - right) + (g - down) + (g - up)
            grad_ref[c, z] = (2.0 * TV_WEIGHT) * smooth

    wait_received(xhalo_ref, halo_recv.at[1], beside_count, 2)
    for c in range(channels):
        smooth_planes(c, range(1, depth - 1))
    wait_received(wholes_ref, whole_sem.at[1], behind_count, reach)
    folded = [[] for _ in range(4)]
    fold_t = jnp.ones((rx, ry), jnp.float32)
    fold_c = [jnp.zeros((rx, ry), jnp.float32)] * 3
    for k in range(1, reach + 1):
        there = slab >= k
        t = wholes_ref[k - 1, 3]
        fold_c = [jnp.where(there, wholes_ref[k - 1, c] + t * fold_c[c], 0.0) for c in range(3)]
        fold_t = jnp.where(there, t * fold_t, 0.0)
        for c in range(4):
            folded[c].append(fold_c[c] if c < 3 else fold_t)
    folds = jnp.concatenate([f for fs in folded for f in fs], axis=0)
    fold_high = folds.astype(jnp.bfloat16)
    fold_low = (folds - fold_high.astype(jnp.float32)).astype(jnp.bfloat16)
    step_rows = reach * rx
    step_ids = lax.broadcasted_iota(jnp.int32, (step_rows, chunk), 0)
    row_ids16 = row_ids.astype(jnp.float32).astype(jnp.bfloat16)
    none = jnp.zeros((), jnp.bfloat16)
    lags = 4

    def scatter(*accs):
        sums_acc = [accs[q * 4:][:4] for q in units]
        accs = accs[4 * len(units):]
        steps = [[accs[b * len(units) + q] for q in units] for b in range(lags)]

        def columns(j, q):
            return onehot_ref[:, pl.ds(j * chunk + q * WIDTH, WIDTH)]

        def front_start(j):
            for q in units:
                pltpu.matmul_push_rhs(columns(j, q), 0, q)
            for half, lhs in enumerate((fold_high, fold_low)):
                for q in units:
                    pltpu.matmul_acc_lhs(steps[j % lags][q], lhs, None if half else 0)

        def front_end(j):
            at_step = step_ref[:, pl.ds(j * chunk, chunk)]
            mask = step_ids == at_step
            u = jnp.concatenate([pltpu.matmul_pop(steps[j % lags][q]) for q in units], axis=1)
            for c in range(4):
                picked = jnp.where(mask, u[c * step_rows:(c + 1) * step_rows], 0.0)
                value = jnp.sum(picked, axis=0, keepdims=True)
                if c == 3:
                    value = jnp.where(at_step < 0, 1.0, value)
                front_ref[j, pl.ds(c, 1), :] = value

        for j in range(min(2, chunks)):
            front_start(j)
        for j in range(min(2, chunks)):
            front_end(j)

        target_load.wait()
        for j in range(chunks):
            lot = [i for i in range(chunks) if lot_of(i, chunks) == lot_of(j, chunks)]
            for n in range(1, reach + 1 if j == lot[0] else 0):
                size = far_ref.shape[1] if n == reach else 4 * n
                part = far_ref.at[pl.ds(j, len(lot)), pl.ds(0, size)]
                pl.when(ahead_count == n)(waiter(part, part_recv.at[lot_of(j, chunks)]).wait_recv)
            if j == 0 and direct(ns, nt):
                for k in (-reach, reach):
                    @pl.when(inside(slab + k))
                    def _(k=k):
                        pl.semaphore_signal(
                            ready_sem, inc=1, device_id={"slab": slab + k}, device_id_type=MESH)
            at = pl.ds(j * chunk, chunk)
            if j + 2 < chunks:
                front_start(j + 2)
            for q in units:
                for half in range(2):
                    pltpu.matmul_push_rhs(columns(j, q), 1 - half, q, transpose=True)
            front_c = front_ref[j, pl.ds(0, 3), :]
            front_t = front_ref[j, pl.ds(3, 1), :]
            beyond = far_ref[j, pl.ds(4 * (reach - 1), 3), 0, :]
            beyond = jnp.where(slab + reach < ns, beyond, BACKGROUND)
            for k in range(reach - 1, 0, -1):
                pc = far_ref[j, pl.ds(4 * (k - 1), 3), 0, :]
                pt = far_ref[j, 4 * k - 1]
                beyond = jnp.where(slab + k < ns, pc + pt * beyond, beyond)
            pc = own_ref[j, pl.ds(0, 3), 0, :]
            pt = own_ref[j, 3]
            rendered = front_c + front_t * (pc + pt * beyond)
            residual = (COTANGENT_SCALE * RENDER_WEIGHT) * (rendered - target_ref[:, at])
            color_cot = front_t * residual
            trans_cot = front_t * jnp.sum(residual * beyond, axis=0, keepdims=True)
            mask = row_ids16 == row_ref[:, at].astype(jnp.float32).astype(jnp.bfloat16)
            cots = [color_cot[c:c + 1] for c in range(3)] + [trans_cot]
            tops = [cot.astype(jnp.bfloat16) for cot in cots]
            lows = [(cot - top.astype(jnp.float32)).astype(jnp.bfloat16) for cot, top in zip(cots, tops)]
            for half, side in enumerate((tops, lows)):
                for c in range(4):
                    spread = jnp.where(mask, side[c], none)
                    if half:
                        spread = spread.astype(FINE)
                    for q in units:
                        pltpu.matmul_acc_lhs(
                            sums_acc[q][c], spread[:, q * WIDTH:(q + 1) * WIDTH], None if c else 1 - half)
            if j + 2 < chunks:
                front_end(j + 2)
        wait_received(zhalo_ref, halo_recv.at[0], level_count, 2)
        for c in range(channels):
            smooth_planes(c, (0, depth - 1) if depth > 1 else (0,))
        for c in range(4):
            gathered = sum(pltpu.matmul_pop(sums_acc[q][c]) for q in units)
            table_ref[pl.ds(c * rows, rows), :] = (1.0 / COTANGENT_SCALE) * gathered

    pl.run_scoped(scatter, *[
        pltpu.ACC(q)((rows, WIDTH), jnp.float32) for q in units for _ in range(4)
    ], *[
        pltpu.ACC(q)((4 * step_rows, WIDTH), jnp.float32) for _ in range(lags) for q in units
    ])

    zero = jnp.zeros((rx, ry), jnp.float32)
    suffix = [zero, zero, zero]
    later = zero
    squares = zero
    for z in range(depth - 1, -1, -1):
        w = weight_ref[z]
        after = trans_ref[z]
        later = later + after * table_ref[pl.ds(3 * rows + z * rx, rx), :]
        dw = zero
        for c in range(3):
            suffix[c] = suffix[c] + table_ref[pl.ds(c * rows + z * rx, rx), :]
            col = sig_ref[c + 1, z]
            dw = dw + col * suffix[c]
            out = grad_ref[c + 1, z] + w * suffix[c] * (col * (1.0 - col))
            grad_ref[c + 1, z] = out
            squares = squares + out * out
        dtau = after * dw - later
        later = later + w * dw
        out = grad_ref[0, z] + dtau * (sig_ref[0, z] * span)
        grad_ref[0, z] = out
        squares = squares + out * out

    lanes = jnp.sum(squares, axis=0, keepdims=True)
    lanes = sum(lanes[:, i * 128:(i + 1) * 128] for i in range(ry // 128))

    def norm_copy(phase, slots, peer=None):
        src = nsend_ref.at[pl.ds(phase, 1)] if peer else nrecv_ref.at[slots]
        return pltpu.make_async_remote_copy(
            src_ref=src, dst_ref=nrecv_ref.at[slots],
            send_sem=norm_send.at[phase], recv_sem=norm_recv.at[phase],
            device_id=peer or tile_peer(1), device_id_type=MESH)

    if direct(ns, nt):
        far = inside(slab - reach).astype(jnp.int32) + inside(slab + reach).astype(jnp.int32)
        pl.semaphore_wait(ready_sem, far)
    value = lanes
    base = 0
    for phase, peers in enumerate(phases):
        nsend_ref[phase] = value
        for i, peer in enumerate(peers):
            norm_copy(phase, pl.ds(base + i, 1), peer).start()
        if phase == 0:
            for copy in moment_loads:
                copy.wait()
            first_ref[...] = BETA_ONE * first_ref[...]
            second_ref[...] = BETA_TWO * second_ref[...]
            wait_sent(zhalo_ref, halo_send.at[0], level_count, 2)
            wait_sent(edge_ref, halo_send.at[1], beside_count, 2)
            wait_sent(wholes_ref, whole_sem.at[0], ahead_count, reach)
            for k in range(1, reach + 1):
                src = last_ref if k == reach else own_ref
                pl.when(slab >= k)(waiter(src, part_send.at[k - 1]).wait_send)
        norm_copy(phase, pl.ds(base, len(peers))).wait_recv()
        value = value + jnp.sum(nrecv_ref[pl.ds(base, len(peers)), 0, :], axis=0, keepdims=True)
        base += len(peers)
    limit = CLIP_RMS * math.sqrt(4.0 * total_depth * (rx * nt) * ry)
    total_square = jnp.sum(value, axis=1, keepdims=True)
    scale_ref[...] = jnp.broadcast_to(limit / jnp.maximum(jnp.sqrt(total_square), limit), (1, 128))
    base = 0
    for phase, peers in enumerate(phases):
        norm_copy(phase, pl.ds(base, len(peers))).wait_send()
        base += len(peers)


def split(depth):
    return math.gcd(depth, PIECES)


def lot_of(j, chunks):
    return j // 2 if j < chunks - 1 else (chunks - 1) // 2 + 1


def span_reach(ns):
    return max(ns // 2, 1)


def direct(ns, nt):
    return ns * nt <= DIRECT_LIMIT


def adam_kernel(
    grid_ref, first_ref, second_ref, grad_ref, scale_ref,
    grid_hbm, first_hbm, second_hbm, grid_out, first_out, second_out, sem,
):
    channels, depth, rx, ry = grid_ref.shape
    gain = (1.0 - BETA_ONE**STEP) / LEARN_RATE
    slope = gain / math.sqrt(1.0 - BETA_TWO**STEP)
    offset = gain * EPSILON
    scale = jnp.broadcast_to(scale_ref[0:1, 0:1], (rx, ry))
    linear = (1.0 - BETA_ONE) * scale
    square = (1.0 - BETA_TWO) * scale * scale
    pairs = ((first_out, first_hbm), (second_out, second_hbm), (grid_out, grid_hbm))
    pieces = split(depth)
    for c in range(channels):
        for p in range(pieces):
            planes = range(p * depth // pieces, (p + 1) * depth // pieces)
            for z in planes:
                g = grad_ref[c, z]
                first = first_ref[c, z] + linear * g
                second = second_ref[c, z] + square * g * g
                first_out[c, z] = first
                second_out[c, z] = second
                root = second * lax.rsqrt(second)
                grid_out[c, z] = grid_ref[c, z] - first / (root * slope + offset)
            at = pl.ds(p * depth // pieces, depth // pieces)
            for i, (a, b) in enumerate(pairs):
                pltpu.make_async_copy(a.at[c, at], b.at[c, at], sem.at[i]).start()
    for i, (a, b) in enumerate(pairs):
        pltpu.make_async_copy(a, b, sem.at[i]).wait()


def per_device(voxel_grid, first_moment, second_moment, pixel_index, start_slab, ray_count, target):
    ns = lax.axis_size("slab")
    nt = lax.axis_size("tile")
    channels, depth, rx, ry = voxel_grid.shape
    rays = pixel_index.shape[0]
    chunk = math.gcd(rays, CHUNK)
    chunks = rays // chunk
    rows = depth * rx
    reach = span_reach(ns)
    phases = 1 if direct(ns, nt) else 2
    messages = ns * nt - 1 if direct(ns, nt) else nt + ns - 2
    f32 = jnp.float32
    vmem = pl.BlockSpec(memory_space=pltpu.VMEM)
    hbm = pl.BlockSpec(memory_space=pltpu.HBM)
    cells = jax.ShapeDtypeStruct(voxel_grid.shape, f32)
    staged = pl.pallas_call(
        functools.partial(kernel, ns, nt, chunk),
        out_shape=(cells, cells, cells, cells, jax.ShapeDtypeStruct((1, 128), f32)),
        in_specs=[hbm] * 7,
        out_specs=(vmem,) * 5,
        scratch_shapes=[
            pltpu.VMEM((3, 1, rays), jnp.int32),
            pltpu.VMEM(target.shape, f32),
            pltpu.VMEM((channels * rows, ry), jnp.bfloat16),
            pltpu.VMEM((channels * rows, ry), FINE),
            pltpu.VMEM((depth, rx, ry), f32),
            pltpu.VMEM((depth, rx, ry), f32),
            pltpu.VMEM((channels, depth, rx, ry), f32),
            pltpu.VMEM((ry, rays), FINE),
            pltpu.VMEM((1, rays), jnp.int32),
            pltpu.VMEM((1, rays), jnp.int32),
            pltpu.VMEM((channels * rows, ry), f32),
            pltpu.VMEM((4, rx, ry), f32),
            pltpu.VMEM((reach, 4, rx, ry), f32),
            pltpu.VMEM((chunks, 4, chunk), f32),
            pltpu.VMEM((chunks, 4, 1, chunk), f32),
            pltpu.VMEM((chunks, 3, 1, chunk), f32),
            pltpu.VMEM((chunks, 4 * reach - 1, 1, chunk), f32),
            pltpu.VMEM((2, channels, depth, ry), f32),
            pltpu.VMEM((2, channels, depth, ry), f32),
            pltpu.VMEM((2, channels, rx, ry), f32),
            pltpu.VMEM((2, 1, 128), f32),
            pltpu.VMEM((messages, 1, 128), f32),
            pltpu.SemaphoreType.DMA((2,)),
            pltpu.SemaphoreType.DMA((reach,)),
            pltpu.SemaphoreType.DMA((lot_of(chunks - 1, chunks) + 1,)),
            pltpu.SemaphoreType.REGULAR,
            pltpu.SemaphoreType.DMA((2,)),
            pltpu.SemaphoreType.DMA((2,)),
            pltpu.SemaphoreType.DMA((phases,)),
            pltpu.SemaphoreType.DMA((phases,)),
            pltpu.SemaphoreType.DMA((3,)),
        ],
        compiler_params=pltpu.CompilerParams(
            collective_id=0, has_side_effects=True, vmem_limit_bytes=32 * 1024 * 1024
        ),
        name="render_step",
    )(*(pltpu.with_memory_space_constraint(a, pltpu.HBM) for a in (
        voxel_grid,
        first_moment,
        second_moment,
        pixel_index.reshape(1, rays),
        start_slab.reshape(1, rays),
        ray_count.reshape(1, rays),
        target,
    )))
    return pl.pallas_call(
        adam_kernel,
        out_shape=(cells, cells, cells),
        in_specs=[vmem] * 5,
        out_specs=(hbm, hbm, hbm),
        scratch_shapes=[
            pltpu.VMEM(voxel_grid.shape, f32),
            pltpu.VMEM(voxel_grid.shape, f32),
            pltpu.VMEM(voxel_grid.shape, f32),
            pltpu.SemaphoreType.DMA((3,)),
        ],
        compiler_params=pltpu.CompilerParams(vmem_limit_bytes=32 * 1024 * 1024),
        name="adam",
    )(*staged)


def solution(mesh):
    cells = P(None, "slab", "tile", None)
    return jax.shard_map(
        per_device,
        mesh=mesh,
        in_specs=(cells, cells, cells, P("tile"), P("tile"), P("tile"), P(None, "tile")),
        out_specs=(cells, cells, cells),
        check_vma=False,
    )
```

```python
import functools
import math

import jax
import jax.numpy as jnp
from jax import lax
from jax.experimental import pallas as pl
from jax.experimental.pallas import tpu as pltpu
from jax.sharding import PartitionSpec as P

STEP = 20
RENDER_WEIGHT = 1000.0
TV_WEIGHT = 0.05
BACKGROUND = 1.0
STEP_SPAN = 4.0
CLIP_RMS = 0.25
LEARN_RATE = 0.02
BETA_ONE = 0.9
BETA_TWO = 0.99
EPSILON = 1e-08
CHUNK = 512
WIDTH = 256
FINE = jnp.float8_e4m3fn
TABLE_SCALE = 65536.0
COTANGENT_SCALE = 32.0
PIECES = 4
DIRECT_LIMIT = 64
MESH = pl.DeviceIdType.MESH


def kernel(
    ns, nt, chunk,
    grid_hbm, first_hbm, second_hbm, pix_hbm, start_hbm, count_hbm, target_hbm,
    grid_ref, first_ref, second_ref, grad_ref, scale_ref,
    ints_ref, target_ref,
    high_ref, low_ref, trans_ref, weight_ref, sig_ref, onehot_ref, row_ref, step_ref, table_ref,
    whole_ref, wholes_ref, front_ref, own_ref, last_ref, far_ref,
    edge_ref, xhalo_ref, zhalo_ref, nsend_ref, nrecv_ref,
    whole_sem, part_send, part_recv, ready_sem, halo_send, halo_recv, norm_send, norm_recv, load_sem,
):
    channels, depth, rx, ry = grid_ref.shape
    rays = ints_ref.shape[2]
    pix_ref, start_ref, count_ref = (ints_ref.at[i] for i in range(3))
    chunks = rays // chunk
    total_depth = depth * ns
    reach = span_reach(ns)
    span = STEP_SPAN / total_depth
    rows = depth * rx
    slab = lax.axis_index("slab")
    tile = lax.axis_index("tile")

    def slab_peer(d):
        return {"slab": lax.rem(slab + d, ns)}

    def tile_peer(d):
        return {"tile": lax.rem(tile + d, nt)}

    if direct(ns, nt):
        phases = [[
            {"slab": lax.rem(slab + k // nt, ns), "tile": lax.rem(tile + k % nt, nt)}
            for k in [*range(nt, ns * nt), *range(1, nt)]
        ]]
        near = reach
    else:
        phases = [[tile_peer(d) for d in range(1, nt)], [slab_peer(d) for d in range(1, ns)]]
        near = ns - 1
    offsets = [k for k in range(-near, near + 1) if k]

    def inside(s):
        return (s >= 0) & (s < ns)

    pieces = split(depth)
    step = depth // pieces
    for i, a in enumerate((pix_hbm, start_hbm, count_hbm)):
        pltpu.make_async_copy(a, ints_ref.at[i], load_sem.at[1]).start()
    ints_load = pltpu.make_async_copy(ints_ref, ints_ref, load_sem.at[1])
    grid_load = pltpu.make_async_copy(grid_hbm, grid_ref, load_sem.at[0])
    for c in range(channels):
        for p in range(pieces):
            at = pl.ds(p * step, step)
            pltpu.make_async_copy(grid_hbm.at[c, at], grid_ref.at[c, at], load_sem.at[0]).start()
    target_load = pltpu.make_async_copy(target_hbm, target_ref, load_sem.at[2])
    target_load.start()
    moment_loads = [
        pltpu.make_async_copy(first_hbm, first_ref, load_sem.at[0]),
        pltpu.make_async_copy(second_hbm, second_ref, load_sem.at[1]),
    ]

    barrier = pltpu.get_barrier_semaphore()
    for d in range(1, nt):
        pl.semaphore_signal(barrier, inc=1, device_id=tile_peer(d), device_id_type=MESH)
    greeters = nt - 1
    for k in offsets:
        @pl.when(inside(slab + k))
        def _(k=k):
            pl.semaphore_signal(
                barrier, inc=1, device_id={"slab": slab + k}, device_id_type=MESH)
        greeters = greeters + inside(slab + k).astype(jnp.int32)

    ints_load.wait()
    y_ids = lax.broadcasted_iota(jnp.int32, (ry, chunk), 0).astype(jnp.float32).astype(jnp.bfloat16)
    for j in range(chunks):
        at = pl.ds(j * chunk, chunk)
        pix = pix_ref[:, at]
        start = start_ref[:, at]
        px = pix // ry
        py = (pix - px * ry).astype(jnp.float32).astype(jnp.bfloat16)
        length = jnp.clip((start - slab) * depth + count_ref[:, at], 0, depth)
        length = jnp.where(slab >= start, length, 0)
        row_ref[:, at] = jnp.where(length > 0, (length - 1) * rx + px, -1)
        step_ref[:, at] = (slab - start - 1) * rx + px
        hot = jnp.where(y_ids == py, jnp.ones((), jnp.bfloat16), jnp.zeros((), jnp.bfloat16))
        hot = hot.astype(FINE)
        onehot_ref[:, at] = hot

    grid_load.wait()
    for copy in moment_loads:
        copy.start()
    edge_ref[0] = grid_ref[:, :, rx - 1, :]
    edge_ref[1] = grid_ref[:, :, 0, :]

    total = jnp.zeros((rx, ry), jnp.float32)
    before = jnp.ones((rx, ry), jnp.float32)
    sums = [jnp.zeros((rx, ry), jnp.float32) for _ in range(3)]
    for z in range(depth):
        s = grid_ref[0, z]
        e = jnp.exp(-jnp.abs(s))
        tau = (jnp.maximum(s, 0.0) + jnp.log(1.0 + e)) * span
        sig_ref[0, z] = jnp.where(s >= 0, 1.0, e) / (1.0 + e)
        total = total + tau
        after = jnp.exp(-total)
        w = before * (1.0 - jnp.exp(-tau))
        before = after
        trans_ref[z] = after
        weight_ref[z] = w
        for c in range(3):
            col = 1.0 / (1.0 + jnp.exp(-grid_ref[c + 1, z]))
            sig_ref[c + 1, z] = col
            sums[c] = sums[c] + w * col
            table_ref[pl.ds(c * rows + z * rx, rx), :] = sums[c]
        table_ref[pl.ds(3 * rows + z * rx, rx), :] = after
    for c in range(3):
        whole_ref[c] = sums[c]
    whole_ref[3] = before
    full = TABLE_SCALE * table_ref[...]
    high = full.astype(jnp.bfloat16)
    high_ref[...] = high
    low_ref[...] = (full - high.astype(jnp.float32)).astype(FINE)

    def waiter(ref, sem):
        return pltpu.make_async_remote_copy(
            src_ref=ref, dst_ref=ref, send_sem=sem, recv_sem=sem,
            device_id=tile_peer(1), device_id_type=MESH)

    def wait_sent(ref, sem, count, most):
        for n in range(1, most + 1):
            pl.when(count == n)(waiter(ref.at[pl.ds(0, n)], sem).wait_send)

    def wait_received(ref, sem, count, most):
        for n in range(1, most + 1):
            pl.when(count == n)(waiter(ref.at[pl.ds(0, n)], sem).wait_recv)

    behind_count = jnp.minimum(slab, reach)
    ahead_count = jnp.minimum(ns - 1 - slab, reach)
    beside_count = (tile < nt - 1).astype(jnp.int32) + (tile > 0).astype(jnp.int32)
    level_count = (slab < ns - 1).astype(jnp.int32) + (slab > 0).astype(jnp.int32)

    def whole_copy(k):
        return pltpu.make_async_remote_copy(
            src_ref=whole_ref, dst_ref=wholes_ref.at[k - 1],
            send_sem=whole_sem.at[0], recv_sem=whole_sem.at[1],
            device_id=slab_peer(k), device_id_type=MESH)

    def halo_copy(src, dst, i, peer):
        return pltpu.make_async_remote_copy(
            src_ref=src, dst_ref=dst, send_sem=halo_send.at[i // 2], recv_sem=halo_recv.at[i // 2],
            device_id=peer, device_id_type=MESH)

    halos = [
        (halo_copy(grid_ref.at[:, depth - 1], zhalo_ref.at[0], 0, slab_peer(1)), slab < ns - 1),
        (halo_copy(grid_ref.at[:, 0], zhalo_ref.at[1], 1, slab_peer(ns - 1)), slab > 0),
        (halo_copy(edge_ref.at[0], xhalo_ref.at[0], 2, tile_peer(1)), tile < nt - 1),
        (halo_copy(edge_ref.at[1], xhalo_ref.at[1], 3, tile_peer(nt - 1)), tile > 0),
    ]
    def part_copy(k, j):
        src = last_ref if k == reach else own_ref
        return pltpu.make_async_remote_copy(
            src_ref=src.at[j], dst_ref=far_ref.at[j, pl.ds(4 * (k - 1), src.shape[1])],
            send_sem=part_send.at[k - 1], recv_sem=part_recv.at[lot_of(j, chunks)],
            device_id=slab_peer(ns - k), device_id_type=MESH)

    row_ids = lax.broadcasted_iota(jnp.int32, (rows, chunk), 0)

    units = range(chunk // WIDTH)

    def enter():
        pl.semaphore_wait(barrier, greeters)
        for k in range(1, min(reach, ns - 1) + 1):
            pl.when(slab == 0)(whole_copy(k).start)
        for k in range(reach, 0, -1):
            pl.when((slab > 0) & (slab + k < ns))(whole_copy(k).start)
        for copy, sends in halos[2:]:
            pl.when(sends)(copy.start)

    def gather(*accs):
        banks = [[accs[(b * len(units) + q) * 4:][:4] for q in units] for b in range(2)]
        for j in range(chunks + 1):
            if j < chunks:
                hot = onehot_ref[:, pl.ds(j * chunk, chunk)]
                for q in units:
                    for half in range(2):
                        pltpu.matmul_push_rhs(hot[:, q * WIDTH:(q + 1) * WIDTH], half, q)
                for half, side in enumerate((low_ref, high_ref)):
                    for c in range(4):
                        lhs = side[pl.ds(c * rows, rows), :]
                        for q in units:
                            pltpu.matmul_acc_lhs(banks[j % 2][q][c], lhs, None if c else half)
            if j == 0:
                continue
            i = j - 1
            row = row_ref[:, pl.ds(i * chunk, chunk)]
            mask = row_ids == row
            for c in range(4):
                u = jnp.concatenate([pltpu.matmul_pop(banks[i % 2][q][c]) for q in units], axis=1)
                part = jnp.sum(jnp.where(mask, u, 0.0), axis=0, keepdims=True)
                part = part * (1.0 / TABLE_SCALE)
                if c == 3:
                    part = jnp.where(row < 0, 1.0, part)
                own_ref[i, c] = part
            for c in range(3):
                last_ref[i, c] = own_ref[i, c] + BACKGROUND * part
            lot = [n for n in range(chunks) if lot_of(n, chunks) == lot_of(i, chunks)]
            if i != lot[-1]:
                continue
            if lot[0] == 0:
                enter()
            for n in lot:
                for k in range(1, reach + 1):
                    pl.when(slab >= k)(part_copy(k, n).start)

    pl.run_scoped(gather, *[
        pltpu.ACC(q)((rows, WIDTH), jnp.float32)
        for _ in range(2) for q in units for _ in range(4)
    ])

    pl.when(halos[1][1])(halos[1][0].start)
    x_ids = lax.broadcasted_iota(jnp.int32, (rx, ry), 0)
    lane_ids = lax.broadcasted_iota(jnp.int32, (rx, ry), 1)
    first_x = tile == 0
    last_x = tile == nt - 1
    def smooth_planes(c, planes):
        for z in planes:
            g = grid_ref[c, z]
            if z > 0:
                below = grid_ref[c, z - 1]
            else:
                below = jnp.where(slab > 0, zhalo_ref[0, c], g)
            if z < depth - 1:
                above = grid_ref[c, z + 1]
            else:
                above = jnp.where(slab < ns - 1, zhalo_ref[1, c], g)
            xl = jnp.broadcast_to(xhalo_ref[0, c, pl.ds(z, 1), :], (rx, ry))
            xh = jnp.broadcast_to(xhalo_ref[1, c, pl.ds(z, 1), :], (rx, ry))
            xl = jnp.where(first_x, g, xl)
            xh = jnp.where(last_x, g, xh)
            left = jnp.where(x_ids == 0, xl, pltpu.roll(g, 1, 0))
            right = jnp.where(x_ids == rx - 1, xh, pltpu.roll(g, rx - 1, 0))
            down = jnp.where(lane_ids == 0, g, pltpu.roll(g, 1, 1))
            up = jnp.where(lane_ids == ry - 1, g, pltpu.roll(g, ry - 1, 1))
            smooth = (g - below) + (g - above) + (g - left) + (g - right) + (g - down) + (g - up)
            grad_ref[c, z] = (2.0 * TV_WEIGHT) * smooth

    wait_received(xhalo_ref, halo_recv.at[1], beside_count, 2)
    for c in range(channels):
        smooth_planes(c, range(1, depth - 1))
    pl.when(halos[0][1])(halos[0][0].start)
    wait_received(wholes_ref, whole_sem.at[1], behind_count, reach)
    folded = [[] for _ in range(4)]
    fold_t = jnp.ones((rx, ry), jnp.float32)
    fold_c = [jnp.zeros((rx, ry), jnp.float32)] * 3
    for k in range(1, reach + 1):
        there = slab >= k
        t = wholes_ref[k - 1, 3]
        fold_c = [jnp.where(there, wholes_ref[k - 1, c] + t * fold_c[c], 0.0) for c in range(3)]
        fold_t = jnp.where(there, t * fold_t, 0.0)
        for c in range(4):
            folded[c].append(fold_c[c] if c < 3 else fold_t)
    folds = jnp.concatenate([f for fs in folded for f in fs], axis=0)
    fold_high = folds.astype(jnp.bfloat16)
    fold_low = (folds - fold_high.astype(jnp.float32)).astype(jnp.bfloat16)
    step_rows = reach * rx
    step_ids = lax.broadcasted_iota(jnp.int32, (step_rows, chunk), 0)
    row_ids16 = row_ids.astype(jnp.float32).astype(jnp.bfloat16)
    none = jnp.zeros((), jnp.bfloat16)
    lags = 4

    def scatter(*accs):
        sums_acc = [accs[q * 4:][:4] for q in units]
        accs = accs[4 * len(units):]
        steps = [[accs[b * len(units) + q] for q in units] for b in range(lags)]

        def columns(j, q):
            return onehot_ref[:, pl.ds(j * chunk + q * WIDTH, WIDTH)]

        def front_start(j):
            for q in units:
                pltpu.matmul_push_rhs(columns(j, q), 0, q)
            for half, lhs in enumerate((fold_high, fold_low)):
                for q in units:
                    pltpu.matmul_acc_lhs(steps[j % lags][q], lhs, None if half else 0)

        def front_end(j):
            at_step = step_ref[:, pl.ds(j * chunk, chunk)]
            mask = step_ids == at_step
            u = jnp.concatenate([pltpu.matmul_pop(steps[j % lags][q]) for q in units], axis=1)
            for c in range(4):
                picked = jnp.where(mask, u[c * step_rows:(c + 1) * step_rows], 0.0)
                value = jnp.sum(picked, axis=0, keepdims=True)
                if c == 3:
                    value = jnp.where(at_step < 0, 1.0, value)
                front_ref[j, pl.ds(c, 1), :] = value

        for j in range(min(2, chunks)):
            front_start(j)
        for j in range(min(2, chunks)):
            front_end(j)

        target_load.wait()
        for j in range(chunks):
            lot = [i for i in range(chunks) if lot_of(i, chunks) == lot_of(j, chunks)]
            for n in range(1, reach + 1 if j == lot[0] else 0):
                size = far_ref.shape[1] if n == reach else 4 * n
                part = far_ref.at[pl.ds(j, len(lot)), pl.ds(0, size)]
                pl.when(ahead_count == n)(waiter(part, part_recv.at[lot_of(j, chunks)]).wait_recv)
            if j == 0 and direct(ns, nt):
                for k in (-reach, reach):
                    @pl.when(inside(slab + k))
                    def _(k=k):
                        pl.semaphore_signal(
                            ready_sem, inc=1, device_id={"slab": slab + k}, device_id_type=MESH)
            at = pl.ds(j * chunk, chunk)
            if j + 2 < chunks:
                front_start(j + 2)
            for q in units:
                for half in range(2):
                    pltpu.matmul_push_rhs(columns(j, q), 1 - half, q, transpose=True)
            front_c = front_ref[j, pl.ds(0, 3), :]
            front_t = front_ref[j, pl.ds(3, 1), :]
            beyond = far_ref[j, pl.ds(4 * (reach - 1), 3), 0, :]
            beyond = jnp.where(slab + reach < ns, beyond, BACKGROUND)
            for k in range(reach - 1, 0, -1):
                pc = far_ref[j, pl.ds(4 * (k - 1), 3), 0, :]
                pt = far_ref[j, 4 * k - 1]
                beyond = jnp.where(slab + k < ns, pc + pt * beyond, beyond)
            pc = own_ref[j, pl.ds(0, 3), 0, :]
            pt = own_ref[j, 3]
            rendered = front_c + front_t * (pc + pt * beyond)
            residual = (COTANGENT_SCALE * RENDER_WEIGHT) * (rendered - target_ref[:, at])
            color_cot = front_t * residual
            trans_cot = front_t * jnp.sum(residual * beyond, axis=0, keepdims=True)
            mask = row_ids16 == row_ref[:, at].astype(jnp.float32).astype(jnp.bfloat16)
            cots = [color_cot[c:c + 1] for c in range(3)] + [trans_cot]
            tops = [cot.astype(jnp.bfloat16) for cot in cots]
            lows = [(cot - top.astype(jnp.float32)).astype(jnp.bfloat16) for cot, top in zip(cots, tops)]
            for half, side in enumerate((tops, lows)):
                for c in range(4):
                    spread = jnp.where(mask, side[c], none)
                    if half:
                        spread = spread.astype(FINE)
                    for q in units:
                        pltpu.matmul_acc_lhs(
                            sums_acc[q][c], spread[:, q * WIDTH:(q + 1) * WIDTH], None if c else 1 - half)
            if j + 2 < chunks:
                front_end(j + 2)
        wait_received(zhalo_ref, halo_recv.at[0], level_count, 2)
        for c in range(channels):
            smooth_planes(c, (0, depth - 1) if depth > 1 else (0,))
        for c in range(4):
            gathered = sum(pltpu.matmul_pop(sums_acc[q][c]) for q in units)
            table_ref[pl.ds(c * rows, rows), :] = (1.0 / COTANGENT_SCALE) * gathered

    pl.run_scoped(scatter, *[
        pltpu.ACC(q)((rows, WIDTH), jnp.float32) for q in units for _ in range(4)
    ], *[
        pltpu.ACC(q)((4 * step_rows, WIDTH), jnp.float32) for _ in range(lags) for q in units
    ])

    zero = jnp.zeros((rx, ry), jnp.float32)
    suffix = [zero, zero, zero]
    later = zero
    squares = zero
    for z in range(depth - 1, -1, -1):
        w = weight_ref[z]
        after = trans_ref[z]
        later = later + after * table_ref[pl.ds(3 * rows + z * rx, rx), :]
        dw = zero
        for c in range(3):
            suffix[c] = suffix[c] + table_ref[pl.ds(c * rows + z * rx, rx), :]
            col = sig_ref[c + 1, z]
            dw = dw + col * suffix[c]
            out = grad_ref[c + 1, z] + w * suffix[c] * (col * (1.0 - col))
            grad_ref[c + 1, z] = out
            squares = squares + out * out
        dtau = after * dw - later
        later = later + w * dw
        out = grad_ref[0, z] + dtau * (sig_ref[0, z] * span)
        grad_ref[0, z] = out
        squares = squares + out * out

    lanes = jnp.sum(squares, axis=0, keepdims=True)
    lanes = sum(lanes[:, i * 128:(i + 1) * 128] for i in range(ry // 128))

    def norm_copy(phase, slots, peer=None):
        src = nsend_ref.at[pl.ds(phase, 1)] if peer else nrecv_ref.at[slots]
        return pltpu.make_async_remote_copy(
            src_ref=src, dst_ref=nrecv_ref.at[slots],
            send_sem=norm_send.at[phase], recv_sem=norm_recv.at[phase],
            device_id=peer or tile_peer(1), device_id_type=MESH)

    if direct(ns, nt):
        far = inside(slab - reach).astype(jnp.int32) + inside(slab + reach).astype(jnp.int32)
        pl.semaphore_wait(ready_sem, far)
    value = lanes
    base = 0
    for phase, peers in enumerate(phases):
        nsend_ref[phase] = value
        for i, peer in enumerate(peers):
            norm_copy(phase, pl.ds(base + i, 1), peer).start()
        if phase == 0:
            for copy in moment_loads:
                copy.wait()
            first_ref[...] = BETA_ONE * first_ref[...]
            second_ref[...] = BETA_TWO * second_ref[...]
            wait_sent(zhalo_ref, halo_send.at[0], level_count, 2)
            wait_sent(edge_ref, halo_send.at[1], beside_count, 2)
            wait_sent(wholes_ref, whole_sem.at[0], ahead_count, reach)
            for k in range(1, reach + 1):
                src = last_ref if k == reach else own_ref
                pl.when(slab >= k)(waiter(src, part_send.at[k - 1]).wait_send)
        norm_copy(phase, pl.ds(base, len(peers))).wait_recv()
        value = value + jnp.sum(nrecv_ref[pl.ds(base, len(peers)), 0, :], axis=0, keepdims=True)
        base += len(peers)
    limit = CLIP_RMS * math.sqrt(4.0 * total_depth * (rx * nt) * ry)
    total_square = jnp.sum(value, axis=1, keepdims=True)
    scale_ref[...] = jnp.broadcast_to(limit / jnp.maximum(jnp.sqrt(total_square), limit), (1, 128))
    base = 0
    for phase, peers in enumerate(phases):
        norm_copy(phase, pl.ds(base, len(peers))).wait_send()
        base += len(peers)


def split(depth):
    return math.gcd(depth, PIECES)


def lot_of(j, chunks):
    return j // 2 if j < chunks - 1 else (chunks - 1) // 2 + 1


def span_reach(ns):
    return max(ns // 2, 1)


def direct(ns, nt):
    return ns * nt <= DIRECT_LIMIT


def adam_kernel(
    grid_ref, first_ref, second_ref, grad_ref, scale_ref,
    grid_hbm, first_hbm, second_hbm, grid_out, first_out, second_out, sem,
):
    channels, depth, rx, ry = grid_ref.shape
    gain = (1.0 - BETA_ONE**STEP) / LEARN_RATE
    slope = gain / math.sqrt(1.0 - BETA_TWO**STEP)
    offset = gain * EPSILON
    scale = jnp.broadcast_to(scale_ref[0:1, 0:1], (rx, ry))
    linear = (1.0 - BETA_ONE) * scale
    square = (1.0 - BETA_TWO) * scale * scale
    pairs = ((first_out, first_hbm), (second_out, second_hbm), (grid_out, grid_hbm))
    pieces = 2
    for c in range(channels):
        for p in range(pieces):
            planes = range(p * depth // pieces, (p + 1) * depth // pieces)
            for z in planes:
                g = grad_ref[c, z]
                first = first_ref[c, z] + linear * g
                second = second_ref[c, z] + square * g * g
                first_out[c, z] = first
                second_out[c, z] = second
                root = second * lax.rsqrt(second)
                grid_out[c, z] = grid_ref[c, z] - first / (root * slope + offset)
            at = pl.ds(p * depth // pieces, depth // pieces)
            for i, (a, b) in enumerate(pairs):
                pltpu.make_async_copy(a.at[c, at], b.at[c, at], sem.at[i]).start()
    for i, (a, b) in enumerate(pairs):
        pltpu.make_async_copy(a, b, sem.at[i]).wait()


def per_device(voxel_grid, first_moment, second_moment, pixel_index, start_slab, ray_count, target):
    ns = lax.axis_size("slab")
    nt = lax.axis_size("tile")
    channels, depth, rx, ry = voxel_grid.shape
    rays = pixel_index.shape[0]
    chunk = math.gcd(rays, CHUNK)
    chunks = rays // chunk
    rows = depth * rx
    reach = span_reach(ns)
    phases = 1 if direct(ns, nt) else 2
    messages = ns * nt - 1 if direct(ns, nt) else nt + ns - 2
    f32 = jnp.float32
    vmem = pl.BlockSpec(memory_space=pltpu.VMEM)
    hbm = pl.BlockSpec(memory_space=pltpu.HBM)
    cells = jax.ShapeDtypeStruct(voxel_grid.shape, f32)
    staged = pl.pallas_call(
        functools.partial(kernel, ns, nt, chunk),
        out_shape=(cells, cells, cells, cells, jax.ShapeDtypeStruct((1, 128), f32)),
        in_specs=[hbm] * 7,
        out_specs=(vmem,) * 5,
        scratch_shapes=[
            pltpu.VMEM((3, 1, rays), jnp.int32),
            pltpu.VMEM(target.shape, f32),
            pltpu.VMEM((channels * rows, ry), jnp.bfloat16),
            pltpu.VMEM((channels * rows, ry), FINE),
            pltpu.VMEM((depth, rx, ry), f32),
            pltpu.VMEM((depth, rx, ry), f32),
            pltpu.VMEM((channels, depth, rx, ry), f32),
            pltpu.VMEM((ry, rays), FINE),
            pltpu.VMEM((1, rays), jnp.int32),
            pltpu.VMEM((1, rays), jnp.int32),
            pltpu.VMEM((channels * rows, ry), f32),
            pltpu.VMEM((4, rx, ry), f32),
            pltpu.VMEM((reach, 4, rx, ry), f32),
            pltpu.VMEM((chunks, 4, chunk), f32),
            pltpu.VMEM((chunks, 4, 1, chunk), f32),
            pltpu.VMEM((chunks, 3, 1, chunk), f32),
            pltpu.VMEM((chunks, 4 * reach - 1, 1, chunk), f32),
            pltpu.VMEM((2, channels, depth, ry), f32),
            pltpu.VMEM((2, channels, depth, ry), f32),
            pltpu.VMEM((2, channels, rx, ry), f32),
            pltpu.VMEM((2, 1, 128), f32),
            pltpu.VMEM((messages, 1, 128), f32),
            pltpu.SemaphoreType.DMA((2,)),
            pltpu.SemaphoreType.DMA((reach,)),
            pltpu.SemaphoreType.DMA((lot_of(chunks - 1, chunks) + 1,)),
            pltpu.SemaphoreType.REGULAR,
            pltpu.SemaphoreType.DMA((2,)),
            pltpu.SemaphoreType.DMA((2,)),
            pltpu.SemaphoreType.DMA((phases,)),
            pltpu.SemaphoreType.DMA((phases,)),
            pltpu.SemaphoreType.DMA((3,)),
        ],
        compiler_params=pltpu.CompilerParams(
            collective_id=0, has_side_effects=True, vmem_limit_bytes=32 * 1024 * 1024
        ),
        name="render_step",
    )(*(pltpu.with_memory_space_constraint(a, pltpu.HBM) for a in (
        voxel_grid,
        first_moment,
        second_moment,
        pixel_index.reshape(1, rays),
        start_slab.reshape(1, rays),
        ray_count.reshape(1, rays),
        target,
    )))
    return pl.pallas_call(
        adam_kernel,
        out_shape=(cells, cells, cells),
        in_specs=[vmem] * 5,
        out_specs=(hbm, hbm, hbm),
        scratch_shapes=[
            pltpu.VMEM(voxel_grid.shape, f32),
            pltpu.VMEM(voxel_grid.shape, f32),
            pltpu.VMEM(voxel_grid.shape, f32),
            pltpu.SemaphoreType.DMA((3,)),
        ],
        compiler_params=pltpu.CompilerParams(vmem_limit_bytes=32 * 1024 * 1024),
        name="adam",
    )(*staged)


def solution(mesh):
    cells = P(None, "slab", "tile", None)
    return jax.shard_map(
        per_device,
        mesh=mesh,
        in_specs=(cells, cells, cells, P("tile"), P("tile"), P("tile"), P(None, "tile")),
        out_specs=(cells, cells, cells),
        check_vma=False,
    )
```

```python
import functools
import math

import jax
import jax.numpy as jnp
from jax import lax
from jax.experimental import pallas as pl
from jax.experimental.pallas import tpu as pltpu
from jax.sharding import PartitionSpec as P

STEP = 20
RENDER_WEIGHT = 1000.0
TV_WEIGHT = 0.05
BACKGROUND = 1.0
STEP_SPAN = 4.0
CLIP_RMS = 0.25
LEARN_RATE = 0.02
BETA_ONE = 0.9
BETA_TWO = 0.99
EPSILON = 1e-08
CHUNK = 512
WIDTH = 256
FINE = jnp.float8_e4m3fn
TABLE_SCALE = 65536.0
COTANGENT_SCALE = 32.0
PIECES = 4
DIRECT_LIMIT = 64
MESH = pl.DeviceIdType.MESH


def kernel(
    ns, nt, chunk,
    grid_hbm, first_hbm, second_hbm, pix_hbm, start_hbm, count_hbm, target_hbm,
    grid_ref, first_ref, second_ref, grad_ref, scale_ref,
    ints_ref, target_ref,
    high_ref, low_ref, trans_ref, weight_ref, sig_ref, onehot_ref, row_ref, step_ref, table_ref,
    whole_ref, wholes_ref, front_ref, own_ref, last_ref, far_ref,
    edge_ref, xhalo_ref, zhalo_ref, nsend_ref, nrecv_ref,
    whole_sem, part_send, part_recv, ready_sem, halo_send, halo_recv, norm_send, norm_recv, load_sem,
):
    channels, depth, rx, ry = grid_ref.shape
    rays = ints_ref.shape[2]
    pix_ref, start_ref, count_ref = (ints_ref.at[i] for i in range(3))
    chunks = rays // chunk
    total_depth = depth * ns
    reach = span_reach(ns)
    span = STEP_SPAN / total_depth
    rows = depth * rx
    slab = lax.axis_index("slab")
    tile = lax.axis_index("tile")

    def slab_peer(d):
        return {"slab": lax.rem(slab + d, ns)}

    def tile_peer(d):
        return {"tile": lax.rem(tile + d, nt)}

    if direct(ns, nt):
        phases = [[
            {"slab": lax.rem(slab + k // nt, ns), "tile": lax.rem(tile + k % nt, nt)}
            for k in [*range(nt, ns * nt), *range(1, nt)]
        ]]
        near = reach
    else:
        phases = [[tile_peer(d) for d in range(1, nt)], [slab_peer(d) for d in range(1, ns)]]
        near = ns - 1
    offsets = [k for k in range(-near, near + 1) if k]

    def inside(s):
        return (s >= 0) & (s < ns)

    pieces = split(depth)
    step = depth // pieces
    barrier = pltpu.get_barrier_semaphore()
    greeters = nt - 1
    for k in offsets:
        @pl.when(inside(slab + k))
        def _(k=k):
            pl.semaphore_signal(
                barrier, inc=1, device_id={"slab": slab + k}, device_id_type=MESH)
        greeters = greeters + inside(slab + k).astype(jnp.int32)
    for d in range(1, nt):
        pl.semaphore_signal(barrier, inc=1, device_id=tile_peer(d), device_id_type=MESH)

    for i, a in enumerate((pix_hbm, start_hbm, count_hbm)):
        pltpu.make_async_copy(a, ints_ref.at[i], load_sem.at[1]).start()
    ints_load = pltpu.make_async_copy(ints_ref, ints_ref, load_sem.at[1])
    grid_load = pltpu.make_async_copy(grid_hbm, grid_ref, load_sem.at[0])
    for c in range(channels):
        for p in range(pieces):
            at = pl.ds(p * step, step)
            pltpu.make_async_copy(grid_hbm.at[c, at], grid_ref.at[c, at], load_sem.at[0]).start()
    target_load = pltpu.make_async_copy(target_hbm, target_ref, load_sem.at[2])
    target_load.start()
    moment_loads = [
        pltpu.make_async_copy(first_hbm, first_ref, load_sem.at[0]),
        pltpu.make_async_copy(second_hbm, second_ref, load_sem.at[1]),
    ]

    ints_load.wait()
    y_ids = lax.broadcasted_iota(jnp.int32, (ry, chunk), 0).astype(jnp.float32).astype(jnp.bfloat16)
    for j in range(chunks):
        at = pl.ds(j * chunk, chunk)
        pix = pix_ref[:, at]
        start = start_ref[:, at]
        px = pix // ry
        py = (pix - px * ry).astype(jnp.float32).astype(jnp.bfloat16)
        length = jnp.clip((start - slab) * depth + count_ref[:, at], 0, depth)
        length = jnp.where(slab >= start, length, 0)
        row_ref[:, at] = jnp.where(length > 0, (length - 1) * rx + px, -1)
        step_ref[:, at] = (slab - start - 1) * rx + px
        hot = jnp.where(y_ids == py, jnp.ones((), jnp.bfloat16), jnp.zeros((), jnp.bfloat16))
        hot = hot.astype(FINE)
        onehot_ref[:, at] = hot

    grid_load.wait()
    for copy in moment_loads:
        copy.start()
    edge_ref[0] = grid_ref[:, :, rx - 1, :]
    edge_ref[1] = grid_ref[:, :, 0, :]

    total = jnp.zeros((rx, ry), jnp.float32)
    before = jnp.ones((rx, ry), jnp.float32)
    sums = [jnp.zeros((rx, ry), jnp.float32) for _ in range(3)]
    for z in range(depth):
        s = grid_ref[0, z]
        e = jnp.exp(-jnp.abs(s))
        tau = (jnp.maximum(s, 0.0) + jnp.log(1.0 + e)) * span
        sig_ref[0, z] = jnp.where(s >= 0, 1.0, e) / (1.0 + e)
        total = total + tau
        after = jnp.exp(-total)
        w = before * (1.0 - jnp.exp(-tau))
        before = after
        trans_ref[z] = after
        weight_ref[z] = w
        for c in range(3):
            col = 1.0 / (1.0 + jnp.exp(-grid_ref[c + 1, z]))
            sig_ref[c + 1, z] = col
            sums[c] = sums[c] + w * col
            table_ref[pl.ds(c * rows + z * rx, rx), :] = sums[c]
        table_ref[pl.ds(3 * rows + z * rx, rx), :] = after
    for c in range(3):
        whole_ref[c] = sums[c]
    whole_ref[3] = before
    full = TABLE_SCALE * table_ref[...]
    high = full.astype(jnp.bfloat16)
    high_ref[...] = high
    low_ref[...] = (full - high.astype(jnp.float32)).astype(FINE)

    def waiter(ref, sem):
        return pltpu.make_async_remote_copy(
            src_ref=ref, dst_ref=ref, send_sem=sem, recv_sem=sem,
            device_id=tile_peer(1), device_id_type=MESH)

    def wait_sent(ref, sem, count, most):
        for n in range(1, most + 1):
            pl.when(count == n)(waiter(ref.at[pl.ds(0, n)], sem).wait_send)

    def wait_received(ref, sem, count, most):
        for n in range(1, most + 1):
            pl.when(count == n)(waiter(ref.at[pl.ds(0, n)], sem).wait_recv)

    behind_count = jnp.minimum(slab, reach)
    ahead_count = jnp.minimum(ns - 1 - slab, reach)
    beside_count = (tile < nt - 1).astype(jnp.int32) + (tile > 0).astype(jnp.int32)
    level_count = (slab < ns - 1).astype(jnp.int32) + (slab > 0).astype(jnp.int32)

    def whole_copy(k):
        return pltpu.make_async_remote_copy(
            src_ref=whole_ref, dst_ref=wholes_ref.at[k - 1],
            send_sem=whole_sem.at[0], recv_sem=whole_sem.at[1],
            device_id=slab_peer(k), device_id_type=MESH)

    def halo_copy(src, dst, i, peer):
        return pltpu.make_async_remote_copy(
            src_ref=src, dst_ref=dst, send_sem=halo_send.at[i // 2], recv_sem=halo_recv.at[i // 2],
            device_id=peer, device_id_type=MESH)

    halos = [
        (halo_copy(grid_ref.at[:, depth - 1], zhalo_ref.at[0], 0, slab_peer(1)), slab < ns - 1),
        (halo_copy(grid_ref.at[:, 0], zhalo_ref.at[1], 1, slab_peer(ns - 1)), slab > 0),
        (halo_copy(edge_ref.at[0], xhalo_ref.at[0], 2, tile_peer(1)), tile < nt - 1),
        (halo_copy(edge_ref.at[1], xhalo_ref.at[1], 3, tile_peer(nt - 1)), tile > 0),
    ]
    def part_copy(k, j):
        src = last_ref if k == reach else own_ref
        return pltpu.make_async_remote_copy(
            src_ref=src.at[j], dst_ref=far_ref.at[j, pl.ds(4 * (k - 1), src.shape[1])],
            send_sem=part_send.at[k - 1], recv_sem=part_recv.at[lot_of(j, chunks)],
            device_id=slab_peer(ns - k), device_id_type=MESH)

    row_ids = lax.broadcasted_iota(jnp.int32, (rows, chunk), 0)

    units = range(chunk // WIDTH)

    def enter():
        pl.semaphore_wait(barrier, greeters)
        for k in range(1, min(reach, ns - 1) + 1):
            pl.when(slab == 0)(whole_copy(k).start)
        for k in range(reach, 0, -1):
            pl.when((slab > 0) & (slab + k < ns))(whole_copy(k).start)
        for copy, sends in halos[2:]:
            pl.when(sends)(copy.start)

    def gather(*accs):
        banks = [[accs[(b * len(units) + q) * 4:][:4] for q in units] for b in range(2)]
        for j in range(chunks + 1):
            if j < chunks:
                hot = onehot_ref[:, pl.ds(j * chunk, chunk)]
                for q in units:
                    for half in range(2):
                        pltpu.matmul_push_rhs(hot[:, q * WIDTH:(q + 1) * WIDTH], half, q)
                for half, side in enumerate((low_ref, high_ref)):
                    for c in range(4):
                        lhs = side[pl.ds(c * rows, rows), :]
                        for q in units:
                            pltpu.matmul_acc_lhs(banks[j % 2][q][c], lhs, None if c else half)
            if j == 0:
                continue
            i = j - 1
            row = row_ref[:, pl.ds(i * chunk, chunk)]
            mask = row_ids == row
            for c in range(4):
                u = jnp.concatenate([pltpu.matmul_pop(banks[i % 2][q][c]) for q in units], axis=1)
                part = jnp.sum(jnp.where(mask, u, 0.0), axis=0, keepdims=True)
                part = part * (1.0 / TABLE_SCALE)
                if c == 3:
                    part = jnp.where(row < 0, 1.0, part)
                own_ref[i, c] = part
            for c in range(3):
                last_ref[i, c] = own_ref[i, c] + BACKGROUND * part
            lot = [n for n in range(chunks) if lot_of(n, chunks) == lot_of(i, chunks)]
            if i != lot[-1]:
                continue
            for n in lot:
                for k in range(1, reach + 1):
                    pl.when(slab >= k)(part_copy(k, n).start)

    enter()
    pl.run_scoped(gather, *[
        pltpu.ACC(q)((rows, WIDTH), jnp.float32)
        for _ in range(2) for q in units for _ in range(4)
    ])

    pl.when(halos[1][1])(halos[1][0].start)
    x_ids = lax.broadcasted_iota(jnp.int32, (rx, ry), 0)
    lane_ids = lax.broadcasted_iota(jnp.int32, (rx, ry), 1)
    first_x = tile == 0
    last_x = tile == nt - 1
    def smooth_planes(c, planes):
        for z in planes:
            g = grid_ref[c, z]
            if z > 0:
                below = grid_ref[c, z - 1]
            else:
                below = jnp.where(slab > 0, zhalo_ref[0, c], g)
            if z < depth - 1:
                above = grid_ref[c, z + 1]
            else:
                above = jnp.where(slab < ns - 1, zhalo_ref[1, c], g)
            xl = jnp.broadcast_to(xhalo_ref[0, c, pl.ds(z, 1), :], (rx, ry))
            xh = jnp.broadcast_to(xhalo_ref[1, c, pl.ds(z, 1), :], (rx, ry))
            xl = jnp.where(first_x, g, xl)
            xh = jnp.where(last_x, g, xh)
            left = jnp.where(x_ids == 0, xl, pltpu.roll(g, 1, 0))
            right = jnp.where(x_ids == rx - 1, xh, pltpu.roll(g, rx - 1, 0))
            down = jnp.where(lane_ids == 0, g, pltpu.roll(g, 1, 1))
            up = jnp.where(lane_ids == ry - 1, g, pltpu.roll(g, ry - 1, 1))
            smooth = (g - below) + (g - above) + (g - left) + (g - right) + (g - down) + (g - up)
            grad_ref[c, z] = (2.0 * TV_WEIGHT) * smooth

    wait_received(xhalo_ref, halo_recv.at[1], beside_count, 2)
    for c in range(channels):
        smooth_planes(c, range(1, depth - 1))
    pl.when(halos[0][1])(halos[0][0].start)
    wait_received(wholes_ref, whole_sem.at[1], behind_count, reach)
    folded = [[] for _ in range(4)]
    fold_t = jnp.ones((rx, ry), jnp.float32)
    fold_c = [jnp.zeros((rx, ry), jnp.float32)] * 3
    for k in range(1, reach + 1):
        there = slab >= k
        t = wholes_ref[k - 1, 3]
        fold_c = [jnp.where(there, wholes_ref[k - 1, c] + t * fold_c[c], 0.0) for c in range(3)]
        fold_t = jnp.where(there, t * fold_t, 0.0)
        for c in range(4):
            folded[c].append(fold_c[c] if c < 3 else fold_t)
    folds = jnp.concatenate([f for fs in folded for f in fs], axis=0)
    fold_high = folds.astype(jnp.bfloat16)
    fold_low = (folds - fold_high.astype(jnp.float32)).astype(jnp.bfloat16)
    step_rows = reach * rx
    step_ids = lax.broadcasted_iota(jnp.int32, (step_rows, chunk), 0)
    row_ids16 = row_ids.astype(jnp.float32).astype(jnp.bfloat16)
    none = jnp.zeros((), jnp.bfloat16)
    lags = 4

    def scatter(*accs):
        sums_acc = [accs[q * 4:][:4] for q in units]
        accs = accs[4 * len(units):]
        steps = [[accs[b * len(units) + q] for q in units] for b in range(lags)]

        def columns(j, q):
            return onehot_ref[:, pl.ds(j * chunk + q * WIDTH, WIDTH)]

        def front_start(j):
            for q in units:
                pltpu.matmul_push_rhs(columns(j, q), 0, q)
            for half, lhs in enumerate((fold_high, fold_low)):
                for q in units:
                    pltpu.matmul_acc_lhs(steps[j % lags][q], lhs, None if half else 0)

        def front_end(j):
            at_step = step_ref[:, pl.ds(j * chunk, chunk)]
            mask = step_ids == at_step
            u = jnp.concatenate([pltpu.matmul_pop(steps[j % lags][q]) for q in units], axis=1)
            for c in range(4):
                picked = jnp.where(mask, u[c * step_rows:(c + 1) * step_rows], 0.0)
                value = jnp.sum(picked, axis=0, keepdims=True)
                if c == 3:
                    value = jnp.where(at_step < 0, 1.0, value)
                front_ref[j, pl.ds(c, 1), :] = value

        for j in range(min(2, chunks)):
            front_start(j)
        for j in range(min(2, chunks)):
            front_end(j)

        target_load.wait()
        for j in range(chunks):
            lot = [i for i in range(chunks) if lot_of(i, chunks) == lot_of(j, chunks)]
            for n in range(1, reach + 1 if j == lot[0] else 0):
                size = far_ref.shape[1] if n == reach else 4 * n
                part = far_ref.at[pl.ds(j, len(lot)), pl.ds(0, size)]
                pl.when(ahead_count == n)(waiter(part, part_recv.at[lot_of(j, chunks)]).wait_recv)
            if j == 0 and direct(ns, nt):
                for k in (-reach, reach):
                    @pl.when(inside(slab + k))
                    def _(k=k):
                        pl.semaphore_signal(
                            ready_sem, inc=1, device_id={"slab": slab + k}, device_id_type=MESH)
            at = pl.ds(j * chunk, chunk)
            if j + 2 < chunks:
                front_start(j + 2)
            for q in units:
                for half in range(2):
                    pltpu.matmul_push_rhs(columns(j, q), 1 - half, q, transpose=True)
            front_c = front_ref[j, pl.ds(0, 3), :]
            front_t = front_ref[j, pl.ds(3, 1), :]
            beyond = far_ref[j, pl.ds(4 * (reach - 1), 3), 0, :]
            beyond = jnp.where(slab + reach < ns, beyond, BACKGROUND)
            for k in range(reach - 1, 0, -1):
                pc = far_ref[j, pl.ds(4 * (k - 1), 3), 0, :]
                pt = far_ref[j, 4 * k - 1]
                beyond = jnp.where(slab + k < ns, pc + pt * beyond, beyond)
            pc = own_ref[j, pl.ds(0, 3), 0, :]
            pt = own_ref[j, 3]
            rendered = front_c + front_t * (pc + pt * beyond)
            residual = (COTANGENT_SCALE * RENDER_WEIGHT) * (rendered - target_ref[:, at])
            color_cot = front_t * residual
            trans_cot = front_t * jnp.sum(residual * beyond, axis=0, keepdims=True)
            mask = row_ids16 == row_ref[:, at].astype(jnp.float32).astype(jnp.bfloat16)
            cots = [color_cot[c:c + 1] for c in range(3)] + [trans_cot]
            tops = [cot.astype(jnp.bfloat16) for cot in cots]
            lows = [(cot - top.astype(jnp.float32)).astype(jnp.bfloat16) for cot, top in zip(cots, tops)]
            for half, side in enumerate((tops, lows)):
                for c in range(4):
                    spread = jnp.where(mask, side[c], none)
                    if half:
                        spread = spread.astype(FINE)
                    for q in units:
                        pltpu.matmul_acc_lhs(
                            sums_acc[q][c], spread[:, q * WIDTH:(q + 1) * WIDTH], None if c else 1 - half)
            if j + 2 < chunks:
                front_end(j + 2)
        wait_received(zhalo_ref, halo_recv.at[0], level_count, 2)
        for c in range(channels):
            smooth_planes(c, (0, depth - 1) if depth > 1 else (0,))
        for c in range(4):
            gathered = sum(pltpu.matmul_pop(sums_acc[q][c]) for q in units)
            table_ref[pl.ds(c * rows, rows), :] = (1.0 / COTANGENT_SCALE) * gathered

    pl.run_scoped(scatter, *[
        pltpu.ACC(q)((rows, WIDTH), jnp.float32) for q in units for _ in range(4)
    ], *[
        pltpu.ACC(q)((4 * step_rows, WIDTH), jnp.float32) for _ in range(lags) for q in units
    ])

    zero = jnp.zeros((rx, ry), jnp.float32)
    suffix = [zero, zero, zero]
    later = zero
    squares = zero
    for z in range(depth - 1, -1, -1):
        w = weight_ref[z]
        after = trans_ref[z]
        later = later + after * table_ref[pl.ds(3 * rows + z * rx, rx), :]
        dw = zero
        for c in range(3):
            suffix[c] = suffix[c] + table_ref[pl.ds(c * rows + z * rx, rx), :]
            col = sig_ref[c + 1, z]
            dw = dw + col * suffix[c]
            out = grad_ref[c + 1, z] + w * suffix[c] * (col * (1.0 - col))
            grad_ref[c + 1, z] = out
            squares = squares + out * out
        dtau = after * dw - later
        later = later + w * dw
        out = grad_ref[0, z] + dtau * (sig_ref[0, z] * span)
        grad_ref[0, z] = out
        squares = squares + out * out

    lanes = jnp.sum(squares, axis=0, keepdims=True)
    lanes = sum(lanes[:, i * 128:(i + 1) * 128] for i in range(ry // 128))

    def norm_copy(phase, slots, peer=None):
        src = nsend_ref.at[pl.ds(phase, 1)] if peer else nrecv_ref.at[slots]
        return pltpu.make_async_remote_copy(
            src_ref=src, dst_ref=nrecv_ref.at[slots],
            send_sem=norm_send.at[phase], recv_sem=norm_recv.at[phase],
            device_id=peer or tile_peer(1), device_id_type=MESH)

    if direct(ns, nt):
        far = inside(slab - reach).astype(jnp.int32) + inside(slab + reach).astype(jnp.int32)
        pl.semaphore_wait(ready_sem, far)
    value = lanes
    base = 0
    for phase, peers in enumerate(phases):
        nsend_ref[phase] = value
        for i, peer in enumerate(peers):
            norm_copy(phase, pl.ds(base + i, 1), peer).start()
        if phase == 0:
            for copy in moment_loads:
                copy.wait()
            first_ref[...] = BETA_ONE * first_ref[...]
            second_ref[...] = BETA_TWO * second_ref[...]
            wait_sent(zhalo_ref, halo_send.at[0], level_count, 2)
            wait_sent(edge_ref, halo_send.at[1], beside_count, 2)
            wait_sent(wholes_ref, whole_sem.at[0], ahead_count, reach)
            for k in range(1, reach + 1):
                src = last_ref if k == reach else own_ref
                pl.when(slab >= k)(waiter(src, part_send.at[k - 1]).wait_send)
        norm_copy(phase, pl.ds(base, len(peers))).wait_recv()
        value = value + jnp.sum(nrecv_ref[pl.ds(base, len(peers)), 0, :], axis=0, keepdims=True)
        base += len(peers)
    limit = CLIP_RMS * math.sqrt(4.0 * total_depth * (rx * nt) * ry)
    total_square = jnp.sum(value, axis=1, keepdims=True)
    scale_ref[...] = jnp.broadcast_to(limit / jnp.maximum(jnp.sqrt(total_square), limit), (1, 128))
    base = 0
    for phase, peers in enumerate(phases):
        norm_copy(phase, pl.ds(base, len(peers))).wait_send()
        base += len(peers)


def split(depth):
    return math.gcd(depth, PIECES)


def lot_of(j, chunks):
    return j // 2 if j < chunks - 1 else (chunks - 1) // 2 + 1


def span_reach(ns):
    return max(ns // 2, 1)


def direct(ns, nt):
    return ns * nt <= DIRECT_LIMIT


def adam_kernel(
    grid_ref, first_ref, second_ref, grad_ref, scale_ref,
    grid_hbm, first_hbm, second_hbm, grid_out, first_out, second_out, sem,
):
    channels, depth, rx, ry = grid_ref.shape
    gain = (1.0 - BETA_ONE**STEP) / LEARN_RATE
    slope = gain / math.sqrt(1.0 - BETA_TWO**STEP)
    offset = gain * EPSILON
    scale = jnp.broadcast_to(scale_ref[0:1, 0:1], (rx, ry))
    linear = (1.0 - BETA_ONE) * scale
    square = (1.0 - BETA_TWO) * scale * scale
    pairs = ((first_out, first_hbm), (second_out, second_hbm), (grid_out, grid_hbm))
    pieces = 2
    for c in range(channels):
        for p in range(pieces):
            planes = range(p * depth // pieces, (p + 1) * depth // pieces)
            for z in planes:
                g = grad_ref[c, z]
                first = first_ref[c, z] + linear * g
                second = second_ref[c, z] + square * g * g
                first_out[c, z] = first
                second_out[c, z] = second
                root = second * lax.rsqrt(second)
                grid_out[c, z] = grid_ref[c, z] - first / (root * slope + offset)
            at = pl.ds(p * depth // pieces, depth // pieces)
            for i, (a, b) in enumerate(pairs):
                pltpu.make_async_copy(a.at[c, at], b.at[c, at], sem.at[i]).start()
    for i, (a, b) in enumerate(pairs):
        pltpu.make_async_copy(a, b, sem.at[i]).wait()


def per_device(voxel_grid, first_moment, second_moment, pixel_index, start_slab, ray_count, target):
    ns = lax.axis_size("slab")
    nt = lax.axis_size("tile")
    channels, depth, rx, ry = voxel_grid.shape
    rays = pixel_index.shape[0]
    chunk = math.gcd(rays, CHUNK)
    chunks = rays // chunk
    rows = depth * rx
    reach = span_reach(ns)
    phases = 1 if direct(ns, nt) else 2
    messages = ns * nt - 1 if direct(ns, nt) else nt + ns - 2
    f32 = jnp.float32
    vmem = pl.BlockSpec(memory_space=pltpu.VMEM)
    hbm = pl.BlockSpec(memory_space=pltpu.HBM)
    cells = jax.ShapeDtypeStruct(voxel_grid.shape, f32)
    staged = pl.pallas_call(
        functools.partial(kernel, ns, nt, chunk),
        out_shape=(cells, cells, cells, cells, jax.ShapeDtypeStruct((1, 128), f32)),
        in_specs=[hbm] * 7,
        out_specs=(vmem,) * 5,
        scratch_shapes=[
            pltpu.VMEM((3, 1, rays), jnp.int32),
            pltpu.VMEM(target.shape, f32),
            pltpu.VMEM((channels * rows, ry), jnp.bfloat16),
            pltpu.VMEM((channels * rows, ry), FINE),
            pltpu.VMEM((depth, rx, ry), f32),
            pltpu.VMEM((depth, rx, ry), f32),
            pltpu.VMEM((channels, depth, rx, ry), f32),
            pltpu.VMEM((ry, rays), FINE),
            pltpu.VMEM((1, rays), jnp.int32),
            pltpu.VMEM((1, rays), jnp.int32),
            pltpu.VMEM((channels * rows, ry), f32),
            pltpu.VMEM((4, rx, ry), f32),
            pltpu.VMEM((reach, 4, rx, ry), f32),
            pltpu.VMEM((chunks, 4, chunk), f32),
            pltpu.VMEM((chunks, 4, 1, chunk), f32),
            pltpu.VMEM((chunks, 3, 1, chunk), f32),
            pltpu.VMEM((chunks, 4 * reach - 1, 1, chunk), f32),
            pltpu.VMEM((2, channels, depth, ry), f32),
            pltpu.VMEM((2, channels, depth, ry), f32),
            pltpu.VMEM((2, channels, rx, ry), f32),
            pltpu.VMEM((2, 1, 128), f32),
            pltpu.VMEM((messages, 1, 128), f32),
            pltpu.SemaphoreType.DMA((2,)),
            pltpu.SemaphoreType.DMA((reach,)),
            pltpu.SemaphoreType.DMA((lot_of(chunks - 1, chunks) + 1,)),
            pltpu.SemaphoreType.REGULAR,
            pltpu.SemaphoreType.DMA((2,)),
            pltpu.SemaphoreType.DMA((2,)),
            pltpu.SemaphoreType.DMA((phases,)),
            pltpu.SemaphoreType.DMA((phases,)),
            pltpu.SemaphoreType.DMA((3,)),
        ],
        compiler_params=pltpu.CompilerParams(
            collective_id=0, has_side_effects=True, vmem_limit_bytes=32 * 1024 * 1024
        ),
        name="render_step",
    )(*(pltpu.with_memory_space_constraint(a, pltpu.HBM) for a in (
        voxel_grid,
        first_moment,
        second_moment,
        pixel_index.reshape(1, rays),
        start_slab.reshape(1, rays),
        ray_count.reshape(1, rays),
        target,
    )))
    return pl.pallas_call(
        adam_kernel,
        out_shape=(cells, cells, cells),
        in_specs=[vmem] * 5,
        out_specs=(hbm, hbm, hbm),
        scratch_shapes=[
            pltpu.VMEM(voxel_grid.shape, f32),
            pltpu.VMEM(voxel_grid.shape, f32),
            pltpu.VMEM(voxel_grid.shape, f32),
            pltpu.SemaphoreType.DMA((3,)),
        ],
        compiler_params=pltpu.CompilerParams(vmem_limit_bytes=32 * 1024 * 1024),
        name="adam",
    )(*staged)


def solution(mesh):
    cells = P(None, "slab", "tile", None)
    return jax.shard_map(
        per_device,
        mesh=mesh,
        in_specs=(cells, cells, cells, P("tile"), P("tile"), P("tile"), P(None, "tile")),
        out_specs=(cells, cells, cells),
        check_vma=False,
    )
```
